256 devices in a mesh: rep: 32 (over z, y), nodes: 8 (over x, core).
Axes of the slice: x: 4, y: 4, z: 8, core: 2. Of those that a mesh axis runs over, the one named last changes fastest.
Arguments:
- adjacency: bfloat16 [32, 512, 16384], P(None, 'nodes', 'rep')
- features: bfloat16 [16384, 50], P(('rep', 'nodes'))
- w_one: float32 [50, 2048], replicated
- w_two: float32 [2048, 121], replicated
- labels: int32 [16384], P(('rep', 'nodes'))
- label_mask: int32 [16384], P(('rep', 'nodes'))
Outputs:
- output 1: float32 [], replicated
- output 2: float32 [50, 2048], replicated
- output 3: float32 [2048, 121], replicated
All inputs are finite; a program needn't handle non-finite values.
Results may differ from the reference program's by a relative error of at most 0.001.
Values are sent between devices in bfloat16 or wider.
A program may use at most 768 MiB of HBM per device.

```python
import jax
import jax.numpy as jnp
from jax import lax

REPLICAS = 32
NODE_GROUP = 8
ROWS_DEV = 64
F_IN = 50
F_HID = 2048
N_CLASS = 121
N_COMM = 16

N_TOTAL = ROWS_DEV * REPLICAS * NODE_GROUP


def make_adjacency(edge_key, community):
    col_ids = jnp.arange(N_TOTAL)

    def one_block(block_id):
        row_ids = block_id * ROWS_DEV + jnp.arange(ROWS_DEV)
        coin_draw = jax.random.randint(jax.random.fold_in(edge_key, block_id), (ROWS_DEV, N_TOTAL), 0, 1000)
        comm_rows = lax.dynamic_slice(community, (block_id * ROWS_DEV,), (ROWS_DEV,))
        same_comm = comm_rows[:, None] == community[None, :]
        has_edge = (coin_draw < jnp.where(same_comm, 500, 40)) | (row_ids[:, None] == col_ids[None, :])
        degree = jnp.sum(has_edge.astype(jnp.int32), axis=1)
        return (has_edge.astype(jnp.float32) / degree[:, None].astype(jnp.float32)).astype(jnp.bfloat16)

    row_blocks = lax.map(one_block, jnp.arange(N_TOTAL // ROWS_DEV))
    return row_blocks.reshape(REPLICAS, N_TOTAL // REPLICAS, N_TOTAL)


def setup_inputs(seed: int = 0) -> dict:
    base_key = jax.random.key(seed)
    key_list = jax.random.split(base_key, 8)
    community = jax.random.randint(key_list[0], (N_TOTAL,), 0, N_COMM)
    adjacency = make_adjacency(key_list[1], community)
    comm_embed = jax.random.normal(key_list[2], (N_COMM, F_IN), jnp.float32)
    feat_noise = 0.5 * jax.random.normal(key_list[3], (N_TOTAL, F_IN), jnp.float32)
    features = (comm_embed[community] + feat_noise).astype(jnp.bfloat16)
    w_one = jax.random.normal(key_list[4], (F_IN, F_HID), jnp.float32) * F_IN ** -0.5
    w_two = 2.0 * jax.random.normal(key_list[5], (F_HID, N_CLASS), jnp.float32) * F_HID ** -0.5
    labels = jax.random.randint(key_list[6], (N_TOTAL,), 0, N_CLASS).astype(jnp.int32)
    mask_draw = jax.random.randint(key_list[7], (N_TOTAL,), 0, 10)
    label_mask = jnp.where((mask_draw < 6) | (jnp.arange(N_TOTAL) == 0), 1, 0).astype(jnp.int32)
    return {"adjacency": adjacency, "features": features, "w_one": w_one, "w_two": w_two, "labels": labels, "label_mask": label_mask}


def reference(adjacency, features, w_one, w_two, labels, label_mask):
    node_count = features.shape[0]
    adj_flat = adjacency.reshape(node_count, node_count)
    w_one_lo = w_one.astype(jnp.bfloat16)
    w_two_lo = w_two.astype(jnp.bfloat16)
    y_one = jnp.dot(features, w_one_lo, preferred_element_type=jnp.float32).astype(jnp.bfloat16)
    z_one = jnp.dot(adj_flat, y_one, preferred_element_type=jnp.float32)
    h_one = jnp.maximum(z_one, 0.0).astype(jnp.bfloat16)
    y_two = jnp.dot(h_one, w_two_lo, preferred_element_type=jnp.float32).astype(jnp.bfloat16)
    z_two = jnp.dot(adj_flat, y_two, preferred_element_type=jnp.float32)
    weights = label_mask.astype(jnp.float32)
    label_count = jnp.sum(weights)
    log_probs = jax.nn.log_softmax(z_two, axis=-1)
    one_hot = (labels[:, None] == jnp.arange(N_CLASS)[None, :]).astype(jnp.float32)
    loss_value = -jnp.sum(weights * jnp.sum(one_hot * log_probs, axis=-1)) / label_count
    g_two = ((jnp.exp(log_probs) - one_hot) * (weights / label_count)[:, None]).astype(jnp.bfloat16)
    dy_two = lax.dot_general(adj_flat, g_two, (((0,), (0,)), ((), ())), preferred_element_type=jnp.float32).astype(jnp.bfloat16)
    dw_two = lax.dot_general(h_one, dy_two, (((0,), (0,)), ((), ())), preferred_element_type=jnp.float32)
    dh_one = lax.dot_general(dy_two, w_two_lo, (((1,), (1,)), ((), ())), preferred_element_type=jnp.float32)
    g_one = jnp.where(z_one > 0.0, dh_one, 0.0).astype(jnp.bfloat16)
    dy_one = lax.dot_general(adj_flat, g_one, (((0,), (0,)), ((), ())), preferred_element_type=jnp.float32).astype(jnp.bfloat16)
    dw_one = lax.dot_general(features, dy_one, (((0,), (0,)), ((), ())), preferred_element_type=jnp.float32)
    return (loss_value, dw_one, dw_two)
```

```python
import functools

import jax
import jax.numpy as jnp
from jax import lax
from jax.experimental import pallas as pl
from jax.experimental.pallas import tpu as pltpu
from jax.sharding import PartitionSpec as P

Y_DIM = 4
X_DIM = 4
CORES = 2
LANES = 128
NSUB = 2
BF = jnp.bfloat16
F32 = jnp.float32


def _step(dims, a_hbm, xs, lab, w1, w2, w2t, dw1_out, dw2_out, loss_out,
          af, xp, y1, cs, cr, sb, rb, z1, h1, y2, yp, zp, zr, g2, gr, dp, rc, rx, ry, g1, gz, gt, dy, rcy, rx1, rx2,
          wb, rwc, rwx, rwy, sy, rwz, fz, oz, oy, ox, oc, ssem, rsem, rsem_a, rsem_b, rsem_f, rsem_ring, rsem_ag, rsem_x):
    Z, Y, X, C, S, CB, H, F, NC = dims
    I = X * C
    NP = Y * I
    HR = H // (2 * NSUB)
    HB = H // Y
    HU = HB // 2
    NCH = Y * S
    rid = lax.axis_index("rep")
    nid = lax.axis_index("nodes")
    z, y, x, c = rid // Y, rid % Y, nid // C, nid % C
    me = y * I + nid
    partner = (rid, x * C + 1 - c)

    def at_z(zz):
        return (zz * Y + y, nid)

    def at_y(yy):
        return (z * Y + yy, nid)

    def at_x(xx):
        return (rid, xx * C + c)

    def send(src, dst, ss, rs, dev):
        pltpu.make_async_remote_copy(src_ref=src, dst_ref=dst, send_sem=ss, recv_sem=rs, device_id=dev,
                                     device_id_type=pl.DeviceIdType.MESH).start()

    def arrived(ref, rs):
        pltpu.make_async_remote_copy(src_ref=ref, dst_ref=ref, send_sem=ssem.at[0], recv_sem=rs, device_id=partner,
                                     device_id_type=pl.DeviceIdType.MESH).wait_recv()

    def sent(ref, ss):
        pltpu.make_async_remote_copy(src_ref=ref, dst_ref=ref, send_sem=ss, recv_sem=rsem.at[0], device_id=partner,
                                     device_id_type=pl.DeviceIdType.MESH).wait_send()

    def dot(a, b):
        return jnp.dot(a, b, preferred_element_type=F32)

    (E_X, E_A, E_B, E_F, E_RING, E_CNT, E_Y2, E_Z2, E_G2, E_DC, E_DX, E_DY, E_G1, E_AG, E_RC0, E_RC1, E_RX, E_WC, E_WX, E_WY, E_WZ,
     E_OZ, E_OY, E_OX, E_OC, E_RX2, E_LOAD) = range(27)

    load = pltpu.make_async_copy(a_hbm, af.at[y], ssem.at[E_LOAD])
    load.start()

    bar = pltpu.get_barrier_semaphore()

    def greet_plane(d, u):
        p = lax.rem(me + d, NP)
        pl.semaphore_signal(bar, inc=1, device_id=(z * Y + p // I, p % I), device_id_type=pl.DeviceIdType.MESH)
        return u

    lax.fori_loop(1, NP, greet_plane, 0)
    for d in range(1, Z):
        pl.semaphore_signal(bar, inc=1, device_id=at_z((z + d) % Z), device_id_type=pl.DeviceIdType.MESH)
    pl.semaphore_wait(bar, NP - 1 + Z - 1)

    def send_x(d, u):
        p = lax.rem(me + d, NP)
        send(xs, xp.at[me], ssem.at[E_X], rsem.at[E_X], (z * Y + p // I, p % I))
        return u

    lax.fori_loop(1, NP, send_x, 0)
    xp[me] = xs[...]
    load.wait()

    order = []
    for k in range(1, Z // 2 + 1):
        order.append(-k)
        if k < Z // 2:
            order.append(k)
    order.append(0)
    for k in order:
        zc = (z + k + Z) % Z
        for d in (1, 3, 2):
            yq = (y + d) % Y
            send(af.at[y, zc, yq], af.at[y, zc, yq], ssem.at[E_A], rsem_a.at[d - 1, zc], at_y(yq))
    for d in (1, 3):
        yq = (y + d) % Y
        for k in range(1, Y):
            ya = (yq + k) % Y
            send(af.at[y, :, ya], af.at[y, :, ya], ssem.at[E_B], rsem_b.at[d // 2, k - 1], at_y(yq))

    arrived(xp.at[pl.ds(0, NP - 1)], rsem.at[E_X])
    HT = HR

    def y1_tile(t, u):
        yb = t // (H // HT)
        col = pl.multiple_of((t % (H // HT)) * HT, HT)
        rows = xp[pl.ds(yb * I, I)].reshape(CB, LANES)
        y1[pl.ds(pl.multiple_of(yb * CB, CB), CB), pl.ds(col, HT)] = dot(rows, w1[:, pl.ds(col, HT)]).astype(BF)
        return u

    lax.fori_loop(0, Y * (H // HT), y1_tile, 0)

    lane = lax.broadcasted_iota(jnp.int32, (S, LANES), 1)
    counted = jnp.sum(xp[...].astype(F32).reshape(NP * S, LANES), axis=0, keepdims=True)
    counted = jnp.sum(jnp.where(lane[0:1] == F, counted, 0.0), axis=1, keepdims=True)
    cs[...] = jnp.broadcast_to(counted, (8, LANES))
    cr[z] = cs[...]
    for d in range(1, Z):
        zq = (z + d) % Z
        send(cs, cr.at[z], ssem.at[E_CNT], rsem.at[E_CNT], at_z(zq))

    def wait_a(zc):
        for d in range(1, Y):
            arrived(af.at[0, 0, 0], rsem_a.at[d - 1, zc])

    def ring(t, u):
        s, j = t // (2 * NSUB), t % (2 * NSUB)
        up = j < NSUB
        dest = lax.rem(jnp.where(up, z - 1 - s, z + 1 + s) + 2 * Z, Z)
        nb = lax.rem(jnp.where(up, z + 1, z - 1) + Z, Z)
        col = pl.multiple_of(j * HR, HR)
        fresh = ((j == 0) & ((s < Z // 2) | (s == Z - 1))) | ((j == NSUB) & (s < Z // 2 - 1))

        @pl.when(fresh)
        def _():
            wait_a(dest)

        acc = dot(af[0, dest, y], y1[pl.ds(0, CB), pl.ds(col, HR)])
        for yb in range(1, Y):
            acc = acc + dot(af[yb, dest, y], y1[pl.ds(yb * CB, CB), pl.ds(col, HR)])
        z1[:, pl.ds(col, HR)] = acc

        @pl.when(s > 0)
        def _():
            prev = jnp.maximum(s - 1, 0)
            arrived(rb.at[0, 0], rsem_ring.at[j, prev])
            z1[:, pl.ds(col, HR)] = z1[:, pl.ds(col, HR)] + rb[j, prev]

        @pl.when(s < Z - 1)
        def _():
            here = jnp.minimum(s, Z - 2)
            sb[j, here] = z1[:, pl.ds(col, HR)]
            send(sb.at[j, here], rb.at[j, here], ssem.at[E_RING], rsem_ring.at[j, here], at_z(nb))

        return u

    lax.fori_loop(0, Z * 2 * NSUB, ring, 0)

    h1[...] = jnp.maximum(z1[...], 0.0).astype(BF)
    y2[...] = dot(h1[...], w2[...]).astype(BF)

    def send_y2(d, u):
        p = lax.rem(me + d, NP)
        send(y2, yp.at[me], ssem.at[E_Y2], rsem.at[E_Y2], (z * Y + p // I, p % I))
        return u

    lax.fori_loop(1, NP, send_y2, 0)
    yp[me] = y2[...]
    arrived(yp.at[pl.ds(0, NP - 1)], rsem.at[E_Y2])
    for yb in range(Y):
        part = dot(af[yb, :, y].reshape(Z * S, CB), yp[yb * I:(yb + 1) * I].reshape(CB, LANES)).reshape(Z, S, LANES)
        zp[...] = part if yb == 0 else zp[...] + part
    for d in range(1, Z):
        zq = (z + d) % Z
        send(zp.at[zq], zr.at[z], ssem.at[E_Z2], rsem.at[E_Z2], at_z(zq))
    zr[z] = zp[z]
    for d in (1, 3):
        for k in range(1, Y):
            arrived(af.at[0, :, 0], rsem_b.at[d // 2, k - 1])
    half = Z // 2
    for d in (1, 3):
        ys, yq = (y - d + Y) % Y, (y + d) % Y
        lo = 0 if d == 1 else half
        for k in range(1, Y):
            ya = (yq + k) % Y
            send(af.at[ys, pl.ds(lo, half), ya], af.at[ys, pl.ds(lo, half), ya], ssem.at[E_F], rsem_f.at[d // 2, k - 1], at_y(yq))
    arrived(zr.at[pl.ds(0, Z - 1)], rsem.at[E_Z2])
    z2 = zr[0]
    for k in range(1, Z):
        z2 = z2 + zr[k]

    arrived(cr.at[pl.ds(0, Z - 1)], rsem.at[E_CNT])
    total = cr[0]
    for k in range(1, Z):
        total = total + cr[k]
    count = total[0:1, 0:1]
    weights = jnp.sum(jnp.where(lane == F, xs[...].astype(F32), 0.0), axis=1, keepdims=True)
    real = lane < NC
    top = jnp.max(jnp.where(real, z2, -jnp.inf), axis=1, keepdims=True)
    shifted = jnp.where(real, z2 - top, 0.0)
    log_probs = shifted - jnp.log(jnp.sum(jnp.where(real, jnp.exp(shifted), 0.0), axis=1, keepdims=True))
    hot = lab[...] == lane
    picked = jnp.sum(jnp.where(hot, log_probs, 0.0), axis=1, keepdims=True)
    loss_part = -jnp.sum(weights * picked, axis=0, keepdims=True)
    diff = jnp.where(real, jnp.exp(log_probs), 0.0) - hot.astype(F32)
    g2[...] = (diff * (weights / count)).astype(BF)
    for d in range(1, Z):
        zq = (z + d) % Z
        send(g2, gr.at[z], ssem.at[E_G2], rsem.at[E_G2], at_z(zq))
    gr[z] = g2[...]
    arrived(gr.at[pl.ds(0, Z - 1)], rsem.at[E_G2])

    g2t = gr[...].reshape(Z * S, LANES).T
    for yb in range(Y):
        part = dot(g2t, af[yb, :, y].reshape(Z * S, CB))
        dp[yb] = part.T.reshape(X, C, S, LANES)
    send(dp.at[:, :, 1 - c], rc, ssem.at[E_DC], rsem.at[E_DC], partner)
    arrived(rc, rsem.at[E_DC])
    rc[...] = rc[...] + dp[:, :, c]
    for d in range(1, X):
        xq = (x + d) % X
        send(rc.at[:, xq], rx.at[x], ssem.at[E_DX], rsem.at[E_DX], at_x(xq))
    rx[x] = rc[:, x]
    arrived(rx.at[pl.ds(0, X - 1)], rsem.at[E_DX])
    acc = rx[0]
    for k in range(1, X):
        acc = acc + rx[k]
    rx[x] = acc
    for d in range(1, Y):
        yq = (y + d) % Y
        send(rx.at[x, yq], ry.at[y], ssem.at[E_DY], rsem.at[E_DY], at_y(yq))
    ry[y] = rx[x, y]
    arrived(ry.at[pl.ds(0, Y - 1)], rsem.at[E_DY])
    acc = ry[0]
    for k in range(1, Y):
        acc = acc + ry[k]
    dy2 = acc.astype(BF)

    for yb in range(Y):
        for v in range(2):
            col = yb * HB + v * HU
            dh = dot(dy2, w2t[:, col:col + HU])
            g1[yb, v] = jnp.where(z1[:, col:col + HU] > 0.0, dh, 0.0).astype(BF)
    for v in range(2):
        for d in range(1, Y):
            yq = (y + d) % Y
            send(g1.at[yq, v], gz.at[v, z, y], ssem.at[E_G1], rsem_x.at[v, 0], at_y(yq))
        gz[v, z, y] = g1[y, v]
    mark = (lax.broadcasted_iota(jnp.int32, (HB, LANES), 0) == 0) & (lax.broadcasted_iota(jnp.int32, (HB, LANES), 1) == NC)
    for k in range(Y):
        part = lax.dot_general(h1[:, k * HB:(k + 1) * HB], dy2, (((0,), (0,)), ((), ())), preferred_element_type=F32)
        if k == 0:
            part = jnp.where(mark, loss_part, part)
        per = HB // (Y * Z * 8)
        rows = part.reshape(per, Y, Z, 8, LANES)
        for m in range(per):
            q = k * per + m
            wb[q // X, q % X, pl.ds(0, Y)] = rows[m]
    for v in range(2):
        arrived(gz.at[v, 0, pl.ds(0, Y - 1)], rsem_x.at[v, 0])
    for t in range(1, half + 1):
        for v in range(2):
            for d in range(2):
                sgn = 1 if d == 0 else -1
                blk = (z - sgn * (t - 1) + Z) % Z
                if t > 1:
                    arrived(gz.at[v, 0], rsem_ag.at[v, d, t - 1])
                ref = gz.at[v, blk]
                if t == half:
                    ref = gz.at[v, blk, pl.ds(d * (Y // 2), Y // 2)]
                send(ref, ref, ssem.at[E_AG], rsem_ag.at[v, d, t], at_z((z + sgn + Z) % Z))
    for d in (1, 3):
        for k in range(1, Y):
            arrived(af.at[0, pl.ds(0, half), 0], rsem_f.at[d // 2, k - 1])

    def dy1_chunk(v):
        def body(q, u):
            yb = q * NCH // CB
            off = pl.multiple_of((q % (CB // NCH)) * NCH, NCH)
            dy[v, q // C, q % C] = dot(gt[...], af[yb, :, :, :, pl.ds(off, NCH)].reshape(Z * Y * S, NCH))
            return u
        return body

    for v in range(2):
        for d in range(2):
            arrived(gz.at[v, 0, pl.ds(0, Y // 2)], rsem_ag.at[v, d, half])
        for k in range(Z):
            gt[:, k * Y * S:(k + 1) * Y * S] = gz[v, k].reshape(Y * S, HU).T
        lax.fori_loop(0, X * C, dy1_chunk(v), 0)
        send(dy.at[v, :, 1 - c], rcy.at[v], ssem.at[E_RC0 + v], rsem.at[E_RC0 + v], partner)
    nxt, prv, opp = (x + 1) % X, (x + X - 1) % X, (x + 2) % X
    hh = HU // 2
    for v in range(2):
        arrived(rcy.at[v], rsem.at[E_RC0 + v])
        for k in range(X):
            rcy[v, k] = rcy[v, k] + dy[v, k, c]
        send(rcy.at[v, opp, pl.ds(0, hh)], rx1.at[v, 0], ssem.at[E_RX], rsem_x.at[v, 1], at_x(nxt))
        send(rcy.at[v, opp, pl.ds(hh, hh)], rx1.at[v, 1], ssem.at[E_RX], rsem_x.at[v, 2], at_x(prv))
    for v in range(2):
        arrived(rx1.at[v, 0], rsem_x.at[v, 1])
        rcy[v, nxt, pl.ds(0, hh)] = rcy[v, nxt, pl.ds(0, hh)] + rx1[v, 0]
        send(rcy.at[v, nxt], rx2.at[v, 0], ssem.at[E_RX2], rsem_x.at[v, 3], at_x(nxt))
        arrived(rx1.at[v, 1], rsem_x.at[v, 2])
        rcy[v, prv, pl.ds(hh, hh)] = rcy[v, prv, pl.ds(hh, hh)] + rx1[v, 1]
        send(rcy.at[v, prv], rx2.at[v, 1], ssem.at[E_RX2], rsem_x.at[v, 4], at_x(prv))
    xn = xp[pl.ds(nid * Y, Y)].reshape(NCH, LANES)
    for v in range(2):
        arrived(rx2.at[v, 0], rsem_x.at[v, 3])
        arrived(rx2.at[v, 1], rsem_x.at[v, 4])
        acc = rcy[v, x] + rx2[v, 0] + rx2[v, 1]
        part = dot(acc.astype(BF), xn)
        per = HU // (Z * 8)
        rows = part.reshape(per, Z, 8, LANES)
        for m in range(per):
            q = v * per + m
            wb[q // X, q % X, Y] = rows[m]

    send(wb.at[1 - c], rwc, ssem.at[E_WC], rsem.at[E_WC], partner)
    arrived(rwc, rsem.at[E_WC])
    rwc[...] = rwc[...] + wb[c]
    for d in range(1, X):
        xq = (x + d) % X
        send(rwc.at[xq], rwx.at[x], ssem.at[E_WX], rsem.at[E_WX], at_x(xq))
    rwx[x] = rwc[x]
    arrived(rwx.at[pl.ds(0, X - 1)], rsem.at[E_WX])
    acc = rwx[0]
    for k in range(1, X):
        acc = acc + rwx[k]
    rwx[x] = acc
    for d in range(1, Y):
        yq = (y + d) % Y
        send(rwx.at[x, yq], rwy.at[y], ssem.at[E_WY], rsem.at[E_WY], at_y(yq))
    rwy[y] = rwx[x, y]
    sy[:, 1] = rwx[x, Y]
    arrived(rwy.at[pl.ds(0, Y - 1)], rsem.at[E_WY])
    acc = rwy[0]
    for k in range(1, Y):
        acc = acc + rwy[k]
    sy[:, 0] = acc
    for d in range(1, Z):
        zq = (z + d) % Z
        send(sy.at[zq], rwz.at[z], ssem.at[E_WZ], rsem.at[E_WZ], at_z(zq))
    rwz[z] = sy[z]
    arrived(rwz.at[pl.ds(0, Z - 1)], rsem.at[E_WZ])
    acc = rwz[0]
    for k in range(1, Z):
        acc = acc + rwz[k]
    fz[...] = acc
    for d in range(1, Z):
        zq = (z + d) % Z
        send(fz, oz.at[z], ssem.at[E_OZ], rsem.at[E_OZ], at_z(zq))
    oz[z] = fz[...]
    arrived(oz.at[pl.ds(0, Z - 1)], rsem.at[E_OZ])
    for d in range(1, Y):
        yq = (y + d) % Y
        send(oz, oy.at[y], ssem.at[E_OY], rsem.at[E_OY], at_y(yq))
    oy[y] = oz[...]
    arrived(oy.at[pl.ds(0, Y - 1)], rsem.at[E_OY])
    for d in range(1, X):
        xq = (x + d) % X
        send(oy, ox.at[x], ssem.at[E_OX], rsem.at[E_OX], at_x(xq))
    ox[x] = oy[...]
    arrived(ox.at[pl.ds(0, X - 1)], rsem.at[E_OX])
    send(ox, oc.at[c], ssem.at[E_OC], rsem.at[E_OC], partner)
    oc[c] = ox[...]
    arrived(oc.at[0], rsem.at[E_OC])

    for k in range(C):
        full = oc[k, :, :, :, 0].reshape(H // C, LANES)
        dw2_out[k * (H // C):(k + 1) * (H // C), :] = full[:, 0:NC]
        if k == 0:
            loss_out[...] = jnp.broadcast_to(full[0:1, NC:NC + 1] / count, (8, LANES))
    for yb in range(Y):
        part = oc[:, :, yb, :, 1].reshape(HB, LANES).T
        dw1_out[:, yb * HB:(yb + 1) * HB] = part[0:F]

    sent(xp.at[pl.ds(0, NP - 1)], ssem.at[E_X])
    sent(af.at[pl.ds(0, Y - 1), :, 0], ssem.at[E_A])
    sent(af.at[pl.ds(0, Y - 1), :, pl.ds(0, 2)], ssem.at[E_B])
    sent(af.at[pl.ds(0, Y - 1), :, 0], ssem.at[E_F])
    sent(sb, ssem.at[E_RING])
    sent(cr.at[pl.ds(0, Z - 1)], ssem.at[E_CNT])
    sent(yp.at[pl.ds(0, NP - 1)], ssem.at[E_Y2])
    sent(zr.at[pl.ds(0, Z - 1)], ssem.at[E_Z2])
    sent(gr.at[pl.ds(0, Z - 1)], ssem.at[E_G2])
    sent(rc, ssem.at[E_DC])
    sent(rx.at[pl.ds(0, X - 1)], ssem.at[E_DX])
    sent(ry.at[pl.ds(0, Y - 1)], ssem.at[E_DY])
    sent(g1.at[pl.ds(0, Y - 1)], ssem.at[E_G1])
    sent(gz.at[:, pl.ds(0, Z - 1)], ssem.at[E_AG])
    sent(rcy.at[0], ssem.at[E_RC0])
    sent(rcy.at[1], ssem.at[E_RC1])
    sent(rx1, ssem.at[E_RX])
    sent(rx2, ssem.at[E_RX2])
    sent(rwc, ssem.at[E_WC])
    sent(rwx.at[pl.ds(0, X - 1)], ssem.at[E_WX])
    sent(rwy.at[pl.ds(0, Y - 1)], ssem.at[E_WY])
    sent(rwz.at[pl.ds(0, Z - 1)], ssem.at[E_WZ])
    sent(oz.at[pl.ds(0, Z - 1)], ssem.at[E_OZ])
    sent(oy.at[pl.ds(0, Y - 1)], ssem.at[E_OY])
    sent(ox.at[pl.ds(0, X - 1)], ssem.at[E_OX])
    sent(oc.at[0], ssem.at[E_OC])


def solution(mesh):
    Y, X, C = Y_DIM, X_DIM, CORES
    Z = mesh.shape["rep"] // Y
    row_spec = P(("rep", "nodes"))

    def device_step(adj_blk, feat_blk, w_one, w_two, label_blk, mask_blk):
        R, S, CB = adj_blk.shape
        F, H = w_one.shape
        NC = w_two.shape[1]
        I = X * C
        NP = Y * I
        HR = H // (2 * NSUB)
        HB = H // Y
        HU = HB // 2
        NCH = Y * S
        assert R == Z * Y and CB == S * I and F < LANES and NC < LANES
        xs = jnp.concatenate([feat_blk, mask_blk[:, None].astype(BF), jnp.zeros((S, LANES - F - 1), BF)], axis=1)
        w1 = jnp.pad(w_one, ((0, LANES - F), (0, 0))).astype(BF)
        w2 = jnp.pad(w_two, ((0, 0), (0, LANES - NC))).astype(BF)
        vm = pltpu.VMEM
        dma = pltpu.SemaphoreType.DMA
        scratch = [
            vm((Y, Z, Y, S, CB), BF),
            vm((NP, S, LANES), BF),
            vm((Y * CB, H), BF),
            vm((8, LANES), F32),
            vm((Z, 8, LANES), F32),
            vm((2 * NSUB, Z - 1, S, HR), F32),
            vm((2 * NSUB, Z - 1, S, HR), F32),
            vm((S, H), F32),
            vm((S, H), BF),
            vm((S, LANES), BF),
            vm((NP, S, LANES), BF),
            vm((Z, S, LANES), F32),
            vm((Z, S, LANES), F32),
            vm((S, LANES), BF),
            vm((Z, S, LANES), BF),
            vm((Y, X, C, S, LANES), F32),
            vm((Y, X, S, LANES), F32),
            vm((X, Y, S, LANES), F32),
            vm((Y, S, LANES), F32),
            vm((Y, 2, S, HU), BF),
            vm((2, Z, Y, S, HU), BF),
            vm((HU, Z * Y * S), BF),
            vm((2, X, C, HU, NCH), F32),
            vm((2, X, HU, NCH), F32),
            vm((2, 2, HU // 2, NCH), F32),
            vm((2, 2, HU, NCH), F32),
            vm((C, X, Y + 1, Z, 8, LANES), F32),
            vm((X, Y + 1, Z, 8, LANES), F32),
            vm((X, Y + 1, Z, 8, LANES), F32),
            vm((Y, Z, 8, LANES), F32),
            vm((Z, 2, 8, LANES), F32),
            vm((Z, 2, 8, LANES), F32),
            vm((2, 8, LANES), F32),
            vm((Z, 2, 8, LANES), F32),
            vm((Y, Z, 2, 8, LANES), F32),
            vm((X, Y, Z, 2, 8, LANES), F32),
            vm((C, X, Y, Z, 2, 8, LANES), F32),
            dma((27,)),
            dma((25,)),
            dma((Y - 1, Z)),
            dma((2, Y - 1)),
            dma((2, Y - 1)),
            dma((2 * NSUB, Z - 1)),
            dma((2, 2, Z // 2 + 1)),
            dma((2, 5)),
        ]
        vspec = pl.BlockSpec(memory_space=pltpu.VMEM)
        dw_one, dw_two, loss = pl.pallas_call(
            functools.partial(_step, (Z, Y, X, C, S, CB, H, F, NC)),
            out_shape=(jax.ShapeDtypeStruct((F, H), F32), jax.ShapeDtypeStruct((H, NC), F32), jax.ShapeDtypeStruct((8, LANES), F32)),
            in_specs=[pl.BlockSpec(memory_space=pl.ANY)] + [vspec] * 5,
            out_specs=(vspec, vspec, vspec),
            scratch_shapes=scratch,
            compiler_params=pltpu.CompilerParams(collective_id=0, has_side_effects=True, vmem_limit_bytes=60 * 1024 * 1024),
            name="gcn_step",
        )(adj_blk.reshape(Z, Y, S, CB), xs, label_blk[:, None], w1, w2, w2.T)
        return loss[0, 0], dw_one, dw_two

    return jax.shard_map(device_step, mesh=mesh, in_specs=(P(None, "nodes", "rep"), row_spec, P(), P(), row_spec, row_spec), out_specs=(P(), P(), P()), check_vma=False)
```

```python
import functools

import jax
import jax.numpy as jnp
from jax import lax
from jax.experimental import pallas as pl
from jax.experimental.pallas import tpu as pltpu
from jax.sharding import PartitionSpec as P

Y_DIM = 4
X_DIM = 4
CORES = 2
LANES = 128
NSUB = 2
NV = 4
NSEM = 36
BF = jnp.bfloat16
F32 = jnp.float32


def _step(dims, a_hbm, feat, lab, msk, w_one, w_two, dw1_out, dw2_out, loss_out,
          af, mt, mtt, w1f, w2f, w1, w2, w2t, xs, xp, y1, cs, cr, sb, rb, z1, h1, y2, yp, zp, zr, g2, gr, dp, rc, rx, ry,
          g1, gz, gt, dy, rcy, rx1, rx2, wb, wc, wx, wy, wz, wf, oz, oy, ox, oc, pb, pc, px, pz, pf, qz, qy, qx,
          ssem, rsem, rsem_a, rsem_b, rsem_f, rsem_ring, rsem_g, rsem_ag, rsem_c, rsem_x):
    Z, Y, X, C, S, CB, H, F, NC = dims
    I = X * C
    NQ = Y * X
    HR = H // (2 * NSUB)
    HB = H // Y
    HU = HB // NV
    NCH = Y * S
    half = Z // 2
    rid = lax.axis_index("rep")
    nid = lax.axis_index("nodes")
    z, y, x, c = rid // Y, rid % Y, nid // C, nid % C
    chip = y * X + x
    partner = (rid, x * C + 1 - c)

    def at_z(zz):
        return (zz * Y + y, nid)

    def at_y(yy):
        return (z * Y + yy, nid)

    def at_x(xx):
        return (rid, xx * C + c)

    def at_chip(q):
        return (z * Y + q // X, (q % X) * C + c)

    def send(src, dst, ss, rs, dev):
        pltpu.make_async_remote_copy(src_ref=src, dst_ref=dst, send_sem=ss, recv_sem=rs, device_id=dev,
                                     device_id_type=pl.DeviceIdType.MESH).start()

    def arrived(ref, rs):
        pltpu.make_async_remote_copy(src_ref=ref, dst_ref=ref, send_sem=ssem.at[0], recv_sem=rs, device_id=partner,
                                     device_id_type=pl.DeviceIdType.MESH).wait_recv()

    def sent(ref, ss):
        pltpu.make_async_remote_copy(src_ref=ref, dst_ref=ref, send_sem=ss, recv_sem=rsem.at[0], device_id=partner,
                                     device_id_type=pl.DeviceIdType.MESH).wait_send()

    def dot(a, b):
        return jnp.dot(a, b, preferred_element_type=F32)

    def most(ref):
        return ref.at[0, pl.ds(0, NQ - 1)]

    def plane_rows(ref, yb):
        return jnp.stack([ref[k, yb * X:(yb + 1) * X] for k in range(C)], axis=1).reshape(CB, LANES)

    def added(ref, n):
        acc = ref[0]
        for k in range(1, n):
            acc = acc + ref[k]
        return acc

    (E_X, E_XC, E_A, E_B, E_F, E_RING, E_CNT, E_Y2, E_Y2C, E_Z2, E_G2, E_DC, E_DX, E_DY, E_G1, E_AG, E_RC, E_RX, E_RX2,
     E_WC, E_WX, E_WY, E_WZ, E_OZ, E_OY, E_OX, E_OC, E_PC, E_PX, E_PZ, E_QZ, E_QY, E_QX, E_LA, E_L1, E_L2) = range(NSEM)

    load_a = pltpu.make_async_copy(a_hbm, af.at[y], ssem.at[E_LA])
    load_1 = pltpu.make_async_copy(w_one, w1f, ssem.at[E_L1])
    load_2 = pltpu.make_async_copy(w_two, w2f, ssem.at[E_L2])
    load_a.start()
    load_1.start()
    load_2.start()

    bar = pltpu.get_barrier_semaphore()
    for d in range(1, Z):
        pl.semaphore_signal(bar, inc=1, device_id=at_z((z + d) % Z), device_id_type=pl.DeviceIdType.MESH)

    def greet_plane(d, u):
        pl.semaphore_signal(bar, inc=1, device_id=at_chip(lax.rem(chip + d, NQ)), device_id_type=pl.DeviceIdType.MESH)
        return u

    lax.fori_loop(1, NQ, greet_plane, 0)
    pl.semaphore_signal(bar, inc=1, device_id=partner, device_id_type=pl.DeviceIdType.MESH)

    mt[...] = jnp.zeros_like(mt)
    mt[0:F] = feat[...].astype(F32)
    mt[F:F + 1] = msk[...].astype(F32)
    mt[F + 1:F + 2] = lab[...].astype(F32)
    mtt[...] = mt[...].T
    xs[...] = mtt[...].astype(BF)
    pl.semaphore_wait(bar, NQ + Z - 1)

    def send_x(d, u):
        q = lax.rem(chip + d, NQ)
        send(xs, xp.at[c, chip], ssem.at[E_X], rsem.at[E_X], at_chip(q))
        return u

    lax.fori_loop(1, NQ, send_x, 0)
    xp[c, chip] = xs[...]
    load_a.wait()

    order = []
    for k in range(1, half + 1):
        order.append(-k)
        if k < half:
            order.append(k)
    order.append(0)
    for k in order:
        zc = (z + k + Z) % Z
        for d in (1, 3, 2):
            yq = (y + d) % Y
            send(af.at[y, zc, yq], af.at[y, zc, yq], ssem.at[E_A], rsem_a.at[d - 1, zc], at_y(yq))
    for d in (1, 3):
        yq = (y + d) % Y
        for k in range(1, Y):
            ya = (yq + k) % Y
            send(af.at[y, :, ya], af.at[y, :, ya], ssem.at[E_B], rsem_b.at[d // 2, k - 1], at_y(yq))

    load_1.wait()
    w1[...] = jnp.zeros_like(w1)
    w1[0:F] = w1f[...].astype(BF)
    load_2.wait()
    w2[...] = jnp.zeros_like(w2)
    for k in range(Y):
        rows = slice(k * HB, (k + 1) * HB)
        w2[rows, 0:NC] = w2f[rows].astype(BF)
        w2t[:, rows] = w2[rows].T

    arrived(most(xp), rsem.at[E_X])
    send(xp.at[c], xp.at[c], ssem.at[E_XC], rsem.at[E_XC], partner)
    arrived(xp.at[0], rsem.at[E_XC])

    def wait_a(zc):
        for d in range(1, Y):
            arrived(af.at[0, 0, 0], rsem_a.at[d - 1, zc])

    def ring(t, u):
        s, j = t // (2 * NSUB), t % (2 * NSUB)
        up = j < NSUB
        dest = lax.rem(jnp.where(up, z - 1 - s, z + 1 + s) + 2 * Z, Z)
        nb = lax.rem(jnp.where(up, z + 1, z - 1) + Z, Z)
        col = pl.multiple_of(j * HR, HR)
        fresh = ((j == 0) & ((s < half) | (s == Z - 1))) | ((j == NSUB) & (s < half - 1))

        @pl.when(s == 0)
        def _():
            for yb in range(Y):
                rows = plane_rows(xp, yb)
                y1[yb * CB:(yb + 1) * CB, pl.ds(col, HR)] = dot(rows, w1[:, pl.ds(col, HR)]).astype(BF)

        @pl.when(fresh)
        def _():
            wait_a(dest)

        acc = dot(af[0, dest, y], y1[pl.ds(0, CB), pl.ds(col, HR)])
        for yb in range(1, Y):
            acc = acc + dot(af[yb, dest, y], y1[pl.ds(yb * CB, CB), pl.ds(col, HR)])
        z1[:, pl.ds(col, HR)] = acc

        @pl.when(s > 0)
        def _():
            prev = jnp.maximum(s - 1, 0)
            arrived(rb.at[0, 0], rsem_ring.at[j, prev])
            z1[:, pl.ds(col, HR)] = z1[:, pl.ds(col, HR)] + rb[j, prev]

        @pl.when(s < Z - 1)
        def _():
            here = jnp.minimum(s, Z - 2)
            sb[j, here] = z1[:, pl.ds(col, HR)]
            send(sb.at[j, here], rb.at[j, here], ssem.at[E_RING], rsem_ring.at[j, here], at_z(nb))

        return u

    lax.fori_loop(0, Z * 2 * NSUB, ring, 0)

    h1[...] = jnp.maximum(z1[...], 0.0).astype(BF)
    y2[...] = dot(h1[...], w2[...]).astype(BF)

    def send_y2(d, u):
        q = lax.rem(chip + d, NQ)
        send(y2, yp.at[c, chip], ssem.at[E_Y2], rsem.at[E_Y2], at_chip(q))
        return u

    lax.fori_loop(1, NQ, send_y2, 0)
    yp[c, chip] = y2[...]
    lane = lax.broadcasted_iota(jnp.int32, (S, LANES), 1)
    counted = jnp.sum(xp[...].astype(F32).reshape(Y * CB, LANES), axis=0, keepdims=True)
    counted = jnp.sum(jnp.where(lane[0:1] == F, counted, 0.0), axis=1, keepdims=True)
    cs[...] = jnp.broadcast_to(counted, (8, LANES))
    cr[z] = cs[...]
    for d in range(1, Z):
        send(cs, cr.at[z], ssem.at[E_CNT], rsem.at[E_CNT], at_z((z + d) % Z))
    arrived(most(yp), rsem.at[E_Y2])
    send(yp.at[c], yp.at[c], ssem.at[E_Y2C], rsem.at[E_Y2C], partner)
    arrived(yp.at[0], rsem.at[E_Y2C])
    for yb in range(Y):
        part = dot(af[yb, :, y].reshape(Z * S, CB), plane_rows(yp, yb)).reshape(Z, S, LANES)
        zp[...] = part if yb == 0 else zp[...] + part
    for d in range(1, Z):
        zq = (z + d) % Z
        send(zp.at[zq], zr.at[z], ssem.at[E_Z2], rsem.at[E_Z2], at_z(zq))
    zr[z] = zp[z]
    for d in (1, 3):
        for k in range(1, Y):
            arrived(af.at[0, :, 0], rsem_b.at[d // 2, k - 1])
    for d in (1, 3):
        ys, yq = (y - d + Y) % Y, (y + d) % Y
        lo = 0 if d == 1 else half
        for k in range(1, Y):
            ya = (yq + k) % Y
            send(af.at[ys, pl.ds(lo, half), ya], af.at[ys, pl.ds(lo, half), ya], ssem.at[E_F], rsem_f.at[d // 2, k - 1], at_y(yq))
    arrived(zr.at[pl.ds(0, Z - 1)], rsem.at[E_Z2])
    z2 = added(zr, Z)

    arrived(cr.at[pl.ds(0, Z - 1)], rsem.at[E_CNT])
    count = added(cr, Z)[0:1, 0:1]
    own = mtt[...]
    weights = jnp.sum(jnp.where(lane == F, own, 0.0), axis=1, keepdims=True)
    labels = jnp.sum(jnp.where(lane == F + 1, own, 0.0), axis=1, keepdims=True)
    real = lane < NC
    top = jnp.max(jnp.where(real, z2, -jnp.inf), axis=1, keepdims=True)
    shifted = jnp.where(real, z2 - top, 0.0)
    log_probs = shifted - jnp.log(jnp.sum(jnp.where(real, jnp.exp(shifted), 0.0), axis=1, keepdims=True))
    hot = labels == lane.astype(F32)
    picked = jnp.sum(jnp.where(hot, log_probs, 0.0), axis=1, keepdims=True)
    loss_part = -jnp.sum(weights * picked, axis=0, keepdims=True)
    diff = jnp.where(real, jnp.exp(log_probs), 0.0) - hot.astype(F32)
    g2[...] = (diff * (weights / count)).astype(BF)
    for d in range(1, Z):
        send(g2, gr.at[z], ssem.at[E_G2], rsem.at[E_G2], at_z((z + d) % Z))
    gr[z] = g2[...]
    arrived(gr.at[pl.ds(0, Z - 1)], rsem.at[E_G2])

    g2t = gr[...].reshape(Z * S, LANES).T
    for yb in range(Y):
        part = dot(g2t, af[yb, :, y].reshape(Z * S, CB))
        dp[yb] = part.T.reshape(X, C, S, LANES)
    send(dp.at[:, :, 1 - c], rc, ssem.at[E_DC], rsem.at[E_DC], partner)
    arrived(rc, rsem.at[E_DC])
    rc[...] = rc[...] + dp[:, :, c]
    for d in range(1, X):
        xq = (x + d) % X
        send(rc.at[:, xq], rx.at[x], ssem.at[E_DX], rsem.at[E_DX], at_x(xq))
    rx[x] = rc[:, x]
    arrived(rx.at[pl.ds(0, X - 1)], rsem.at[E_DX])
    rx[x] = added(rx, X)
    for d in range(1, Y):
        yq = (y + d) % Y
        send(rx.at[x, yq], ry.at[y], ssem.at[E_DY], rsem.at[E_DY], at_y(yq))
    ry[y] = rx[x, y]
    arrived(ry.at[pl.ds(0, Y - 1)], rsem.at[E_DY])
    dy2 = added(ry, Y).astype(BF)

    for v in range(NV):
        for yb in range(Y):
            col = yb * HB + v * HU
            dh = dot(dy2, w2t[:, col:col + HU])
            g1[yb, v] = jnp.where(z1[:, col:col + HU] > 0.0, dh, 0.0).astype(BF)
        for d in (1, 3, 2):
            yq = (y + d) % Y
            send(g1.at[yq, v], gz.at[v, z, y], ssem.at[E_G1], rsem_g.at[v], at_y(yq))
        gz[v, z, y] = g1[y, v]

    def gather_step(v, t):
        if t == 1:
            arrived(gz.at[v, 0, pl.ds(0, Y - 1)], rsem_g.at[v])
        for d in range(2):
            sgn = 1 if d == 0 else -1
            blk = (z - sgn * (t - 1) + Z) % Z
            if t > 1:
                arrived(gz.at[v, 0], rsem_ag.at[v, d, t - 1])
            ref = gz.at[v, blk] if t < half else gz.at[v, blk, pl.ds(d * (Y // 2), Y // 2)]
            send(ref, ref, ssem.at[E_AG], rsem_ag.at[v, d, t], at_z((z + sgn + Z) % Z))

    def product(v):
        for d in range(2):
            arrived(gz.at[v, 0, pl.ds(0, Y // 2)], rsem_ag.at[v, d, half])
        for k in range(Z):
            gt[v, :, k * Y * S:(k + 1) * Y * S] = gz[v, k].reshape(Y * S, HU).T

        def chunk(q, u):
            yb = q * NCH // CB
            off = pl.multiple_of((q % (CB // NCH)) * NCH, NCH)
            dy[v, q // C, q % C] = dot(gt[v], af[yb, :, :, :, pl.ds(off, NCH)].reshape(Z * Y * S, NCH))
            return u

        lax.fori_loop(0, X * C, chunk, 0)
        send(dy.at[v, :, 1 - c], rcy.at[v], ssem.at[E_RC], rsem_c.at[v], partner)

    nxt, prv, opp = (x + 1) % X, (x + X - 1) % X, (x + 2) % X
    hh = HU // 2

    def reduce_core(v):
        arrived(rcy.at[v], rsem_c.at[v])
        for k in range(X):
            rcy[v, k] = rcy[v, k] + dy[v, k, c]
        send(rcy.at[v, opp, pl.ds(0, hh)], rx1.at[v, 0], ssem.at[E_RX], rsem_x.at[v, 0], at_x(nxt))
        send(rcy.at[v, opp, pl.ds(hh, hh)], rx1.at[v, 1], ssem.at[E_RX], rsem_x.at[v, 1], at_x(prv))

    def reduce_x(v):
        arrived(rx1.at[v, 0], rsem_x.at[v, 0])
        rcy[v, nxt, pl.ds(0, hh)] = rcy[v, nxt, pl.ds(0, hh)] + rx1[v, 0]
        send(rcy.at[v, nxt], rx2.at[v, 0], ssem.at[E_RX2], rsem_x.at[v, 2], at_x(nxt))
        arrived(rx1.at[v, 1], rsem_x.at[v, 1])
        rcy[v, prv, pl.ds(hh, hh)] = rcy[v, prv, pl.ds(hh, hh)] + rx1[v, 1]
        send(rcy.at[v, prv], rx2.at[v, 1], ssem.at[E_RX2], rsem_x.at[v, 3], at_x(prv))

    def own_x():
        return jnp.concatenate([xp[m % C, nid * (Y // C) + m // C] for m in range(Y)], axis=0)

    def grad_one(v):
        arrived(rx2.at[v, 0], rsem_x.at[v, 2])
        arrived(rx2.at[v, 1], rsem_x.at[v, 3])
        acc = (rcy[v, x] + rx2[v, 0] + rx2[v, 1]).astype(BF)
        part = dot(acc, own_x())
        if v >= NV // 2:
            part = jnp.concatenate([part[:, LANES // 2:], part[:, 0:LANES // 2]], axis=1)
        per = HU // (Z * 8)
        rows = part.reshape(per, Z, 8, LANES)
        for m in range(per):
            k = (v % (NV // 2)) * per + m
            pb[k] = rows[m] if v < NV // 2 else pb[k] + rows[m]

    def w_begin():
        mark = (lax.broadcasted_iota(jnp.int32, (HB, LANES), 0) == 0) & (lax.broadcasted_iota(jnp.int32, (HB, LANES), 1) == NC)
        for k in range(Y):
            part = lax.dot_general(h1[:, k * HB:(k + 1) * HB], dy2, (((0,), (0,)), ((), ())), preferred_element_type=F32)
            if k == 0:
                part = jnp.where(mark, loss_part, part)
            per = HB // (Y * Z * 8)
            rows = part.reshape(per, Y, Z, 8, LANES)
            for m in range(per):
                q = k * per + m
                wb[q // X, q % X] = rows[m]
        send(wb.at[1 - c], wc, ssem.at[E_WC], rsem.at[E_WC], partner)

    def w_core():
        arrived(wc, rsem.at[E_WC])
        wc[...] = wc[...] + wb[c]
        for d in (1, 3, 2):
            xq = (x + d) % X
            send(wc.at[xq], wx.at[x], ssem.at[E_WX], rsem.at[E_WX], at_x(xq))
        wx[x] = wc[x]

    def w_x():
        arrived(wx.at[pl.ds(0, X - 1)], rsem.at[E_WX])
        wx[x] = added(wx, X)
        for d in (1, 3, 2):
            yq = (y + d) % Y
            send(wx.at[x, yq], wy.at[y], ssem.at[E_WY], rsem.at[E_WY], at_y(yq))
        wy[y] = wx[x, y]

    def w_y():
        arrived(wy.at[pl.ds(0, Y - 1)], rsem.at[E_WY])
        wy[y] = added(wy, Y)
        for d in range(1, Z):
            zq = (z + d) % Z
            send(wy.at[y, zq], wz.at[z], ssem.at[E_WZ], rsem.at[E_WZ], at_z(zq))
        wz[z] = wy[y, z]

    def w_z():
        arrived(wz.at[pl.ds(0, Z - 1)], rsem.at[E_WZ])
        wf[...] = added(wz, Z)
        for d in range(1, Z):
            send(wf, oz.at[z], ssem.at[E_OZ], rsem.at[E_OZ], at_z((z + d) % Z))
        oz[z] = wf[...]

    def o_z():
        arrived(oz.at[pl.ds(0, Z - 1)], rsem.at[E_OZ])
        for d in (1, 3, 2):
            send(oz, oy.at[y], ssem.at[E_OY], rsem.at[E_OY], at_y((y + d) % Y))
        oy[y] = oz[...]

    def o_y():
        arrived(oy.at[pl.ds(0, Y - 1)], rsem.at[E_OY])
        for d in (1, 3, 2):
            send(oy, ox.at[x], ssem.at[E_OX], rsem.at[E_OX], at_x((x + d) % X))
        ox[x] = oy[...]

    def o_x():
        arrived(ox.at[pl.ds(0, X - 1)], rsem.at[E_OX])
        send(ox, oc.at[c], ssem.at[E_OC], rsem.at[E_OC], partner)
        oc[c] = ox[...]

    gather_step(0, 1)
    w_begin()
    for r in range(1, NV + half - 1):
        for v in range(NV):
            t = r - v + 1
            if 1 <= t <= half:
                gather_step(v, t)
        if r == 1:
            w_core()
        if r == half:
            w_x()
            for d in (1, 3):
                for k in range(1, Y):
                    arrived(af.at[0, pl.ds(0, half), 0], rsem_f.at[d // 2, k - 1])
        v = r - half
        if v >= 0:
            product(v)
        if v >= 1:
            reduce_core(v - 1)
        if v >= 2:
            reduce_x(v - 2)
        if r == half + 1:
            w_y()
    product(NV - 1)
    reduce_core(NV - 2)
    reduce_x(NV - 3)
    reduce_core(NV - 1)
    w_z()
    reduce_x(NV - 2)
    for v in range(NV - 2):
        grad_one(v)
    reduce_x(NV - 1)
    o_z()
    grad_one(NV - 2)
    grad_one(NV - 1)

    send(pb, pc, ssem.at[E_PC], rsem.at[E_PC], partner)
    arrived(pc, rsem.at[E_PC])
    pc[...] = pc[...] + pb[...]
    for d in (1, 3, 2):
        xq = (x + d) % X
        send(pc.at[xq], px.at[x], ssem.at[E_PX], rsem.at[E_PX], at_x(xq))
    px[x] = pc[x]
    o_y()
    arrived(px.at[pl.ds(0, X - 1)], rsem.at[E_PX])
    px[x] = added(px, X)
    for d in range(1, Z):
        zq = (z + d) % Z
        send(px.at[x, zq], pz.at[z], ssem.at[E_PZ], rsem.at[E_PZ], at_z(zq))
    pz[z] = px[x, z]
    arrived(pz.at[pl.ds(0, Z - 1)], rsem.at[E_PZ])
    pf[...] = added(pz, Z)
    for d in range(1, Z):
        send(pf, qz.at[z], ssem.at[E_QZ], rsem.at[E_QZ], at_z((z + d) % Z))
    qz[z] = pf[...]
    o_x()
    arrived(qz.at[pl.ds(0, Z - 1)], rsem.at[E_QZ])
    for d in (1, 3, 2):
        send(qz, qy.at[y], ssem.at[E_QY], rsem.at[E_QY], at_y((y + d) % Y))
    qy[y] = qz[...]
    arrived(oc.at[0], rsem.at[E_OC])
    for k in range(C):
        full = oc[k].reshape(H // C, LANES)
        dw2_out[k * (H // C):(k + 1) * (H // C), :] = full[:, 0:NC]
        if k == 0:
            loss_out[...] = jnp.broadcast_to(full[0:1, NC:NC + 1] / count, (8, LANES))
    arrived(qy.at[pl.ds(0, Y - 1)], rsem.at[E_QY])
    for d in (1, 3, 2):
        send(qy, qx.at[x], ssem.at[E_QX], rsem.at[E_QX], at_x((x + d) % X))
    qx[x] = qy[...]
    arrived(qx.at[pl.ds(0, X - 1)], rsem.at[E_QX])
    for yb in range(Y):
        part = qx[:, yb].reshape(HB // 2, LANES).T
        dw1_out[:, yb * HB:yb * HB + HB // 2] = part[0:F]
        dw1_out[:, yb * HB + HB // 2:(yb + 1) * HB] = part[LANES // 2:LANES // 2 + F]

    sent(most(xp), ssem.at[E_X])
    sent(xp.at[0], ssem.at[E_XC])
    sent(af.at[pl.ds(0, Y - 1), :, 0], ssem.at[E_A])
    sent(af.at[pl.ds(0, Y - 1), :, pl.ds(0, 2)], ssem.at[E_B])
    sent(af.at[pl.ds(0, Y - 1), :, 0], ssem.at[E_F])
    sent(sb, ssem.at[E_RING])
    sent(cr.at[pl.ds(0, Z - 1)], ssem.at[E_CNT])
    sent(most(yp), ssem.at[E_Y2])
    sent(yp.at[0], ssem.at[E_Y2C])
    sent(zr.at[pl.ds(0, Z - 1)], ssem.at[E_Z2])
    sent(gr.at[pl.ds(0, Z - 1)], ssem.at[E_G2])
    sent(rc, ssem.at[E_DC])
    sent(rx.at[pl.ds(0, X - 1)], ssem.at[E_DX])
    sent(ry.at[pl.ds(0, Y - 1)], ssem.at[E_DY])
    sent(g1.at[pl.ds(0, Y - 1)], ssem.at[E_G1])
    sent(gz.at[:, pl.ds(0, Z - 1)], ssem.at[E_AG])
    sent(rcy, ssem.at[E_RC])
    sent(rx1, ssem.at[E_RX])
    sent(rx2, ssem.at[E_RX2])
    sent(wc, ssem.at[E_WC])
    sent(wx.at[pl.ds(0, X - 1)], ssem.at[E_WX])
    sent(wy.at[pl.ds(0, Y - 1)], ssem.at[E_WY])
    sent(wz.at[pl.ds(0, Z - 1)], ssem.at[E_WZ])
    sent(oz.at[pl.ds(0, Z - 1)], ssem.at[E_OZ])
    sent(oy.at[pl.ds(0, Y - 1)], ssem.at[E_OY])
    sent(ox.at[pl.ds(0, X - 1)], ssem.at[E_OX])
    sent(oc.at[0], ssem.at[E_OC])
    sent(pc, ssem.at[E_PC])
    sent(px.at[pl.ds(0, X - 1)], ssem.at[E_PX])
    sent(pz.at[pl.ds(0, Z - 1)], ssem.at[E_PZ])
    sent(qz.at[pl.ds(0, Z - 1)], ssem.at[E_QZ])
    sent(qy.at[pl.ds(0, Y - 1)], ssem.at[E_QY])
    sent(qx.at[pl.ds(0, X - 1)], ssem.at[E_QX])


def solution(mesh):
    Y, X, C = Y_DIM, X_DIM, CORES
    Z = mesh.shape["rep"] // Y
    row_spec = P(("rep", "nodes"))

    def device_step(adj_blk, feat_blk, w_one, w_two, label_blk, mask_blk):
        R, S, CB = adj_blk.shape
        F, H = w_one.shape
        NC = w_two.shape[1]
        I = X * C
        NQ = Y * X
        HR = H // (2 * NSUB)
        HB = H // Y
        HU = HB // NV
        NCH = Y * S
        assert R == Z * Y and CB == S * I and F + 2 <= LANES // 2 and NC < LANES
        vm = pltpu.VMEM
        dma = pltpu.SemaphoreType.DMA
        scratch = [
            vm((Y, Z, Y, S, CB), BF),
            vm((LANES, S), F32),
            vm((S, LANES), F32),
            vm((F, H), F32),
            vm((H, NC), F32),
            vm((LANES, H), BF),
            vm((H, LANES), BF),
            vm((LANES, H), BF),
            vm((S, LANES), BF),
            vm((C, NQ, S, LANES), BF),
            vm((Y * CB, H), BF),
            vm((8, LANES), F32),
            vm((Z, 8, LANES), F32),
            vm((2 * NSUB, Z - 1, S, HR), F32),
            vm((2 * NSUB, Z - 1, S, HR), F32),
            vm((S, H), F32),
            vm((S, H), BF),
            vm((S, LANES), BF),
            vm((C, NQ, S, LANES), BF),
            vm((Z, S, LANES), F32),
            vm((Z, S, LANES), F32),
            vm((S, LANES), BF),
            vm((Z, S, LANES), BF),
            vm((Y, X, C, S, LANES), F32),
            vm((Y, X, S, LANES), F32),
            vm((X, Y, S, LANES), F32),
            vm((Y, S, LANES), F32),
            vm((Y, NV, S, HU), BF),
            vm((NV, Z, Y, S, HU), BF),
            vm((NV, HU, Z * Y * S), BF),
            vm((NV, X, C, HU, NCH), F32),
            vm((NV, X, HU, NCH), F32),
            vm((NV, 2, HU // 2, NCH), F32),
            vm((NV, 2, HU, NCH), F32),
            vm((C, X, Y, Z, 8, LANES), F32),
            vm((X, Y, Z, 8, LANES), F32),
            vm((X, Y, Z, 8, LANES), F32),
            vm((Y, Z, 8, LANES), F32),
            vm((Z, 8, LANES), F32),
            vm((8, LANES), F32),
            vm((Z, 8, LANES), F32),
            vm((Y, Z, 8, LANES), F32),
            vm((X, Y, Z, 8, LANES), F32),
            vm((C, X, Y, Z, 8, LANES), F32),
            vm((X, Z, 8, LANES), F32),
            vm((X, Z, 8, LANES), F32),
            vm((X, Z, 8, LANES), F32),
            vm((Z, 8, LANES), F32),
            vm((8, LANES), F32),
            vm((Z, 8, LANES), F32),
            vm((Y, Z, 8, LANES), F32),
            vm((X, Y, Z, 8, LANES), F32),
            dma((NSEM,)),
            dma((NSEM,)),
            dma((Y - 1, Z)),
            dma((2, Y - 1)),
            dma((2, Y - 1)),
            dma((2 * NSUB, Z - 1)),
            dma((NV,)),
            dma((NV, 2, Z // 2 + 1)),
            dma((NV,)),
            dma((NV, 4)),
        ]
        vspec = pl.BlockSpec(memory_space=pltpu.VMEM)
        aspec = pl.BlockSpec(memory_space=pl.ANY)
        dw_one, dw_two, loss = pl.pallas_call(
            functools.partial(_step, (Z, Y, X, C, S, CB, H, F, NC)),
            out_shape=(jax.ShapeDtypeStruct((F, H), F32), jax.ShapeDtypeStruct((H, NC), F32), jax.ShapeDtypeStruct((8, LANES), F32)),
            in_specs=[aspec, vspec, vspec, vspec, aspec, aspec],
            out_specs=(vspec, vspec, vspec),
            scratch_shapes=scratch,
            compiler_params=pltpu.CompilerParams(collective_id=0, has_side_effects=True, vmem_limit_bytes=62 * 1024 * 1024),
            name="gcn_step",
        )(adj_blk.reshape(Z, Y, S, CB), feat_blk.T, label_blk[None, :], mask_blk[None, :], w_one, w_two)
        return loss[0, 0], dw_one, dw_two

    return jax.shard_map(device_step, mesh=mesh, in_specs=(P(None, "nodes", "rep"), row_spec, P(), P(), row_spec, row_spec), out_specs=(P(), P(), P()), check_vma=False)
```

```python
import functools

import jax
import jax.numpy as jnp
from jax import lax
from jax.experimental import pallas as pl
from jax.experimental.pallas import tpu as pltpu
from jax.sharding import PartitionSpec as P

Y_DIM = 4
X_DIM = 4
CORES = 2
LANES = 128
NSUB = 2
NV = 4
NSEM = 39
BF = jnp.bfloat16
F32 = jnp.float32


def _step(dims, a_hbm, feat, lab, msk, w_one, w_two, dw1_out, dw2_out, loss_out,
          af, mt, mtt, w1f, w2f, w1, w2, w2t, xs, xp, y1, cs, cr, sb, rb, z1, h1, y2, yp, zp, zr, g2, gr, dp, rc, rx, ry, ry2, rx2d,
          d2, dg, ms, mk, gz, gt, dy, rcy, rx1, rx2, wb, wc, wx, wy, wz, wf, oz, oy, ox, oc, pb, pc, px, pz, pf, qz, qy, qx,
          ssem, rsem, rsem_a, rsem_b, rsem_f, rsem_ring, rsem_ag, rsem_c, rsem_x):
    Z, Y, X, C, S, CB, H, F, NC = dims
    I = X * C
    NQ = Y * X
    HR = H // (2 * NSUB)
    HB = H // Y
    HU = HB // NV
    NCH = Y * S
    half = Z // 2
    rid = lax.axis_index("rep")
    nid = lax.axis_index("nodes")
    z, y, x, c = rid // Y, rid % Y, nid // C, nid % C
    chip = y * X + x
    partner = (rid, x * C + 1 - c)

    def at_z(zz):
        return (zz * Y + y, nid)

    def at_y(yy):
        return (z * Y + yy, nid)

    def at_x(xx):
        return (rid, xx * C + c)

    def at_chip(q):
        return (z * Y + q // X, (q % X) * C + c)

    def send(src, dst, ss, rs, dev):
        pltpu.make_async_remote_copy(src_ref=src, dst_ref=dst, send_sem=ss, recv_sem=rs, device_id=dev,
                                     device_id_type=pl.DeviceIdType.MESH).start()

    def arrived(ref, rs):
        pltpu.make_async_remote_copy(src_ref=ref, dst_ref=ref, send_sem=ssem.at[0], recv_sem=rs, device_id=partner,
                                     device_id_type=pl.DeviceIdType.MESH).wait_recv()

    def sent(ref, ss):
        pltpu.make_async_remote_copy(src_ref=ref, dst_ref=ref, send_sem=ss, recv_sem=rsem.at[0], device_id=partner,
                                     device_id_type=pl.DeviceIdType.MESH).wait_send()

    def dot(a, b):
        return jnp.dot(a, b, preferred_element_type=F32)

    def most(ref):
        return ref.at[0, pl.ds(0, NQ - 1)]

    def plane_rows(ref, yb):
        return jnp.stack([ref[k, yb * X:(yb + 1) * X] for k in range(C)], axis=1).reshape(CB, LANES)

    def added(ref, n):
        acc = ref[0]
        for k in range(1, n):
            acc = acc + ref[k]
        return acc

    (E_X, E_XC, E_A, E_B, E_F, E_RING, E_CNT, E_Y2, E_Y2C, E_Z2, E_G2, E_DC, E_DX, E_DY, E_AG, E_RC, E_RX, E_RX2,
     E_WC, E_WX, E_WY, E_WZ, E_OZ, E_OY, E_OX, E_OC, E_PC, E_PX, E_PZ, E_QZ, E_QY, E_QX, E_LA, E_L1, E_L2,
     E_M, E_DY2, E_DX2, E_DG) = range(NSEM)

    load_a = pltpu.make_async_copy(a_hbm, af.at[y], ssem.at[E_LA])
    load_1 = pltpu.make_async_copy(w_one, w1f, ssem.at[E_L1])
    load_2 = pltpu.make_async_copy(w_two, w2f, ssem.at[E_L2])
    load_a.start()
    load_1.start()
    load_2.start()

    bar = pltpu.get_barrier_semaphore()
    for d in range(1, Z):
        pl.semaphore_signal(bar, inc=1, device_id=at_z((z + d) % Z), device_id_type=pl.DeviceIdType.MESH)

    def greet_plane(d, u):
        pl.semaphore_signal(bar, inc=1, device_id=at_chip(lax.rem(chip + d, NQ)), device_id_type=pl.DeviceIdType.MESH)
        return u

    lax.fori_loop(1, NQ, greet_plane, 0)
    pl.semaphore_signal(bar, inc=1, device_id=partner, device_id_type=pl.DeviceIdType.MESH)

    mt[...] = jnp.zeros_like(mt)
    mt[0:F] = feat[...].astype(F32)
    mt[F:F + 1] = msk[...].astype(F32)
    mt[F + 1:F + 2] = lab[...].astype(F32)
    mtt[...] = mt[...].T
    xs[...] = mtt[...].astype(BF)
    pl.semaphore_wait(bar, NQ + Z - 1)

    def send_x(d, u):
        q = lax.rem(chip + d, NQ)
        send(xs, xp.at[c, chip], ssem.at[E_X], rsem.at[E_X], at_chip(q))
        return u

    lax.fori_loop(1, NQ, send_x, 0)
    xp[c, chip] = xs[...]
    load_a.wait()

    order = []
    for k in range(1, half + 1):
        order.append(-k)
        if k < half:
            order.append(k)
    order.append(0)
    for k in order:
        zc = (z + k + Z) % Z
        for d in (1, 3, 2):
            yq = (y + d) % Y
            send(af.at[y, zc, yq], af.at[y, zc, yq], ssem.at[E_A], rsem_a.at[d - 1, zc], at_y(yq))
    def spread_a(k):
        for d in (1, 3):
            yq = (y + d) % Y
            ya = (yq + k) % Y
            send(af.at[y, :, ya], af.at[y, :, ya], ssem.at[E_B], rsem_b.at[d // 2, k - 1], at_y(yq))

    def forward_a():
        for k in range(1, Y):
            for d in (1, 3):
                arrived(af.at[0, :, 0], rsem_b.at[d // 2, k - 1])
        for k in range(1, Y):
            for d in (1, 3):
                ys, yq = (y - d + Y) % Y, (y + d) % Y
                lo = 0 if d == 1 else half
                ya = (yq + k) % Y
                send(af.at[ys, pl.ds(lo, half), ya], af.at[ys, pl.ds(lo, half), ya], ssem.at[E_F], rsem_f.at[d // 2, k - 1], at_y(yq))

    spread_a(1)
    spread_a(2)

    load_1.wait()
    w1[...] = jnp.zeros_like(w1)
    w1[0:F] = w1f[...].astype(BF)
    load_2.wait()
    w2[...] = jnp.zeros_like(w2)
    for k in range(Y):
        rows = slice(k * HB, (k + 1) * HB)
        w2[rows, 0:NC] = w2f[rows].astype(BF)
        w2t[:, rows] = w2[rows].T

    arrived(most(xp), rsem.at[E_X])
    send(xp.at[c], xp.at[c], ssem.at[E_XC], rsem.at[E_XC], partner)
    arrived(xp.at[0], rsem.at[E_XC])

    def wait_a(zc):
        for d in range(1, Y):
            arrived(af.at[0, 0, 0], rsem_a.at[d - 1, zc])

    def ring(t, u):
        s, j = t // (2 * NSUB), t % (2 * NSUB)
        up = j < NSUB
        dest = lax.rem(jnp.where(up, z - 1 - s, z + 1 + s) + 2 * Z, Z)
        nb = lax.rem(jnp.where(up, z + 1, z - 1) + Z, Z)
        col = pl.multiple_of(j * HR, HR)
        fresh = ((j == 0) & ((s < half) | (s == Z - 1))) | ((j == NSUB) & (s < half - 1))

        @pl.when(s == 0)
        def _():
            for yb in range(Y):
                rows = plane_rows(xp, yb)
                y1[yb * CB:(yb + 1) * CB, pl.ds(col, HR)] = dot(rows, w1[:, pl.ds(col, HR)]).astype(BF)

        @pl.when(fresh)
        def _():
            wait_a(dest)

        acc = dot(af[0, dest, y], y1[pl.ds(0, CB), pl.ds(col, HR)])
        for yb in range(1, Y):
            acc = acc + dot(af[yb, dest, y], y1[pl.ds(yb * CB, CB), pl.ds(col, HR)])
        z1[:, pl.ds(col, HR)] = acc

        @pl.when(s > 0)
        def _():
            prev = jnp.maximum(s - 1, 0)
            arrived(rb.at[0, 0], rsem_ring.at[j, prev])
            z1[:, pl.ds(col, HR)] = z1[:, pl.ds(col, HR)] + rb[j, prev]

        @pl.when(s < Z - 1)
        def _():
            here = jnp.minimum(s, Z - 2)
            sb[j, here] = z1[:, pl.ds(col, HR)]
            send(sb.at[j, here], rb.at[j, here], ssem.at[E_RING], rsem_ring.at[j, here], at_z(nb))

        return u

    lax.fori_loop(0, Z * 2 * NSUB, ring, 0)

    h1[...] = jnp.maximum(z1[...], 0.0).astype(BF)
    y2[...] = dot(h1[...], w2[...]).astype(BF)

    def send_y2(d, u):
        q = lax.rem(chip + d, NQ)
        send(y2, yp.at[c, chip], ssem.at[E_Y2], rsem.at[E_Y2], at_chip(q))
        return u

    lax.fori_loop(1, NQ, send_y2, 0)
    yp[c, chip] = y2[...]
    lane = lax.broadcasted_iota(jnp.int32, (S, LANES), 1)
    counted = jnp.sum(xp[...].astype(F32).reshape(Y * CB, LANES), axis=0, keepdims=True)
    counted = jnp.sum(jnp.where(lane[0:1] == F, counted, 0.0), axis=1, keepdims=True)
    cs[...] = jnp.broadcast_to(counted, (8, LANES))
    cr[z] = cs[...]
    for d in range(1, Z):
        send(cs, cr.at[z], ssem.at[E_CNT], rsem.at[E_CNT], at_z((z + d) % Z))
    arrived(most(yp), rsem.at[E_Y2])
    send(yp.at[c], yp.at[c], ssem.at[E_Y2C], rsem.at[E_Y2C], partner)
    arrived(yp.at[0], rsem.at[E_Y2C])
    for yb in range(Y):
        ms[yb] = jnp.where(z1[:, yb * HB:(yb + 1) * HB] > 0.0, 1.0, 0.0).astype(BF)
    for yb in range(Y):
        part = dot(af[yb, :, y].reshape(Z * S, CB), plane_rows(yp, yb)).reshape(Z, S, LANES)
        zp[...] = part if yb == 0 else zp[...] + part
    for d in range(1, Z):
        zq = (z + d) % Z
        send(zp.at[zq], zr.at[z], ssem.at[E_Z2], rsem.at[E_Z2], at_z(zq))
    zr[z] = zp[z]
    for d in (1, 3, 2):
        yq = (y + d) % Y
        send(ms.at[yq], mk.at[y], ssem.at[E_M], rsem.at[E_M], at_y(yq))
    mk[y] = ms[y]
    spread_a(3)
    arrived(zr.at[pl.ds(0, Z - 1)], rsem.at[E_Z2])
    z2 = added(zr, Z)

    arrived(cr.at[pl.ds(0, Z - 1)], rsem.at[E_CNT])
    count = added(cr, Z)[0:1, 0:1]
    own = mtt[...]
    weights = jnp.sum(jnp.where(lane == F, own, 0.0), axis=1, keepdims=True)
    labels = jnp.sum(jnp.where(lane == F + 1, own, 0.0), axis=1, keepdims=True)
    real = lane < NC
    top = jnp.max(jnp.where(real, z2, -jnp.inf), axis=1, keepdims=True)
    shifted = jnp.where(real, z2 - top, 0.0)
    log_probs = shifted - jnp.log(jnp.sum(jnp.where(real, jnp.exp(shifted), 0.0), axis=1, keepdims=True))
    hot = labels == lane.astype(F32)
    picked = jnp.sum(jnp.where(hot, log_probs, 0.0), axis=1, keepdims=True)
    loss_part = -jnp.sum(weights * picked, axis=0, keepdims=True)
    diff = jnp.where(real, jnp.exp(log_probs), 0.0) - hot.astype(F32)
    g2[...] = (diff * (weights / count)).astype(BF)
    for d in range(1, Z):
        send(g2, gr.at[z], ssem.at[E_G2], rsem.at[E_G2], at_z((z + d) % Z))
    gr[z] = g2[...]
    arrived(gr.at[pl.ds(0, Z - 1)], rsem.at[E_G2])

    g2t = gr[...].reshape(Z * S, LANES).T
    for yb in range(Y):
        part = dot(g2t, af[yb, :, y].reshape(Z * S, CB))
        dp[yb] = part.T.reshape(X, C, S, LANES)
    send(dp.at[:, :, 1 - c], rc, ssem.at[E_DC], rsem.at[E_DC], partner)
    arrived(rc, rsem.at[E_DC])
    rc[...] = rc[...] + dp[:, :, c]
    sh = S // 2
    for d in (1, 3, 2):
        xq, yq = (x + d) % X, (y + d) % Y
        send(rc.at[:, xq, pl.ds(0, sh)], rx.at[x], ssem.at[E_DX], rsem.at[E_DX], at_x(xq))
        send(rc.at[yq, :, pl.ds(sh, sh)], ry.at[y], ssem.at[E_DY], rsem.at[E_DY], at_y(yq))
    rx[x] = rc[:, x, 0:sh]
    ry[y] = rc[y, :, sh:S]
    arrived(rx.at[pl.ds(0, X - 1)], rsem.at[E_DX])
    rx[x] = added(rx, X)
    for d in (1, 3, 2):
        yq = (y + d) % Y
        send(rx.at[x, yq], ry2.at[y], ssem.at[E_DY2], rsem.at[E_DY2], at_y(yq))
    ry2[y] = rx[x, y]
    arrived(ry.at[pl.ds(0, Y - 1)], rsem.at[E_DY])
    ry[y] = added(ry, Y)
    for d in (1, 3, 2):
        xq = (x + d) % X
        send(ry.at[y, xq], rx2d.at[x], ssem.at[E_DX2], rsem.at[E_DX2], at_x(xq))
    rx2d[x] = ry[y, x]
    arrived(ry2.at[pl.ds(0, Y - 1)], rsem.at[E_DY2])
    arrived(rx2d.at[pl.ds(0, X - 1)], rsem.at[E_DX2])
    d2[0:sh] = added(ry2, Y).astype(BF)
    d2[sh:S] = added(rx2d, X).astype(BF)
    for d in (1, 3, 2):
        send(d2, dg.at[y], ssem.at[E_DG], rsem.at[E_DG], at_y((y + d) % Y))
    dg[y] = d2[...]
    forward_a()
    dy2 = d2[...]

    def g_one(v):
        col = pl.multiple_of(y * HB + v * HU, HU)
        dh = dot(dg[...].reshape(Y * S, LANES), w2t[:, pl.ds(col, HU)])
        keep = mk[:, :, v * HU:(v + 1) * HU].reshape(Y * S, HU).astype(F32)
        gz[v, z] = jnp.where(keep > 0.0, dh, 0.0).astype(BF).reshape(Y, S, HU)

    def gather_step(v, t):
        for d in range(2):
            sgn = 1 if d == 0 else -1
            blk = (z - sgn * (t - 1) + Z) % Z
            if t > 1:
                arrived(gz.at[v, 0], rsem_ag.at[v, d, t - 1])
            ref = gz.at[v, blk] if t < half else gz.at[v, blk, pl.ds(d * (Y // 2), Y // 2)]
            send(ref, ref, ssem.at[E_AG], rsem_ag.at[v, d, t], at_z((z + sgn + Z) % Z))

    def product(v):
        for d in range(2):
            arrived(gz.at[v, 0, pl.ds(0, Y // 2)], rsem_ag.at[v, d, half])
        for k in range(Z):
            gt[v, :, k * Y * S:(k + 1) * Y * S] = gz[v, k].reshape(Y * S, HU).T

        def chunk(k, u):
            hops = k // (CB // NCH)
            yb = lax.rem(y + hops + jnp.where(hops == 2, 1, 0) - jnp.where(hops == 3, 1, 0), Y)
            q = yb * (CB // NCH) + k % (CB // NCH)
            off = pl.multiple_of((q % (CB // NCH)) * NCH, NCH)
            dy[v, q // C, q % C] = dot(gt[v], af[yb, :, :, :, pl.ds(off, NCH)].reshape(Z * Y * S, NCH))
            return u

        first = (Y - 1) * (CB // NCH) if v == 0 else 0
        lax.fori_loop(0, first, chunk, 0)
        if v == 0:
            for d in (1, 3):
                for k in range(1, Y):
                    arrived(af.at[0, pl.ds(0, half), 0], rsem_f.at[d // 2, k - 1])
        lax.fori_loop(first, X * C, chunk, 0)
        send(dy.at[v, :, 1 - c], rcy.at[v], ssem.at[E_RC], rsem_c.at[v], partner)

    nxt, prv, opp = (x + 1) % X, (x + X - 1) % X, (x + 2) % X
    hh = HU // 2

    def reduce_core(v):
        arrived(rcy.at[v], rsem_c.at[v])
        for k in range(X):
            rcy[v, k] = rcy[v, k] + dy[v, k, c]
        send(rcy.at[v, opp, pl.ds(0, hh)], rx1.at[v, 0], ssem.at[E_RX], rsem_x.at[v, 0], at_x(nxt))
        send(rcy.at[v, opp, pl.ds(hh, hh)], rx1.at[v, 1], ssem.at[E_RX], rsem_x.at[v, 1], at_x(prv))

    def reduce_x(v):
        arrived(rx1.at[v, 0], rsem_x.at[v, 0])
        rcy[v, nxt, pl.ds(0, hh)] = rcy[v, nxt, pl.ds(0, hh)] + rx1[v, 0]
        send(rcy.at[v, nxt], rx2.at[v, 0], ssem.at[E_RX2], rsem_x.at[v, 2], at_x(nxt))
        arrived(rx1.at[v, 1], rsem_x.at[v, 1])
        rcy[v, prv, pl.ds(hh, hh)] = rcy[v, prv, pl.ds(hh, hh)] + rx1[v, 1]
        send(rcy.at[v, prv], rx2.at[v, 1], ssem.at[E_RX2], rsem_x.at[v, 3], at_x(prv))

    def own_x():
        return jnp.concatenate([xp[m % C, nid * (Y // C) + m // C] for m in range(Y)], axis=0)

    def grad_one(v):
        arrived(rx2.at[v, 0], rsem_x.at[v, 2])
        arrived(rx2.at[v, 1], rsem_x.at[v, 3])
        acc = (rcy[v, x] + rx2[v, 0] + rx2[v, 1]).astype(BF)
        part = dot(acc, own_x())
        if v >= NV // 2:
            part = jnp.concatenate([part[:, LANES // 2:], part[:, 0:LANES // 2]], axis=1)
        per = HU // (Z * 8)
        rows = part.reshape(per, Z, 8, LANES)
        for m in range(per):
            k = (v % (NV // 2)) * per + m
            pb[k] = rows[m] if v < NV // 2 else pb[k] + rows[m]

    def w_begin():
        mark = (lax.broadcasted_iota(jnp.int32, (HB, LANES), 0) == 0) & (lax.broadcasted_iota(jnp.int32, (HB, LANES), 1) == NC)
        for k in range(Y):
            part = lax.dot_general(h1[:, k * HB:(k + 1) * HB], dy2, (((0,), (0,)), ((), ())), preferred_element_type=F32)
            if k == 0:
                part = jnp.where(mark, loss_part, part)
            per = HB // (Y * Z * 8)
            rows = part.reshape(per, Y, Z, 8, LANES)
            for m in range(per):
                q = k * per + m
                wb[q // X, q % X] = rows[m]
        send(wb.at[1 - c], wc, ssem.at[E_WC], rsem.at[E_WC], partner)

    def w_core():
        arrived(wc, rsem.at[E_WC])
        wc[...] = wc[...] + wb[c]
        for d in (1, 3, 2):
            xq = (x + d) % X
            send(wc.at[xq], wx.at[x], ssem.at[E_WX], rsem.at[E_WX], at_x(xq))
        wx[x] = wc[x]

    def w_x():
        arrived(wx.at[pl.ds(0, X - 1)], rsem.at[E_WX])
        wx[x] = added(wx, X)
        for d in (1, 3, 2):
            yq = (y + d) % Y
            send(wx.at[x, yq], wy.at[y], ssem.at[E_WY], rsem.at[E_WY], at_y(yq))
        wy[y] = wx[x, y]

    def w_y():
        arrived(wy.at[pl.ds(0, Y - 1)], rsem.at[E_WY])
        wy[y] = added(wy, Y)
        for d in range(1, Z):
            zq = (z + d) % Z
            send(wy.at[y, zq], wz.at[z], ssem.at[E_WZ], rsem.at[E_WZ], at_z(zq))
        wz[z] = wy[y, z]

    def w_z():
        arrived(wz.at[pl.ds(0, Z - 1)], rsem.at[E_WZ])
        wf[...] = added(wz, Z)
        for d in range(1, Z):
            send(wf, oz.at[z], ssem.at[E_OZ], rsem.at[E_OZ], at_z((z + d) % Z))
        oz[z] = wf[...]

    def o_z():
        arrived(oz.at[pl.ds(0, Z - 1)], rsem.at[E_OZ])
        for d in (1, 3, 2):
            send(oz, oy.at[y], ssem.at[E_OY], rsem.at[E_OY], at_y((y + d) % Y))
        oy[y] = oz[...]

    def o_y():
        arrived(oy.at[pl.ds(0, Y - 1)], rsem.at[E_OY])
        for d in (1, 3, 2):
            send(oy, ox.at[x], ssem.at[E_OX], rsem.at[E_OX], at_x((x + d) % X))
        ox[x] = oy[...]

    def o_x():
        arrived(ox.at[pl.ds(0, X - 1)], rsem.at[E_OX])
        send(ox, oc.at[c], ssem.at[E_OC], rsem.at[E_OC], partner)
        oc[c] = ox[...]

    arrived(mk.at[pl.ds(0, Y - 1)], rsem.at[E_M])
    arrived(dg.at[pl.ds(0, Y - 1)], rsem.at[E_DG])
    steps = [
        (g_one, 0), (gather_step, 0, 1), (g_one, 1), (gather_step, 1, 1), (g_one, 2), (g_one, 3), (w_begin,),
        (gather_step, 0, 2), (gather_step, 1, 2), (w_core,)]
    for t in range(3, half + 1):
        steps += [(gather_step, 0, t), (gather_step, 1, t)]
    steps += [(gather_step, 2, 1), (gather_step, 3, 1), (product, 0), (gather_step, 2, 2), (gather_step, 3, 2), (w_x,), (product, 1),
              (reduce_core, 0)]
    for t in range(3, half + 1):
        steps += [(gather_step, 2, t), (gather_step, 3, t)]
        if t == 3:
            steps += [(reduce_core, 1), (reduce_x, 0), (w_y,)]
    steps += [(reduce_x, 1), (product, 2), (product, 3), (reduce_core, 2), (grad_one, 0), (reduce_core, 3), (reduce_x, 2), (w_z,),
              (grad_one, 1), (reduce_x, 3), (o_z,), (grad_one, 2), (grad_one, 3)]
    for step in steps:
        step[0](*step[1:])

    send(pb, pc, ssem.at[E_PC], rsem.at[E_PC], partner)
    arrived(pc, rsem.at[E_PC])
    pc[...] = pc[...] + pb[...]
    for d in (1, 3, 2):
        xq = (x + d) % X
        send(pc.at[xq], px.at[x], ssem.at[E_PX], rsem.at[E_PX], at_x(xq))
    px[x] = pc[x]
    o_y()
    arrived(px.at[pl.ds(0, X - 1)], rsem.at[E_PX])
    px[x] = added(px, X)
    for d in range(1, Z):
        zq = (z + d) % Z
        send(px.at[x, zq], pz.at[z], ssem.at[E_PZ], rsem.at[E_PZ], at_z(zq))
    pz[z] = px[x, z]
    arrived(pz.at[pl.ds(0, Z - 1)], rsem.at[E_PZ])
    pf[...] = added(pz, Z)
    for d in range(1, Z):
        send(pf, qz.at[z], ssem.at[E_QZ], rsem.at[E_QZ], at_z((z + d) % Z))
    qz[z] = pf[...]
    o_x()
    arrived(qz.at[pl.ds(0, Z - 1)], rsem.at[E_QZ])
    for d in (1, 3, 2):
        send(qz, qy.at[y], ssem.at[E_QY], rsem.at[E_QY], at_y((y + d) % Y))
    qy[y] = qz[...]
    arrived(oc.at[0], rsem.at[E_OC])
    for k in range(C):
        full = oc[k].reshape(H // C, LANES)
        dw2_out[k * (H // C):(k + 1) * (H // C), :] = full[:, 0:NC]
        if k == 0:
            loss_out[...] = jnp.broadcast_to(full[0:1, NC:NC + 1] / count, (8, LANES))
    arrived(qy.at[pl.ds(0, Y - 1)], rsem.at[E_QY])
    for d in (1, 3, 2):
        send(qy, qx.at[x], ssem.at[E_QX], rsem.at[E_QX], at_x((x + d) % X))
    qx[x] = qy[...]
    arrived(qx.at[pl.ds(0, X - 1)], rsem.at[E_QX])
    for yb in range(Y):
        part = qx[:, yb].reshape(HB // 2, LANES).T
        dw1_out[:, yb * HB:yb * HB + HB // 2] = part[0:F]
        dw1_out[:, yb * HB + HB // 2:(yb + 1) * HB] = part[LANES // 2:LANES // 2 + F]

    sent(most(xp), ssem.at[E_X])
    sent(xp.at[0], ssem.at[E_XC])
    sent(af.at[pl.ds(0, Y - 1), :, 0], ssem.at[E_A])
    sent(af.at[pl.ds(0, Y - 1), :, pl.ds(0, 2)], ssem.at[E_B])
    sent(af.at[pl.ds(0, Y - 1), :, 0], ssem.at[E_F])
    sent(sb, ssem.at[E_RING])
    sent(cr.at[pl.ds(0, Z - 1)], ssem.at[E_CNT])
    sent(most(yp), ssem.at[E_Y2])
    sent(yp.at[0], ssem.at[E_Y2C])
    sent(zr.at[pl.ds(0, Z - 1)], ssem.at[E_Z2])
    sent(gr.at[pl.ds(0, Z - 1)], ssem.at[E_G2])
    sent(rc, ssem.at[E_DC])
    sent(rx.at[pl.ds(0, X - 1)], ssem.at[E_DX])
    sent(ry.at[pl.ds(0, Y - 1)], ssem.at[E_DY])
    sent(ry2.at[pl.ds(0, Y - 1)], ssem.at[E_DY2])
    sent(rx2d.at[pl.ds(0, X - 1)], ssem.at[E_DX2])
    sent(dg.at[pl.ds(0, Y - 1)], ssem.at[E_DG])
    sent(mk.at[pl.ds(0, Y - 1)], ssem.at[E_M])
    sent(gz.at[:, pl.ds(0, Z - 1)], ssem.at[E_AG])
    sent(rcy, ssem.at[E_RC])
    sent(rx1, ssem.at[E_RX])
    sent(rx2, ssem.at[E_RX2])
    sent(wc, ssem.at[E_WC])
    sent(wx.at[pl.ds(0, X - 1)], ssem.at[E_WX])
    sent(wy.at[pl.ds(0, Y - 1)], ssem.at[E_WY])
    sent(wz.at[pl.ds(0, Z - 1)], ssem.at[E_WZ])
    sent(oz.at[pl.ds(0, Z - 1)], ssem.at[E_OZ])
    sent(oy.at[pl.ds(0, Y - 1)], ssem.at[E_OY])
    sent(ox.at[pl.ds(0, X - 1)], ssem.at[E_OX])
    sent(oc.at[0], ssem.at[E_OC])
    sent(pc, ssem.at[E_PC])
    sent(px.at[pl.ds(0, X - 1)], ssem.at[E_PX])
    sent(pz.at[pl.ds(0, Z - 1)], ssem.at[E_PZ])
    sent(qz.at[pl.ds(0, Z - 1)], ssem.at[E_QZ])
    sent(qy.at[pl.ds(0, Y - 1)], ssem.at[E_QY])
    sent(qx.at[pl.ds(0, X - 1)], ssem.at[E_QX])


def solution(mesh):
    Y, X, C = Y_DIM, X_DIM, CORES
    Z = mesh.shape["rep"] // Y
    row_spec = P(("rep", "nodes"))

    def device_step(adj_blk, feat_blk, w_one, w_two, label_blk, mask_blk):
        R, S, CB = adj_blk.shape
        F, H = w_one.shape
        NC = w_two.shape[1]
        I = X * C
        NQ = Y * X
        HR = H // (2 * NSUB)
        HB = H // Y
        HU = HB // NV
        NCH = Y * S
        assert R == Z * Y and CB == S * I and F + 2 <= LANES // 2 and NC < LANES
        vm = pltpu.VMEM
        dma = pltpu.SemaphoreType.DMA
        scratch = [
            vm((Y, Z, Y, S, CB), BF),
            vm((LANES, S), F32),
            vm((S, LANES), F32),
            vm((F, H), F32),
            vm((H, NC), F32),
            vm((LANES, H), BF),
            vm((H, LANES), BF),
            vm((LANES, H), BF),
            vm((S, LANES), BF),
            vm((C, NQ, S, LANES), BF),
            vm((Y * CB, H), BF),
            vm((8, LANES), F32),
            vm((Z, 8, LANES), F32),
            vm((2 * NSUB, Z - 1, S, HR), F32),
            vm((2 * NSUB, Z - 1, S, HR), F32),
            vm((S, H), F32),
            vm((S, H), BF),
            vm((S, LANES), BF),
            vm((C, NQ, S, LANES), BF),
            vm((Z, S, LANES), F32),
            vm((Z, S, LANES), F32),
            vm((S, LANES), BF),
            vm((Z, S, LANES), BF),
            vm((Y, X, C, S, LANES), F32),
            vm((Y, X, S, LANES), F32),
            vm((X, Y, S // 2, LANES), F32),
            vm((Y, X, S // 2, LANES), F32),
            vm((Y, S // 2, LANES), F32),
            vm((X, S // 2, LANES), F32),
            vm((S, LANES), BF),
            vm((Y, S, LANES), BF),
            vm((Y, S, HB), BF),
            vm((Y, S, HB), BF),
            vm((NV, Z, Y, S, HU), BF),
            vm((NV, HU, Z * Y * S), BF),
            vm((NV, X, C, HU, NCH), F32),
            vm((NV, X, HU, NCH), F32),
            vm((NV, 2, HU // 2, NCH), F32),
            vm((NV, 2, HU, NCH), F32),
            vm((C, X, Y, Z, 8, LANES), F32),
            vm((X, Y, Z, 8, LANES), F32),
            vm((X, Y, Z, 8, LANES), F32),
            vm((Y, Z, 8, LANES), F32),
            vm((Z, 8, LANES), F32),
            vm((8, LANES), F32),
            vm((Z, 8, LANES), F32),
            vm((Y, Z, 8, LANES), F32),
            vm((X, Y, Z, 8, LANES), F32),
            vm((C, X, Y, Z, 8, LANES), F32),
            vm((X, Z, 8, LANES), F32),
            vm((X, Z, 8, LANES), F32),
            vm((X, Z, 8, LANES), F32),
            vm((Z, 8, LANES), F32),
            vm((8, LANES), F32),
            vm((Z, 8, LANES), F32),
            vm((Y, Z, 8, LANES), F32),
            vm((X, Y, Z, 8, LANES), F32),
            dma((NSEM,)),
            dma((NSEM,)),
            dma((Y - 1, Z)),
            dma((2, Y - 1)),
            dma((2, Y - 1)),
            dma((2 * NSUB, Z - 1)),
            dma((NV, 2, Z // 2 + 1)),
            dma((NV,)),
            dma((NV, 4)),
        ]
        vspec = pl.BlockSpec(memory_space=pltpu.VMEM)
        aspec = pl.BlockSpec(memory_space=pl.ANY)
        dw_one, dw_two, loss = pl.pallas_call(
            functools.partial(_step, (Z, Y, X, C, S, CB, H, F, NC)),
            out_shape=(jax.ShapeDtypeStruct((F, H), F32), jax.ShapeDtypeStruct((H, NC), F32), jax.ShapeDtypeStruct((8, LANES), F32)),
            in_specs=[aspec, vspec, vspec, vspec, aspec, aspec],
            out_specs=(vspec, vspec, vspec),
            scratch_shapes=scratch,
            compiler_params=pltpu.CompilerParams(collective_id=0, has_side_effects=True, vmem_limit_bytes=62 * 1024 * 1024),
            name="gcn_step",
        )(adj_blk.reshape(Z, Y, S, CB), feat_blk.T, label_blk[None, :], mask_blk[None, :], w_one, w_two)
        return loss[0, 0], dw_one, dw_two

    return jax.shard_map(device_step, mesh=mesh, in_specs=(P(None, "nodes", "rep"), row_spec, P(), P(), row_spec, row_spec), out_specs=(P(), P(), P()), check_vma=False)
```

```python
import functools

import jax
import jax.numpy as jnp
from jax import lax
from jax.experimental import pallas as pl
from jax.experimental.pallas import tpu as pltpu
from jax.sharding import PartitionSpec as P

Y_DIM = 4
X_DIM = 4
CORES = 2
LANES = 128
NSUB = 4
NV = 4
NSEM = 41
BF = jnp.bfloat16
F32 = jnp.float32


def _step(dims, a_hbm, feat, lab, msk, w_one, w_two, dw1_out, dw2_out, loss_out,
          af, mt, mtt, w1f, w2f, w1, w2, w2t, xs, xp, y1, cs, cr, sb, rb, z1, h1, y2, yp, zp, zr, g2, gr, dp, rc, rx, ry, ry2, rx2d,
          d2, dg, ms, mk, gz, gt, dy, rcy, rx1, rx2, wb, wc, wx, wy, wz, wf, oz, oy, ox, oc, pb, pc, px, pz, pf, qz, qy, qx, qxy, qyx,
          ssem, rsem, rsem_a, rsem_b, rsem_f, rsem_ring, rsem_ag, rsem_c, rsem_x):
    Z, Y, X, C, S, CB, H, F, NC = dims
    I = X * C
    NQ = Y * X
    HR = H // (2 * NSUB)
    HB = H // Y
    HU = HB // NV
    NCH = Y * S
    half = Z // 2
    rid = lax.axis_index("rep")
    nid = lax.axis_index("nodes")
    z, y, x, c = rid // Y, rid % Y, nid // C, nid % C
    chip = y * X + x
    partner = (rid, x * C + 1 - c)

    far = sorted(range(1, Z), key=lambda d: -min(d, Z - d))

    def at_z(zz):
        return (zz * Y + y, nid)

    def at_y(yy):
        return (z * Y + yy, nid)

    def at_x(xx):
        return (rid, xx * C + c)

    def at_chip(q):
        return (z * Y + q // X, (q % X) * C + c)

    def send(src, dst, ss, rs, dev):
        pltpu.make_async_remote_copy(src_ref=src, dst_ref=dst, send_sem=ss, recv_sem=rs, device_id=dev,
                                     device_id_type=pl.DeviceIdType.MESH).start()

    def arrived(ref, rs):
        pltpu.make_async_remote_copy(src_ref=ref, dst_ref=ref, send_sem=ssem.at[0], recv_sem=rs, device_id=partner,
                                     device_id_type=pl.DeviceIdType.MESH).wait_recv()

    def sent(ref, ss):
        pltpu.make_async_remote_copy(src_ref=ref, dst_ref=ref, send_sem=ss, recv_sem=rsem.at[0], device_id=partner,
                                     device_id_type=pl.DeviceIdType.MESH).wait_send()

    def dot(a, b):
        return jnp.dot(a, b, preferred_element_type=F32)

    def most(ref):
        return ref.at[0, pl.ds(0, NQ - 1)]

    def plane_rows(ref, yb):
        return jnp.stack([ref[k, yb * X:(yb + 1) * X] for k in range(C)], axis=1).reshape(CB, LANES)

    def added(ref, n):
        acc = ref[0]
        for k in range(1, n):
            acc = acc + ref[k]
        return acc

    (E_X, E_XC, E_A, E_B, E_F, E_RING, E_CNT, E_Y2, E_Y2C, E_Z2, E_G2, E_DC, E_DX, E_DY, E_AG, E_RC, E_RX, E_RX2,
     E_WC, E_WX, E_WY, E_WZ, E_OZ, E_OY, E_OX, E_OC, E_PC, E_PX, E_PZ, E_QZ, E_QY, E_QX, E_LA, E_L1, E_L2,
     E_M, E_DY2, E_DX2, E_DG, E_QXY, E_QYX) = range(NSEM)

    load_a = pltpu.make_async_copy(a_hbm, af.at[y], ssem.at[E_LA])
    load_1 = pltpu.make_async_copy(w_one, w1f, ssem.at[E_L1])
    load_2 = pltpu.make_async_copy(w_two, w2f, ssem.at[E_L2])
    load_a.start()
    load_1.start()
    load_2.start()

    bar = pltpu.get_barrier_semaphore()
    for d in far:
        pl.semaphore_signal(bar, inc=1, device_id=at_z((z + d) % Z), device_id_type=pl.DeviceIdType.MESH)

    def greet_plane(d, u):
        pl.semaphore_signal(bar, inc=1, device_id=at_chip(lax.rem(chip + d, NQ)), device_id_type=pl.DeviceIdType.MESH)
        return u

    lax.fori_loop(1, NQ, greet_plane, 0)
    pl.semaphore_signal(bar, inc=1, device_id=partner, device_id_type=pl.DeviceIdType.MESH)

    mt[...] = jnp.zeros_like(mt)
    mt[0:F] = feat[...].astype(F32)
    mt[F:F + 1] = msk[...].astype(F32)
    mt[F + 1:F + 2] = lab[...].astype(F32)
    mtt[...] = mt[...].T
    xs[...] = mtt[...].astype(BF)
    pl.semaphore_wait(bar, NQ + Z - 1)

    def send_x(d, u):
        q = lax.rem(chip + d, NQ)
        send(xs, xp.at[c, chip], ssem.at[E_X], rsem.at[E_X], at_chip(q))
        return u

    lax.fori_loop(1, NQ, send_x, 0)
    xp[c, chip] = xs[...]
    load_a.wait()

    order = []
    for k in range(1, half + 1):
        order.append(-k)
        if k < half:
            order.append(k)
    order.append(0)
    for k in order:
        zc = (z + k + Z) % Z
        for d in (2, 1, 3):
            yq = (y + d) % Y
            send(af.at[y, zc, yq], af.at[y, zc, yq], ssem.at[E_A], rsem_a.at[d - 1, zc], at_y(yq))
    def spread_a(k):
        for d in (1, 3):
            yq = (y + d) % Y
            ya = (yq + k) % Y
            send(af.at[y, :, ya], af.at[y, :, ya], ssem.at[E_B], rsem_b.at[d // 2, k - 1], at_y(yq))

    def forward_a():
        for k in range(1, Y):
            for d in (1, 3):
                arrived(af.at[0, :, 0], rsem_b.at[d // 2, k - 1])
        for k in range(1, Y):
            for d in (1, 3):
                ys, yq = (y - d + Y) % Y, (y + d) % Y
                lo = 0 if d == 1 else half
                ya = (yq + k) % Y
                send(af.at[ys, pl.ds(lo, half), ya], af.at[ys, pl.ds(lo, half), ya], ssem.at[E_F], rsem_f.at[d // 2, k - 1], at_y(yq))

    spread_a(1)
    spread_a(2)

    load_1.wait()
    w1[...] = jnp.zeros_like(w1)
    w1[0:F] = w1f[...].astype(BF)
    load_2.wait()
    w2[...] = jnp.zeros_like(w2)
    for k in range(Y):
        rows = slice(k * HB, (k + 1) * HB)
        w2[rows, 0:NC] = w2f[rows].astype(BF)
        w2t[:, rows] = w2[rows].T

    arrived(most(xp), rsem.at[E_X])
    send(xp.at[c], xp.at[c], ssem.at[E_XC], rsem.at[E_XC], partner)
    arrived(xp.at[0], rsem.at[E_XC])

    def wait_a(zc):
        for d in range(1, Y):
            arrived(af.at[0, 0, 0], rsem_a.at[d - 1, zc])

    def ring(t, u):
        s, j = t // (2 * NSUB), t % (2 * NSUB)
        up = j % 2 == 0
        dest = lax.rem(jnp.where(up, z - 1 - s, z + 1 + s) + 2 * Z, Z)
        nb = lax.rem(jnp.where(up, z + 1, z - 1) + Z, Z)
        col = pl.multiple_of(j * HR, HR)
        fresh = ((j == 0) & ((s < half) | (s == Z - 1))) | ((j == 1) & (s < half - 1))

        @pl.when(s == 0)
        def _():
            for yb in range(Y):
                rows = plane_rows(xp, yb)
                y1[yb * CB:(yb + 1) * CB, pl.ds(col, HR)] = dot(rows, w1[:, pl.ds(col, HR)]).astype(BF)

        @pl.when(fresh)
        def _():
            wait_a(dest)

        acc = dot(af[0, dest, y], y1[pl.ds(0, CB), pl.ds(col, HR)])
        for yb in range(1, Y):
            acc = acc + dot(af[yb, dest, y], y1[pl.ds(yb * CB, CB), pl.ds(col, HR)])
        z1[:, pl.ds(col, HR)] = acc

        @pl.when(s > 0)
        def _():
            prev = jnp.maximum(s - 1, 0)
            arrived(rb.at[0, 0], rsem_ring.at[j, prev])
            z1[:, pl.ds(col, HR)] = z1[:, pl.ds(col, HR)] + rb[j, prev]

        @pl.when(s < Z - 1)
        def _():
            here = jnp.minimum(s, Z - 2)
            sb[j, here] = z1[:, pl.ds(col, HR)]
            send(sb.at[j, here], rb.at[j, here], ssem.at[E_RING], rsem_ring.at[j, here], at_z(nb))

        return u

    lax.fori_loop(0, Z * 2 * NSUB, ring, 0)

    h1[...] = jnp.maximum(z1[...], 0.0).astype(BF)
    y2[...] = dot(h1[...], w2[...]).astype(BF)

    def send_y2(d, u):
        q = lax.rem(chip + d, NQ)
        send(y2, yp.at[c, chip], ssem.at[E_Y2], rsem.at[E_Y2], at_chip(q))
        return u

    lax.fori_loop(1, NQ, send_y2, 0)
    yp[c, chip] = y2[...]
    lane = lax.broadcasted_iota(jnp.int32, (S, LANES), 1)
    counted = jnp.sum(xp[...].astype(F32).reshape(Y * CB, LANES), axis=0, keepdims=True)
    counted = jnp.sum(jnp.where(lane[0:1] == F, counted, 0.0), axis=1, keepdims=True)
    cs[...] = jnp.broadcast_to(counted, (8, LANES))
    cr[z] = cs[...]
    for d in far:
        send(cs, cr.at[z], ssem.at[E_CNT], rsem.at[E_CNT], at_z((z + d) % Z))
    arrived(most(yp), rsem.at[E_Y2])
    send(yp.at[c], yp.at[c], ssem.at[E_Y2C], rsem.at[E_Y2C], partner)
    arrived(yp.at[0], rsem.at[E_Y2C])
    for yb in range(Y):
        ms[yb] = jnp.where(z1[:, yb * HB:(yb + 1) * HB] > 0.0, 1.0, 0.0).astype(BF)
    for yb in range(Y):
        part = dot(af[yb, :, y].reshape(Z * S, CB), plane_rows(yp, yb)).reshape(Z, S, LANES)
        zp[...] = part if yb == 0 else zp[...] + part
    for d in far:
        zq = (z + d) % Z
        send(zp.at[zq], zr.at[z], ssem.at[E_Z2], rsem.at[E_Z2], at_z(zq))
    zr[z] = zp[z]
    for d in (2, 1, 3):
        yq = (y + d) % Y
        send(ms.at[yq], mk.at[y], ssem.at[E_M], rsem.at[E_M], at_y(yq))
    mk[y] = ms[y]
    spread_a(3)
    arrived(zr.at[pl.ds(0, Z - 1)], rsem.at[E_Z2])
    z2 = added(zr, Z)

    arrived(cr.at[pl.ds(0, Z - 1)], rsem.at[E_CNT])
    count = added(cr, Z)[0:1, 0:1]
    own = mtt[...]
    weights = jnp.sum(jnp.where(lane == F, own, 0.0), axis=1, keepdims=True)
    labels = jnp.sum(jnp.where(lane == F + 1, own, 0.0), axis=1, keepdims=True)
    real = lane < NC
    top = jnp.max(jnp.where(real, z2, -jnp.inf), axis=1, keepdims=True)
    shifted = jnp.where(real, z2 - top, 0.0)
    log_probs = shifted - jnp.log(jnp.sum(jnp.where(real, jnp.exp(shifted), 0.0), axis=1, keepdims=True))
    hot = labels == lane.astype(F32)
    picked = jnp.sum(jnp.where(hot, log_probs, 0.0), axis=1, keepdims=True)
    loss_part = -jnp.sum(weights * picked, axis=0, keepdims=True)
    diff = jnp.where(real, jnp.exp(log_probs), 0.0) - hot.astype(F32)
    g2[...] = (diff * (weights / count)).astype(BF)
    for d in far:
        send(g2, gr.at[z], ssem.at[E_G2], rsem.at[E_G2], at_z((z + d) % Z))
    gr[z] = g2[...]
    arrived(gr.at[pl.ds(0, Z - 1)], rsem.at[E_G2])

    g2t = gr[...].reshape(Z * S, LANES).T
    for yb in range(Y):
        part = dot(g2t, af[yb, :, y].reshape(Z * S, CB))
        dp[yb] = part.T.reshape(X, C, S, LANES)
    send(dp.at[:, :, 1 - c], rc, ssem.at[E_DC], rsem.at[E_DC], partner)
    arrived(rc, rsem.at[E_DC])
    rc[...] = rc[...] + dp[:, :, c]
    sh = S // 2
    for d in (2, 1, 3):
        xq, yq = (x + d) % X, (y + d) % Y
        send(rc.at[:, xq, pl.ds(0, sh)], rx.at[x], ssem.at[E_DX], rsem.at[E_DX], at_x(xq))
        send(rc.at[yq, :, pl.ds(sh, sh)], ry.at[y], ssem.at[E_DY], rsem.at[E_DY], at_y(yq))
    rx[x] = rc[:, x, 0:sh]
    ry[y] = rc[y, :, sh:S]
    arrived(rx.at[pl.ds(0, X - 1)], rsem.at[E_DX])
    rx[x] = added(rx, X)
    for d in (2, 1, 3):
        yq = (y + d) % Y
        send(rx.at[x, yq], ry2.at[y], ssem.at[E_DY2], rsem.at[E_DY2], at_y(yq))
    ry2[y] = rx[x, y]
    arrived(ry.at[pl.ds(0, Y - 1)], rsem.at[E_DY])
    ry[y] = added(ry, Y)
    for d in (2, 1, 3):
        xq = (x + d) % X
        send(ry.at[y, xq], rx2d.at[x], ssem.at[E_DX2], rsem.at[E_DX2], at_x(xq))
    rx2d[x] = ry[y, x]
    arrived(ry2.at[pl.ds(0, Y - 1)], rsem.at[E_DY2])
    arrived(rx2d.at[pl.ds(0, X - 1)], rsem.at[E_DX2])
    d2[0:sh] = added(ry2, Y).astype(BF)
    d2[sh:S] = added(rx2d, X).astype(BF)
    for d in (2, 1, 3):
        send(d2, dg.at[y], ssem.at[E_DG], rsem.at[E_DG], at_y((y + d) % Y))
    dg[y] = d2[...]
    forward_a()
    dy2 = d2[...]

    def g_one(v):
        col = pl.multiple_of(y * HB + v * HU, HU)
        dh = dot(dg[...].reshape(Y * S, LANES), w2t[:, pl.ds(col, HU)])
        keep = mk[:, :, v * HU:(v + 1) * HU].reshape(Y * S, HU).astype(F32)
        gz[v, z] = jnp.where(keep > 0.0, dh, 0.0).astype(BF).reshape(Y, S, HU)

    def gather_step(v, t):
        for d in range(2):
            sgn = 1 if d == 0 else -1
            blk = (z - sgn * (t - 1) + Z) % Z
            if t > 1:
                arrived(gz.at[v, 0], rsem_ag.at[v, d, t - 1])
            ref = gz.at[v, blk] if t < half else gz.at[v, blk, pl.ds(d * (Y // 2), Y // 2)]
            send(ref, ref, ssem.at[E_AG], rsem_ag.at[v, d, t], at_z((z + sgn + Z) % Z))

    def piece(v):
        return pl.ds(v % 2 * HU, HU)

    def product(p):
        for v in (2 * p, 2 * p + 1):
            for d in range(2):
                arrived(gz.at[v, 0, pl.ds(0, Y // 2)], rsem_ag.at[v, d, half])
            for k in range(Z):
                gt[p, piece(v), k * Y * S:(k + 1) * Y * S] = gz[v, k].reshape(Y * S, HU).T

        def chunk(core):
            def body(k, u):
                yb = lax.rem(y + k + jnp.where(k == 2, 1, 0) - jnp.where(k == 3, 1, 0), Y)
                q = yb * C + core
                off = pl.multiple_of(core * NCH, NCH)
                dy[p, q // C, core] = dot(gt[p], af[yb, :, :, :, pl.ds(off, NCH)].reshape(Z * Y * S, NCH))
                return u
            return body

        first = Y - 1 if p == 0 else 0
        lax.fori_loop(0, first, chunk(1 - c), 0)
        if p == 0:
            for d in (1, 3):
                for k in range(1, Y):
                    arrived(af.at[0, pl.ds(0, half), 0], rsem_f.at[d // 2, k - 1])
        lax.fori_loop(first, Y, chunk(1 - c), 0)
        for v in (2 * p, 2 * p + 1):
            send(dy.at[p, :, 1 - c, piece(v)], rcy.at[p, :, piece(v)], ssem.at[E_RC], rsem_c.at[v], partner)
        lax.fori_loop(0, Y, chunk(c), 0)

    nxt, prv, opp = (x + 1) % X, (x + X - 1) % X, (x + 2) % X
    hh = HU // 2

    def low(v):
        return pl.ds(v % 2 * HU, hh)

    def high(v):
        return pl.ds(v % 2 * HU + hh, hh)

    def reduce_core(v):
        p = v // 2
        arrived(rcy.at[p, :, piece(v)], rsem_c.at[v])
        for k in range(X):
            rcy[p, k, piece(v)] = rcy[p, k, piece(v)] + dy[p, k, c, piece(v)]
        send(rcy.at[p, opp, low(v)], rx1.at[v, 0], ssem.at[E_RX], rsem_x.at[v, 0], at_x(nxt))
        send(rcy.at[p, opp, high(v)], rx1.at[v, 1], ssem.at[E_RX], rsem_x.at[v, 1], at_x(prv))

    def reduce_x(v):
        p = v // 2
        arrived(rx1.at[v, 0], rsem_x.at[v, 0])
        rcy[p, nxt, low(v)] = rcy[p, nxt, low(v)] + rx1[v, 0]
        send(rcy.at[p, nxt, piece(v)], rx2.at[v, 0], ssem.at[E_RX2], rsem_x.at[v, 2], at_x(nxt))
        arrived(rx1.at[v, 1], rsem_x.at[v, 1])
        rcy[p, prv, high(v)] = rcy[p, prv, high(v)] + rx1[v, 1]
        send(rcy.at[p, prv, piece(v)], rx2.at[v, 1], ssem.at[E_RX2], rsem_x.at[v, 3], at_x(prv))

    def own_x():
        return jnp.concatenate([xp[m % C, nid * (Y // C) + m // C] for m in range(Y)], axis=0)

    def grad_one(v):
        arrived(rx2.at[v, 0], rsem_x.at[v, 2])
        arrived(rx2.at[v, 1], rsem_x.at[v, 3])
        acc = (rcy[v // 2, x, piece(v)] + rx2[v, 0] + rx2[v, 1]).astype(BF)
        part = dot(acc, own_x())
        if v >= NV // 2:
            part = jnp.concatenate([part[:, LANES // 2:], part[:, 0:LANES // 2]], axis=1)
        per = HU // (Z * 8)
        rows = part.reshape(per, Z, 8, LANES)
        for m in range(per):
            k = (v % (NV // 2)) * per + m
            pb[k] = rows[m] if v < NV // 2 else pb[k] + rows[m]

    def w_begin():
        mark = (lax.broadcasted_iota(jnp.int32, (HB, LANES), 0) == 0) & (lax.broadcasted_iota(jnp.int32, (HB, LANES), 1) == NC)
        for k in range(Y):
            part = lax.dot_general(h1[:, k * HB:(k + 1) * HB], dy2, (((0,), (0,)), ((), ())), preferred_element_type=F32)
            if k == 0:
                part = jnp.where(mark, loss_part, part)
            per = HB // (Y * Z * 8)
            rows = part.reshape(per, Y, Z, 8, LANES)
            for m in range(per):
                q = k * per + m
                wb[q // X, q % X] = rows[m]
        send(wb.at[1 - c], wc, ssem.at[E_WC], rsem.at[E_WC], partner)

    def w_core():
        arrived(wc, rsem.at[E_WC])
        wc[...] = wc[...] + wb[c]
        for d in (2, 1, 3):
            xq = (x + d) % X
            send(wc.at[xq], wx.at[x], ssem.at[E_WX], rsem.at[E_WX], at_x(xq))
        wx[x] = wc[x]

    def w_x():
        arrived(wx.at[pl.ds(0, X - 1)], rsem.at[E_WX])
        wx[x] = added(wx, X)
        for d in (2, 1, 3):
            yq = (y + d) % Y
            send(wx.at[x, yq], wy.at[y], ssem.at[E_WY], rsem.at[E_WY], at_y(yq))
        wy[y] = wx[x, y]

    def w_y():
        arrived(wy.at[pl.ds(0, Y - 1)], rsem.at[E_WY])
        wy[y] = added(wy, Y)
        for d in far:
            zq = (z + d) % Z
            send(wy.at[y, zq], wz.at[z], ssem.at[E_WZ], rsem.at[E_WZ], at_z(zq))
        wz[z] = wy[y, z]

    def w_z():
        arrived(wz.at[pl.ds(0, Z - 1)], rsem.at[E_WZ])
        wf[...] = added(wz, Z)
        for d in far:
            send(wf, oz.at[z], ssem.at[E_OZ], rsem.at[E_OZ], at_z((z + d) % Z))
        oz[z] = wf[...]

    def o_z():
        arrived(oz.at[pl.ds(0, Z - 1)], rsem.at[E_OZ])
        for d in (2, 1, 3):
            send(oz, oy.at[y], ssem.at[E_OY], rsem.at[E_OY], at_y((y + d) % Y))
        oy[y] = oz[...]

    def o_y():
        arrived(oy.at[pl.ds(0, Y - 1)], rsem.at[E_OY])
        for d in (2, 1, 3):
            send(oy, ox.at[x], ssem.at[E_OX], rsem.at[E_OX], at_x((x + d) % X))
        ox[x] = oy[...]

    def o_x():
        arrived(ox.at[pl.ds(0, X - 1)], rsem.at[E_OX])
        send(ox, oc.at[c], ssem.at[E_OC], rsem.at[E_OC], partner)
        oc[c] = ox[...]

    arrived(mk.at[pl.ds(0, Y - 1)], rsem.at[E_M])
    arrived(dg.at[pl.ds(0, Y - 1)], rsem.at[E_DG])
    steps = [
        (g_one, 0), (gather_step, 0, 1), (g_one, 1), (gather_step, 1, 1), (g_one, 2), (g_one, 3), (w_begin,),
        (gather_step, 0, 2), (gather_step, 1, 2), (w_core,)]
    for t in range(3, half + 1):
        steps += [(gather_step, 0, t), (gather_step, 1, t)]
    steps += [(gather_step, 2, 1), (gather_step, 3, 1), (product, 0), (gather_step, 2, 2), (gather_step, 3, 2), (w_x,), (reduce_core, 0),
              (reduce_core, 1)]
    for t in range(3, half + 1):
        steps += [(gather_step, 2, t), (gather_step, 3, t)]
        if t == 3:
            steps += [(reduce_x, 0), (w_y,), (reduce_x, 1)]
    steps += [(product, 1), (reduce_core, 2), (reduce_core, 3), (grad_one, 0), (grad_one, 1), (reduce_x, 2), (reduce_x, 3), (w_z,),
              (o_z,), (grad_one, 2), (grad_one, 3)]
    for step in steps:
        step[0](*step[1:])

    send(pb, pc, ssem.at[E_PC], rsem.at[E_PC], partner)
    arrived(pc, rsem.at[E_PC])
    pc[...] = pc[...] + pb[...]
    for d in (2, 1, 3):
        xq = (x + d) % X
        send(pc.at[xq], px.at[x], ssem.at[E_PX], rsem.at[E_PX], at_x(xq))
    px[x] = pc[x]
    o_y()
    arrived(px.at[pl.ds(0, X - 1)], rsem.at[E_PX])
    px[x] = added(px, X)
    for d in far:
        zq = (z + d) % Z
        send(px.at[x, zq], pz.at[z], ssem.at[E_PZ], rsem.at[E_PZ], at_z(zq))
    pz[z] = px[x, z]
    arrived(pz.at[pl.ds(0, Z - 1)], rsem.at[E_PZ])
    pf[...] = added(pz, Z)
    for d in far:
        send(pf, qz.at[z], ssem.at[E_QZ], rsem.at[E_QZ], at_z((z + d) % Z))
    qz[z] = pf[...]
    o_x()
    arrived(qz.at[pl.ds(0, Z - 1)], rsem.at[E_QZ])
    zl, zh = pl.ds(0, half), pl.ds(half, half)
    for d in (2, 1, 3):
        send(qz.at[zl], qy.at[y], ssem.at[E_QY], rsem.at[E_QY], at_y((y + d) % Y))
        send(qz.at[zh], qx.at[x], ssem.at[E_QX], rsem.at[E_QX], at_x((x + d) % X))
    qy[y] = qz[zl]
    qx[x] = qz[zh]
    arrived(oc.at[0], rsem.at[E_OC])
    for k in range(C):
        full = oc[k].reshape(H // C, LANES)
        dw2_out[k * (H // C):(k + 1) * (H // C), :] = full[:, 0:NC]
        if k == 0:
            loss_out[...] = jnp.broadcast_to(full[0:1, NC:NC + 1] / count, (8, LANES))
    arrived(qy.at[pl.ds(0, Y - 1)], rsem.at[E_QY])
    for d in (2, 1, 3):
        send(qy, qxy.at[x], ssem.at[E_QXY], rsem.at[E_QXY], at_x((x + d) % X))
    qxy[x] = qy[...]
    arrived(qx.at[pl.ds(0, X - 1)], rsem.at[E_QX])
    for d in (2, 1, 3):
        send(qx, qyx.at[y], ssem.at[E_QYX], rsem.at[E_QYX], at_y((y + d) % Y))
    qyx[y] = qx[...]
    arrived(qxy.at[pl.ds(0, X - 1)], rsem.at[E_QXY])
    arrived(qyx.at[pl.ds(0, Y - 1)], rsem.at[E_QYX])
    for yb in range(Y):
        part = jnp.concatenate([qxy[:, yb], qyx[yb]], axis=1).reshape(HB // 2, LANES).T
        dw1_out[:, yb * HB:yb * HB + HB // 2] = part[0:F]
        dw1_out[:, yb * HB + HB // 2:(yb + 1) * HB] = part[LANES // 2:LANES // 2 + F]

    sent(most(xp), ssem.at[E_X])
    sent(xp.at[0], ssem.at[E_XC])
    sent(af.at[pl.ds(0, Y - 1), :, 0], ssem.at[E_A])
    sent(af.at[pl.ds(0, Y - 1), :, pl.ds(0, 2)], ssem.at[E_B])
    sent(af.at[pl.ds(0, Y - 1), :, 0], ssem.at[E_F])
    sent(sb, ssem.at[E_RING])
    sent(cr.at[pl.ds(0, Z - 1)], ssem.at[E_CNT])
    sent(most(yp), ssem.at[E_Y2])
    sent(yp.at[0], ssem.at[E_Y2C])
    sent(zr.at[pl.ds(0, Z - 1)], ssem.at[E_Z2])
    sent(gr.at[pl.ds(0, Z - 1)], ssem.at[E_G2])
    sent(rc, ssem.at[E_DC])
    sent(rx.at[pl.ds(0, X - 1)], ssem.at[E_DX])
    sent(ry.at[pl.ds(0, Y - 1)], ssem.at[E_DY])
    sent(ry2.at[pl.ds(0, Y - 1)], ssem.at[E_DY2])
    sent(rx2d.at[pl.ds(0, X - 1)], ssem.at[E_DX2])
    sent(dg.at[pl.ds(0, Y - 1)], ssem.at[E_DG])
    sent(mk.at[pl.ds(0, Y - 1)], ssem.at[E_M])
    sent(gz.at[:, pl.ds(0, Z - 1)], ssem.at[E_AG])
    sent(rcy, ssem.at[E_RC])
    sent(rx1, ssem.at[E_RX])
    sent(rx2, ssem.at[E_RX2])
    sent(wc, ssem.at[E_WC])
    sent(wx.at[pl.ds(0, X - 1)], ssem.at[E_WX])
    sent(wy.at[pl.ds(0, Y - 1)], ssem.at[E_WY])
    sent(wz.at[pl.ds(0, Z - 1)], ssem.at[E_WZ])
    sent(oz.at[pl.ds(0, Z - 1)], ssem.at[E_OZ])
    sent(oy.at[pl.ds(0, Y - 1)], ssem.at[E_OY])
    sent(ox.at[pl.ds(0, X - 1)], ssem.at[E_OX])
    sent(oc.at[0], ssem.at[E_OC])
    sent(pc, ssem.at[E_PC])
    sent(px.at[pl.ds(0, X - 1)], ssem.at[E_PX])
    sent(pz.at[pl.ds(0, Z - 1)], ssem.at[E_PZ])
    sent(qz.at[pl.ds(0, Z - 1)], ssem.at[E_QZ])
    sent(qy.at[pl.ds(0, Y - 1)], ssem.at[E_QY])
    sent(qx.at[pl.ds(0, X - 1)], ssem.at[E_QX])
    sent(qxy.at[pl.ds(0, X - 1)], ssem.at[E_QXY])
    sent(qyx.at[pl.ds(0, Y - 1)], ssem.at[E_QYX])


def solution(mesh):
    Y, X, C = Y_DIM, X_DIM, CORES
    Z = mesh.shape["rep"] // Y
    row_spec = P(("rep", "nodes"))

    def device_step(adj_blk, feat_blk, w_one, w_two, label_blk, mask_blk):
        R, S, CB = adj_blk.shape
        F, H = w_one.shape
        NC = w_two.shape[1]
        I = X * C
        NQ = Y * X
        HR = H // (2 * NSUB)
        HB = H // Y
        HU = HB // NV
        NCH = Y * S
        assert R == Z * Y and CB == S * I and X == Y and F + 2 <= LANES // 2 and NC < LANES
        vm = pltpu.VMEM
        dma = pltpu.SemaphoreType.DMA
        scratch = [
            vm((Y, Z, Y, S, CB), BF),
            vm((LANES, S), F32),
            vm((S, LANES), F32),
            vm((F, H), F32),
            vm((H, NC), F32),
            vm((LANES, H), BF),
            vm((H, LANES), BF),
            vm((LANES, H), BF),
            vm((S, LANES), BF),
            vm((C, NQ, S, LANES), BF),
            vm((Y * CB, H), BF),
            vm((8, LANES), F32),
            vm((Z, 8, LANES), F32),
            vm((2 * NSUB, Z - 1, S, HR), F32),
            vm((2 * NSUB, Z - 1, S, HR), F32),
            vm((S, H), F32),
            vm((S, H), BF),
            vm((S, LANES), BF),
            vm((C, NQ, S, LANES), BF),
            vm((Z, S, LANES), F32),
            vm((Z, S, LANES), F32),
            vm((S, LANES), BF),
            vm((Z, S, LANES), BF),
            vm((Y, X, C, S, LANES), F32),
            vm((Y, X, S, LANES), F32),
            vm((X, Y, S // 2, LANES), F32),
            vm((Y, X, S // 2, LANES), F32),
            vm((Y, S // 2, LANES), F32),
            vm((X, S // 2, LANES), F32),
            vm((S, LANES), BF),
            vm((Y, S, LANES), BF),
            vm((Y, S, HB), BF),
            vm((Y, S, HB), BF),
            vm((NV, Z, Y, S, HU), BF),
            vm((NV // 2, 2 * HU, Z * Y * S), BF),
            vm((NV // 2, X, C, 2 * HU, NCH), F32),
            vm((NV // 2, X, 2 * HU, NCH), F32),
            vm((NV, 2, HU // 2, NCH), F32),
            vm((NV, 2, HU, NCH), F32),
            vm((C, X, Y, Z, 8, LANES), F32),
            vm((X, Y, Z, 8, LANES), F32),
            vm((X, Y, Z, 8, LANES), F32),
            vm((Y, Z, 8, LANES), F32),
            vm((Z, 8, LANES), F32),
            vm((8, LANES), F32),
            vm((Z, 8, LANES), F32),
            vm((Y, Z, 8, LANES), F32),
            vm((X, Y, Z, 8, LANES), F32),
            vm((C, X, Y, Z, 8, LANES), F32),
            vm((X, Z, 8, LANES), F32),
            vm((X, Z, 8, LANES), F32),
            vm((X, Z, 8, LANES), F32),
            vm((Z, 8, LANES), F32),
            vm((8, LANES), F32),
            vm((Z, 8, LANES), F32),
            vm((Y, Z // 2, 8, LANES), F32),
            vm((X, Z // 2, 8, LANES), F32),
            vm((X, Y, Z // 2, 8, LANES), F32),
            vm((Y, X, Z // 2, 8, LANES), F32),
            dma((NSEM,)),
            dma((NSEM,)),
            dma((Y - 1, Z)),
            dma((2, Y - 1)),
            dma((2, Y - 1)),
            dma((2 * NSUB, Z - 1)),
            dma((NV, 2, Z // 2 + 1)),
            dma((NV,)),
            dma((NV, 4)),
        ]
        vspec = pl.BlockSpec(memory_space=pltpu.VMEM)
        aspec = pl.BlockSpec(memory_space=pl.ANY)
        dw_one, dw_two, loss = pl.pallas_call(
            functools.partial(_step, (Z, Y, X, C, S, CB, H, F, NC)),
            out_shape=(jax.ShapeDtypeStruct((F, H), F32), jax.ShapeDtypeStruct((H, NC), F32), jax.ShapeDtypeStruct((8, LANES), F32)),
            in_specs=[aspec, vspec, vspec, vspec, aspec, aspec],
            out_specs=(vspec, vspec, vspec),
            scratch_shapes=scratch,
            compiler_params=pltpu.CompilerParams(collective_id=0, has_side_effects=True, vmem_limit_bytes=52 * 1024 * 1024),
            name="gcn_step",
        )(adj_blk.reshape(Z, Y, S, CB), feat_blk.T, label_blk[None, :], mask_blk[None, :], w_one, w_two)
        return loss[0, 0], dw_one, dw_two

    return jax.shard_map(device_step, mesh=mesh, in_specs=(P(None, "nodes", "rep"), row_spec, P(), P(), row_spec, row_spec), out_specs=(P(), P(), P()), check_vma=False)
```

```python
import functools

import jax
import jax.numpy as jnp
from jax import lax
from jax.experimental import pallas as pl
from jax.experimental.pallas import tpu as pltpu
from jax.sharding import PartitionSpec as P

Y_DIM = 4
X_DIM = 4
CORES = 2
LANES = 128
NSUB = 4
NV = 4
NSEM = 44
BF = jnp.bfloat16
F32 = jnp.float32


def _step(dims, a_hbm, feat_hbm, lab_hbm, msk_hbm, w_one, w_two, dw1_out, dw2_out, loss_out,
          af, feat, lab, msk, mt, mtt, w1f, w2f, w1, w2, w2t, xs, xp, y1, cs, cr, sb, rb, z1, h1, y2, yp, zp, zr, g2, gr, dp, rc, rx, ry, ry2, rx2d,
          d2, dg, ms, mk, gz, gt, dy, rcy, rx1, rx2, wb, wc, wx, wy, wz, wf, oz, oy, ox, oc, pb, pc, px, pz, pf, qz, qy, qx, qxy, qyx,
          ssem, rsem, rsem_a, rsem_b, rsem_f, rsem_ring, rsem_ag, rsem_c, rsem_x):
    Z, Y, X, C, S, CB, H, F, NC = dims
    I = X * C
    NQ = Y * X
    HR = H // (2 * NSUB)
    HB = H // Y
    HU = HB // NV
    NCH = Y * S
    half = Z // 2
    rid = lax.axis_index("rep")
    nid = lax.axis_index("nodes")
    z, y, x, c = rid // Y, rid % Y, nid // C, nid % C
    chip = y * X + x
    partner = (rid, x * C + 1 - c)

    far = sorted(range(1, Z), key=lambda d: -min(d, Z - d))

    def at_z(zz):
        return (zz * Y + y, nid)

    def at_y(yy):
        return (z * Y + yy, nid)

    def at_x(xx):
        return (rid, xx * C + c)

    def at_chip(q):
        return (z * Y + q // X, (q % X) * C + c)

    def send(src, dst, ss, rs, dev):
        pltpu.make_async_remote_copy(src_ref=src, dst_ref=dst, send_sem=ss, recv_sem=rs, device_id=dev,
                                     device_id_type=pl.DeviceIdType.MESH).start()

    def arrived(ref, rs):
        pltpu.make_async_remote_copy(src_ref=ref, dst_ref=ref, send_sem=ssem.at[0], recv_sem=rs, device_id=partner,
                                     device_id_type=pl.DeviceIdType.MESH).wait_recv()

    def sent(ref, ss):
        pltpu.make_async_remote_copy(src_ref=ref, dst_ref=ref, send_sem=ss, recv_sem=rsem.at[0], device_id=partner,
                                     device_id_type=pl.DeviceIdType.MESH).wait_send()

    def dot(a, b):
        return jnp.dot(a, b, preferred_element_type=F32)

    def most(ref):
        return ref.at[0, pl.ds(0, NQ - 1)]

    def plane_rows(ref, yb):
        return jnp.stack([ref[k, yb * X:(yb + 1) * X] for k in range(C)], axis=1).reshape(CB, LANES)

    def added(ref, n):
        acc = ref[0]
        for k in range(1, n):
            acc = acc + ref[k]
        return acc

    (E_X, E_XC, E_A, E_B, E_F, E_RING, E_CNT, E_Y2, E_Y2C, E_Z2, E_G2, E_DC, E_DX, E_DY, E_AG, E_RC, E_RX, E_RX2,
     E_WC, E_WX, E_WY, E_WZ, E_OZ, E_OY, E_OX, E_OC, E_PC, E_PX, E_PZ, E_QZ, E_QY, E_QX, E_LA, E_L1, E_L2,
     E_M, E_DY2, E_DX2, E_DG, E_QXY, E_QYX, E_IN, E_IN1, E_IN2) = range(NSEM)

    load_a = pltpu.make_async_copy(a_hbm, af.at[y], ssem.at[E_LA])
    load_1 = pltpu.make_async_copy(w_one, w1f, ssem.at[E_L1])
    load_2 = pltpu.make_async_copy(w_two, w2f, ssem.at[E_L2])
    loads = [pltpu.make_async_copy(src, dst, ssem.at[E_IN + k]) for k, (src, dst) in
             enumerate(((feat_hbm, feat), (lab_hbm, lab), (msk_hbm, msk)))]
    for load in loads:
        load.start()
    load_a.start()
    load_1.start()
    load_2.start()

    bar = pltpu.get_barrier_semaphore()
    for d in far:
        pl.semaphore_signal(bar, inc=1, device_id=at_z((z + d) % Z), device_id_type=pl.DeviceIdType.MESH)

    def greet_plane(d, u):
        pl.semaphore_signal(bar, inc=1, device_id=at_chip(lax.rem(chip + d, NQ)), device_id_type=pl.DeviceIdType.MESH)
        return u

    lax.fori_loop(1, NQ, greet_plane, 0)
    pl.semaphore_signal(bar, inc=1, device_id=partner, device_id_type=pl.DeviceIdType.MESH)

    for load in loads:
        load.wait()
    mt[...] = jnp.zeros_like(mt)
    mt[0:F] = feat[...].astype(F32)
    mt[F:F + 1] = msk[...].astype(F32)
    mt[F + 1:F + 2] = lab[...].astype(F32)
    mtt[...] = mt[...].T
    xs[...] = mtt[...].astype(BF)
    pl.semaphore_wait(bar, NQ + Z - 1)

    def send_x(d, u):
        q = lax.rem(chip + d, NQ)
        send(xs, xp.at[c, chip], ssem.at[E_X], rsem.at[E_X], at_chip(q))
        return u

    lax.fori_loop(1, NQ, send_x, 0)
    xp[c, chip] = xs[...]
    load_a.wait()

    order = []
    for k in range(1, half + 1):
        order.append(-k)
        if k < half:
            order.append(k)
    order.append(0)
    for k in order:
        zc = (z + k + Z) % Z
        for d in (2, 1, 3):
            yq = (y + d) % Y
            send(af.at[y, zc, yq], af.at[y, zc, yq], ssem.at[E_A], rsem_a.at[d - 1, zc], at_y(yq))
    def spread_a(k):
        for d in (1, 3):
            yq = (y + d) % Y
            ya = (yq + k) % Y
            send(af.at[y, :, ya], af.at[y, :, ya], ssem.at[E_B], rsem_b.at[d // 2, k - 1], at_y(yq))

    def forward_a():
        for k in range(1, Y):
            for d in (1, 3):
                arrived(af.at[0, :, 0], rsem_b.at[d // 2, k - 1])
        for k in range(1, Y):
            for d in (1, 3):
                ys, yq = (y - d + Y) % Y, (y + d) % Y
                lo = 0 if d == 1 else half
                ya = (yq + k) % Y
                send(af.at[ys, pl.ds(lo, half), ya], af.at[ys, pl.ds(lo, half), ya], ssem.at[E_F], rsem_f.at[d // 2, k - 1], at_y(yq))

    spread_a(1)
    spread_a(2)

    load_1.wait()
    w1[...] = jnp.zeros_like(w1)
    w1[0:F] = w1f[...].astype(BF)
    load_2.wait()
    w2[...] = jnp.zeros_like(w2)
    for k in range(Y):
        rows = slice(k * HB, (k + 1) * HB)
        w2[rows, 0:NC] = w2f[rows].astype(BF)
        w2t[:, rows] = w2[rows].T

    arrived(most(xp), rsem.at[E_X])
    send(xp.at[c], xp.at[c], ssem.at[E_XC], rsem.at[E_XC], partner)
    arrived(xp.at[0], rsem.at[E_XC])

    def wait_a(zc):
        for d in range(1, Y):
            arrived(af.at[0, 0, 0], rsem_a.at[d - 1, zc])

    def columns(j):
        return pl.ds(pl.multiple_of(j * HR, HR), HR)

    def products(s, j):
        up = j % 2 == 0
        dest = lax.rem(jnp.where(up, z - 1 - s, z + 1 + s) + 2 * Z, Z)
        fresh = ((j == 0) & ((s < half) | (s == Z - 1))) | ((j == 1) & (s < half - 1))

        @pl.when(fresh)
        def _():
            wait_a(dest)

        acc = dot(af[0, dest, y], y1[pl.ds(0, CB), columns(j)])
        for yb in range(1, Y):
            acc = acc + dot(af[yb, dest, y], y1[pl.ds(yb * CB, CB), columns(j)])
        return acc

    def pass_on(s, j):
        nb = lax.rem(jnp.where(j % 2 == 0, z + 1, z - 1) + Z, Z)
        send(sb.at[j, s], rb.at[j, s], ssem.at[E_RING], rsem_ring.at[j, s], at_z(nb))

    def ring_first(j, u):
        for yb in range(Y):
            y1[yb * CB:(yb + 1) * CB, columns(j)] = dot(plane_rows(xp, yb), w1[:, columns(j)]).astype(BF)
        sb[j, 0] = products(0, j)
        pass_on(0, j)
        return u

    def ring_next(t, u):
        s, j = t // (2 * NSUB) + 1, t % (2 * NSUB)
        acc = products(s, j)
        arrived(rb.at[0, 0], rsem_ring.at[j, s - 1])
        sb[j, s] = acc + rb[j, s - 1]
        pass_on(s, j)
        return u

    def ring_last(j, u):
        acc = products(Z - 1, j)
        arrived(rb.at[0, 0], rsem_ring.at[j, Z - 2])
        z1[:, columns(j)] = acc + rb[j, Z - 2]
        return u

    lax.fori_loop(0, 2 * NSUB, ring_first, 0)
    lax.fori_loop(0, (Z - 2) * 2 * NSUB, ring_next, 0)
    lax.fori_loop(0, 2 * NSUB, ring_last, 0)

    h1[...] = jnp.maximum(z1[...], 0.0).astype(BF)
    y2[...] = dot(h1[...], w2[...]).astype(BF)

    def send_y2(d, u):
        q = lax.rem(chip + d, NQ)
        send(y2, yp.at[c, chip], ssem.at[E_Y2], rsem.at[E_Y2], at_chip(q))
        return u

    lax.fori_loop(1, NQ, send_y2, 0)
    yp[c, chip] = y2[...]
    lane = lax.broadcasted_iota(jnp.int32, (S, LANES), 1)
    counted = jnp.sum(xp[...].astype(F32).reshape(Y * CB, LANES), axis=0, keepdims=True)
    counted = jnp.sum(jnp.where(lane[0:1] == F, counted, 0.0), axis=1, keepdims=True)
    cs[...] = jnp.broadcast_to(counted, (8, LANES))
    cr[z] = cs[...]
    for d in far:
        send(cs, cr.at[z], ssem.at[E_CNT], rsem.at[E_CNT], at_z((z + d) % Z))
    arrived(most(yp), rsem.at[E_Y2])
    send(yp.at[c], yp.at[c], ssem.at[E_Y2C], rsem.at[E_Y2C], partner)
    arrived(yp.at[0], rsem.at[E_Y2C])
    for yb in range(Y):
        ms[yb] = jnp.where(z1[:, yb * HB:(yb + 1) * HB] > 0.0, 1.0, 0.0).astype(BF)
    for yb in range(Y):
        part = dot(af[yb, :, y].reshape(Z * S, CB), plane_rows(yp, yb)).reshape(Z, S, LANES)
        zp[...] = part if yb == 0 else zp[...] + part
    for d in far:
        zq = (z + d) % Z
        send(zp.at[zq], zr.at[z], ssem.at[E_Z2], rsem.at[E_Z2], at_z(zq))
    zr[z] = zp[z]
    for d in (2, 1, 3):
        yq = (y + d) % Y
        send(ms.at[yq], mk.at[y], ssem.at[E_M], rsem.at[E_M], at_y(yq))
    mk[y] = ms[y]
    spread_a(3)
    arrived(zr.at[pl.ds(0, Z - 1)], rsem.at[E_Z2])
    z2 = added(zr, Z)

    arrived(cr.at[pl.ds(0, Z - 1)], rsem.at[E_CNT])
    count = added(cr, Z)[0:1, 0:1]
    own = mtt[...]
    weights = jnp.sum(jnp.where(lane == F, own, 0.0), axis=1, keepdims=True)
    labels = jnp.sum(jnp.where(lane == F + 1, own, 0.0), axis=1, keepdims=True)
    real = lane < NC
    top = jnp.max(jnp.where(real, z2, -jnp.inf), axis=1, keepdims=True)
    shifted = jnp.where(real, z2 - top, 0.0)
    log_probs = shifted - jnp.log(jnp.sum(jnp.where(real, jnp.exp(shifted), 0.0), axis=1, keepdims=True))
    hot = labels == lane.astype(F32)
    picked = jnp.sum(jnp.where(hot, log_probs, 0.0), axis=1, keepdims=True)
    loss_part = -jnp.sum(weights * picked, axis=0, keepdims=True)
    diff = jnp.where(real, jnp.exp(log_probs), 0.0) - hot.astype(F32)
    g2[...] = (diff * (weights / count)).astype(BF)
    for d in far:
        send(g2, gr.at[z], ssem.at[E_G2], rsem.at[E_G2], at_z((z + d) % Z))
    gr[z] = g2[...]
    arrived(gr.at[pl.ds(0, Z - 1)], rsem.at[E_G2])

    g2t = gr[...].reshape(Z * S, LANES).T
    for yb in range(Y):
        part = dot(g2t, af[yb, :, y].reshape(Z * S, CB))
        dp[yb] = part.T.reshape(X, C, S, LANES)
    send(dp.at[:, :, 1 - c], rc, ssem.at[E_DC], rsem.at[E_DC], partner)
    arrived(rc, rsem.at[E_DC])
    rc[...] = rc[...] + dp[:, :, c]
    sh = S // 2
    for d in (2, 1, 3):
        xq, yq = (x + d) % X, (y + d) % Y
        send(rc.at[:, xq, pl.ds(0, sh)], rx.at[x], ssem.at[E_DX], rsem.at[E_DX], at_x(xq))
        send(rc.at[yq, :, pl.ds(sh, sh)], ry.at[y], ssem.at[E_DY], rsem.at[E_DY], at_y(yq))
    rx[x] = rc[:, x, 0:sh]
    ry[y] = rc[y, :, sh:S]
    arrived(rx.at[pl.ds(0, X - 1)], rsem.at[E_DX])
    rx[x] = added(rx, X)
    for d in (2, 1, 3):
        yq = (y + d) % Y
        send(rx.at[x, yq], ry2.at[y], ssem.at[E_DY2], rsem.at[E_DY2], at_y(yq))
    ry2[y] = rx[x, y]
    arrived(ry.at[pl.ds(0, Y - 1)], rsem.at[E_DY])
    ry[y] = added(ry, Y)
    for d in (2, 1, 3):
        xq = (x + d) % X
        send(ry.at[y, xq], rx2d.at[x], ssem.at[E_DX2], rsem.at[E_DX2], at_x(xq))
    rx2d[x] = ry[y, x]
    arrived(ry2.at[pl.ds(0, Y - 1)], rsem.at[E_DY2])
    arrived(rx2d.at[pl.ds(0, X - 1)], rsem.at[E_DX2])
    d2[0:sh] = added(ry2, Y).astype(BF)
    d2[sh:S] = added(rx2d, X).astype(BF)
    for d in (2, 1, 3):
        send(d2, dg.at[y], ssem.at[E_DG], rsem.at[E_DG], at_y((y + d) % Y))
    dg[y] = d2[...]
    forward_a()
    dy2 = d2[...]

    def g_one(v):
        col = pl.multiple_of(y * HB + v * HU, HU)
        dh = dot(dg[...].reshape(Y * S, LANES), w2t[:, pl.ds(col, HU)])
        keep = mk[:, :, v * HU:(v + 1) * HU].reshape(Y * S, HU).astype(F32)
        gz[v, z] = jnp.where(keep > 0.0, dh, 0.0).astype(BF).reshape(Y, S, HU)

    def gather_step(v, t):
        for d in range(2):
            sgn = 1 if d == 0 else -1
            blk = (z - sgn * (t - 1) + Z) % Z
            if t > 1:
                arrived(gz.at[v, 0], rsem_ag.at[v, d, t - 1])
            ref = gz.at[v, blk] if t < half else gz.at[v, blk, pl.ds(d * (Y // 2), Y // 2)]
            send(ref, ref, ssem.at[E_AG], rsem_ag.at[v, d, t], at_z((z + sgn + Z) % Z))

    def piece(v):
        return pl.ds(v % 2 * HU, HU)

    def prepare(p):
        for v in (2 * p, 2 * p + 1):
            for d in range(2):
                arrived(gz.at[v, 0, pl.ds(0, Y // 2)], rsem_ag.at[v, d, half])
            for k in range(Z):
                gt[p, piece(v), k * Y * S:(k + 1) * Y * S] = gz[v, k].reshape(Y * S, HU).T

    def chunks(p, lo, hi):
        def chunk(n, u):
            k = n % Y
            core = jnp.where(n < Y, 1 - c, c)
            yb = lax.rem(y + k + jnp.where(k == 2, 1, 0) - jnp.where(k == 3, 1, 0), Y)
            off = pl.multiple_of(core * NCH, NCH)
            dy[p, yb, core] = dot(gt[p], af[yb, :, :, :, pl.ds(off, NCH)].reshape(Z * Y * S, NCH))
            return u

        if p == 0 and lo < Y <= hi:
            lax.fori_loop(lo, Y - 1, chunk, 0)
            for d in (1, 3):
                for k in range(1, Y):
                    arrived(af.at[0, pl.ds(0, half), 0], rsem_f.at[d // 2, k - 1])
            lo = Y - 1
        lax.fori_loop(lo, hi, chunk, 0)

    def send_core(p):
        for v in (2 * p, 2 * p + 1):
            send(dy.at[p, :, 1 - c, piece(v)], rcy.at[p, :, piece(v)], ssem.at[E_RC], rsem_c.at[v], partner)

    nxt, prv, opp = (x + 1) % X, (x + X - 1) % X, (x + 2) % X
    hh = HU // 2

    def low(v):
        return pl.ds(v % 2 * HU, hh)

    def high(v):
        return pl.ds(v % 2 * HU + hh, hh)

    def reduce_core(v):
        p = v // 2
        arrived(rcy.at[p, :, piece(v)], rsem_c.at[v])
        for k in range(X):
            rcy[p, k, piece(v)] = rcy[p, k, piece(v)] + dy[p, k, c, piece(v)]
        send(rcy.at[p, opp, low(v)], rx1.at[v, 0], ssem.at[E_RX], rsem_x.at[v, 0], at_x(nxt))
        send(rcy.at[p, opp, high(v)], rx1.at[v, 1], ssem.at[E_RX], rsem_x.at[v, 1], at_x(prv))

    def reduce_x(v):
        p = v // 2
        arrived(rx1.at[v, 0], rsem_x.at[v, 0])
        rcy[p, nxt, low(v)] = rcy[p, nxt, low(v)] + rx1[v, 0]
        send(rcy.at[p, nxt, piece(v)], rx2.at[v, 0], ssem.at[E_RX2], rsem_x.at[v, 2], at_x(nxt))
        arrived(rx1.at[v, 1], rsem_x.at[v, 1])
        rcy[p, prv, high(v)] = rcy[p, prv, high(v)] + rx1[v, 1]
        send(rcy.at[p, prv, piece(v)], rx2.at[v, 1], ssem.at[E_RX2], rsem_x.at[v, 3], at_x(prv))

    def own_x():
        return jnp.concatenate([xp[m % C, nid * (Y // C) + m // C] for m in range(Y)], axis=0)

    def grad_one(v):
        arrived(rx2.at[v, 0], rsem_x.at[v, 2])
        arrived(rx2.at[v, 1], rsem_x.at[v, 3])
        acc = (rcy[v // 2, x, piece(v)] + rx2[v, 0] + rx2[v, 1]).astype(BF)
        part = dot(acc, own_x())
        if v >= NV // 2:
            part = jnp.concatenate([part[:, LANES // 2:], part[:, 0:LANES // 2]], axis=1)
        per = HU // (Z * 8)
        rows = part.reshape(per, Z, 8, LANES)
        for m in range(per):
            k = (v % (NV // 2)) * per + m
            pb[k] = rows[m] if v < NV // 2 else pb[k] + rows[m]

    def w_begin():
        mark = (lax.broadcasted_iota(jnp.int32, (HB, LANES), 0) == 0) & (lax.broadcasted_iota(jnp.int32, (HB, LANES), 1) == NC)
        for k in range(Y):
            part = lax.dot_general(h1[:, k * HB:(k + 1) * HB], dy2, (((0,), (0,)), ((), ())), preferred_element_type=F32)
            if k == 0:
                part = jnp.where(mark, loss_part, part)
            per = HB // (Y * Z * 8)
            rows = part.reshape(per, Y, Z, 8, LANES)
            for m in range(per):
                q = k * per + m
                wb[q // X, q % X] = rows[m]
        send(wb.at[1 - c], wc, ssem.at[E_WC], rsem.at[E_WC], partner)

    def w_core():
        arrived(wc, rsem.at[E_WC])
        wc[...] = wc[...] + wb[c]
        for d in (2, 1, 3):
            xq = (x + d) % X
            send(wc.at[xq], wx.at[x], ssem.at[E_WX], rsem.at[E_WX], at_x(xq))
        wx[x] = wc[x]

    def w_x():
        arrived(wx.at[pl.ds(0, X - 1)], rsem.at[E_WX])
        wx[x] = added(wx, X)
        for d in (2, 1, 3):
            yq = (y + d) % Y
            send(wx.at[x, yq], wy.at[y], ssem.at[E_WY], rsem.at[E_WY], at_y(yq))
        wy[y] = wx[x, y]

    def w_y():
        arrived(wy.at[pl.ds(0, Y - 1)], rsem.at[E_WY])
        wy[y] = added(wy, Y)
        for d in far:
            zq = (z + d) % Z
            send(wy.at[y, zq], wz.at[z], ssem.at[E_WZ], rsem.at[E_WZ], at_z(zq))
        wz[z] = wy[y, z]

    def w_z():
        arrived(wz.at[pl.ds(0, Z - 1)], rsem.at[E_WZ])
        wf[...] = added(wz, Z)
        for d in far:
            send(wf, oz.at[z], ssem.at[E_OZ], rsem.at[E_OZ], at_z((z + d) % Z))
        oz[z] = wf[...]

    def o_z():
        arrived(oz.at[pl.ds(0, Z - 1)], rsem.at[E_OZ])
        for d in (2, 1, 3):
            send(oz, oy.at[y], ssem.at[E_OY], rsem.at[E_OY], at_y((y + d) % Y))
        oy[y] = oz[...]

    def o_y():
        arrived(oy.at[pl.ds(0, Y - 1)], rsem.at[E_OY])
        for d in (2, 1, 3):
            send(oy, ox.at[x], ssem.at[E_OX], rsem.at[E_OX], at_x((x + d) % X))
        ox[x] = oy[...]

    def o_x():
        arrived(ox.at[pl.ds(0, X - 1)], rsem.at[E_OX])
        send(ox, oc.at[c], ssem.at[E_OC], rsem.at[E_OC], partner)
        oc[c] = ox[...]

    arrived(mk.at[pl.ds(0, Y - 1)], rsem.at[E_M])
    arrived(dg.at[pl.ds(0, Y - 1)], rsem.at[E_DG])
    steps = [
        (g_one, 0), (gather_step, 0, 1), (g_one, 1), (gather_step, 1, 1), (g_one, 2), (g_one, 3), (w_begin,),
        (gather_step, 0, 2), (gather_step, 1, 2), (w_core,)]
    for t in range(3, half + 1):
        steps += [(gather_step, 0, t), (gather_step, 1, t)]
    steps += [(gather_step, 2, 1), (gather_step, 3, 1), (prepare, 0), (chunks, 0, 0, 2), (gather_step, 2, 2), (gather_step, 3, 2),
              (chunks, 0, 2, 4), (send_core, 0), (chunks, 0, 4, 6)]
    for t in range(3, half + 1):
        steps += [(gather_step, 2, t), (gather_step, 3, t)]
        if t == 3:
            steps += [(chunks, 0, 6, 8), (w_x,), (reduce_core, 0), (reduce_core, 1)]
    steps += [(reduce_x, 0), (reduce_x, 1), (w_y,), (prepare, 1), (chunks, 1, 0, 4), (send_core, 1), (chunks, 1, 4, 8), (reduce_core, 2),
              (reduce_core, 3), (grad_one, 0), (grad_one, 1), (w_z,), (reduce_x, 2), (reduce_x, 3), (o_z,), (grad_one, 2), (grad_one, 3)]
    for step in steps:
        step[0](*step[1:])

    send(pb, pc, ssem.at[E_PC], rsem.at[E_PC], partner)
    arrived(pc, rsem.at[E_PC])
    pc[...] = pc[...] + pb[...]
    for d in (2, 1, 3):
        xq = (x + d) % X
        send(pc.at[xq], px.at[x], ssem.at[E_PX], rsem.at[E_PX], at_x(xq))
    px[x] = pc[x]
    o_y()
    arrived(px.at[pl.ds(0, X - 1)], rsem.at[E_PX])
    px[x] = added(px, X)
    for d in far:
        zq = (z + d) % Z
        send(px.at[x, zq], pz.at[z], ssem.at[E_PZ], rsem.at[E_PZ], at_z(zq))
    pz[z] = px[x, z]
    arrived(pz.at[pl.ds(0, Z - 1)], rsem.at[E_PZ])
    pf[...] = added(pz, Z)
    for d in far:
        send(pf, qz.at[z], ssem.at[E_QZ], rsem.at[E_QZ], at_z((z + d) % Z))
    qz[z] = pf[...]
    o_x()
    arrived(qz.at[pl.ds(0, Z - 1)], rsem.at[E_QZ])
    zl, zh = pl.ds(0, half), pl.ds(half, half)
    for d in (2, 1, 3):
        send(qz.at[zl], qy.at[y], ssem.at[E_QY], rsem.at[E_QY], at_y((y + d) % Y))
        send(qz.at[zh], qx.at[x], ssem.at[E_QX], rsem.at[E_QX], at_x((x + d) % X))
    qy[y] = qz[zl]
    qx[x] = qz[zh]
    arrived(oc.at[0], rsem.at[E_OC])
    for k in range(C):
        full = oc[k].reshape(H // C, LANES)
        dw2_out[k * (H // C):(k + 1) * (H // C), :] = full[:, 0:NC]
        if k == 0:
            loss_out[...] = jnp.broadcast_to(full[0:1, NC:NC + 1] / count, (8, LANES))
    arrived(qy.at[pl.ds(0, Y - 1)], rsem.at[E_QY])
    for d in (2, 1, 3):
        send(qy, qxy.at[x], ssem.at[E_QXY], rsem.at[E_QXY], at_x((x + d) % X))
    qxy[x] = qy[...]
    arrived(qx.at[pl.ds(0, X - 1)], rsem.at[E_QX])
    for d in (2, 1, 3):
        send(qx, qyx.at[y], ssem.at[E_QYX], rsem.at[E_QYX], at_y((y + d) % Y))
    qyx[y] = qx[...]
    arrived(qxy.at[pl.ds(0, X - 1)], rsem.at[E_QXY])
    arrived(qyx.at[pl.ds(0, Y - 1)], rsem.at[E_QYX])
    for yb in range(Y):
        part = jnp.concatenate([qxy[:, yb], qyx[yb]], axis=1).reshape(HB // 2, LANES).T
        dw1_out[:, yb * HB:yb * HB + HB // 2] = part[0:F]
        dw1_out[:, yb * HB + HB // 2:(yb + 1) * HB] = part[LANES // 2:LANES // 2 + F]

    sent(most(xp), ssem.at[E_X])
    sent(xp.at[0], ssem.at[E_XC])
    sent(af.at[pl.ds(0, Y - 1), :, 0], ssem.at[E_A])
    sent(af.at[pl.ds(0, Y - 1), :, pl.ds(0, 2)], ssem.at[E_B])
    sent(af.at[pl.ds(0, Y - 1), :, 0], ssem.at[E_F])
    sent(sb, ssem.at[E_RING])
    sent(cr.at[pl.ds(0, Z - 1)], ssem.at[E_CNT])
    sent(most(yp), ssem.at[E_Y2])
    sent(yp.at[0], ssem.at[E_Y2C])
    sent(zr.at[pl.ds(0, Z - 1)], ssem.at[E_Z2])
    sent(gr.at[pl.ds(0, Z - 1)], ssem.at[E_G2])
    sent(rc, ssem.at[E_DC])
    sent(rx.at[pl.ds(0, X - 1)], ssem.at[E_DX])
    sent(ry.at[pl.ds(0, Y - 1)], ssem.at[E_DY])
    sent(ry2.at[pl.ds(0, Y - 1)], ssem.at[E_DY2])
    sent(rx2d.at[pl.ds(0, X - 1)], ssem.at[E_DX2])
    sent(dg.at[pl.ds(0, Y - 1)], ssem.at[E_DG])
    sent(mk.at[pl.ds(0, Y - 1)], ssem.at[E_M])
    sent(gz.at[:, pl.ds(0, Z - 1)], ssem.at[E_AG])
    sent(rcy, ssem.at[E_RC])
    sent(rx1, ssem.at[E_RX])
    sent(rx2, ssem.at[E_RX2])
    sent(wc, ssem.at[E_WC])
    sent(wx.at[pl.ds(0, X - 1)], ssem.at[E_WX])
    sent(wy.at[pl.ds(0, Y - 1)], ssem.at[E_WY])
    sent(wz.at[pl.ds(0, Z - 1)], ssem.at[E_WZ])
    sent(oz.at[pl.ds(0, Z - 1)], ssem.at[E_OZ])
    sent(oy.at[pl.ds(0, Y - 1)], ssem.at[E_OY])
    sent(ox.at[pl.ds(0, X - 1)], ssem.at[E_OX])
    sent(oc.at[0], ssem.at[E_OC])
    sent(pc, ssem.at[E_PC])
    sent(px.at[pl.ds(0, X - 1)], ssem.at[E_PX])
    sent(pz.at[pl.ds(0, Z - 1)], ssem.at[E_PZ])
    sent(qz.at[pl.ds(0, Z - 1)], ssem.at[E_QZ])
    sent(qy.at[pl.ds(0, Y - 1)], ssem.at[E_QY])
    sent(qx.at[pl.ds(0, X - 1)], ssem.at[E_QX])
    sent(qxy.at[pl.ds(0, X - 1)], ssem.at[E_QXY])
    sent(qyx.at[pl.ds(0, Y - 1)], ssem.at[E_QYX])


def solution(mesh):
    Y, X, C = Y_DIM, X_DIM, CORES
    Z = mesh.shape["rep"] // Y
    row_spec = P(("rep", "nodes"))

    def device_step(adj_blk, feat_blk, w_one, w_two, label_blk, mask_blk):
        R, S, CB = adj_blk.shape
        F, H = w_one.shape
        NC = w_two.shape[1]
        I = X * C
        NQ = Y * X
        HR = H // (2 * NSUB)
        HB = H // Y
        HU = HB // NV
        NCH = Y * S
        assert R == Z * Y and CB == S * I and X == Y and F + 2 <= LANES // 2 and NC < LANES
        vm = pltpu.VMEM
        dma = pltpu.SemaphoreType.DMA
        scratch = [
            vm((Y, Z, Y, S, CB), BF),
            vm((F, S), BF),
            vm((1, S), jnp.int32),
            vm((1, S), jnp.int32),
            vm((LANES, S), F32),
            vm((S, LANES), F32),
            vm((F, H), F32),
            vm((H, NC), F32),
            vm((LANES, H), BF),
            vm((H, LANES), BF),
            vm((LANES, H), BF),
            vm((S, LANES), BF),
            vm((C, NQ, S, LANES), BF),
            vm((Y * CB, H), BF),
            vm((8, LANES), F32),
            vm((Z, 8, LANES), F32),
            vm((2 * NSUB, Z - 1, S, HR), F32),
            vm((2 * NSUB, Z - 1, S, HR), F32),
            vm((S, H), F32),
            vm((S, H), BF),
            vm((S, LANES), BF),
            vm((C, NQ, S, LANES), BF),
            vm((Z, S, LANES), F32),
            vm((Z, S, LANES), F32),
            vm((S, LANES), BF),
            vm((Z, S, LANES), BF),
            vm((Y, X, C, S, LANES), F32),
            vm((Y, X, S, LANES), F32),
            vm((X, Y, S // 2, LANES), F32),
            vm((Y, X, S // 2, LANES), F32),
            vm((Y, S // 2, LANES), F32),
            vm((X, S // 2, LANES), F32),
            vm((S, LANES), BF),
            vm((Y, S, LANES), BF),
            vm((Y, S, HB), BF),
            vm((Y, S, HB), BF),
            vm((NV, Z, Y, S, HU), BF),
            vm((NV // 2, 2 * HU, Z * Y * S), BF),
            vm((NV // 2, X, C, 2 * HU, NCH), F32),
            vm((NV // 2, X, 2 * HU, NCH), F32),
            vm((NV, 2, HU // 2, NCH), F32),
            vm((NV, 2, HU, NCH), F32),
            vm((C, X, Y, Z, 8, LANES), F32),
            vm((X, Y, Z, 8, LANES), F32),
            vm((X, Y, Z, 8, LANES), F32),
            vm((Y, Z, 8, LANES), F32),
            vm((Z, 8, LANES), F32),
            vm((8, LANES), F32),
            vm((Z, 8, LANES), F32),
            vm((Y, Z, 8, LANES), F32),
            vm((X, Y, Z, 8, LANES), F32),
            vm((C, X, Y, Z, 8, LANES), F32),
            vm((X, Z, 8, LANES), F32),
            vm((X, Z, 8, LANES), F32),
            vm((X, Z, 8, LANES), F32),
            vm((Z, 8, LANES), F32),
            vm((8, LANES), F32),
            vm((Z, 8, LANES), F32),
            vm((Y, Z // 2, 8, LANES), F32),
            vm((X, Z // 2, 8, LANES), F32),
            vm((X, Y, Z // 2, 8, LANES), F32),
            vm((Y, X, Z // 2, 8, LANES), F32),
            dma((NSEM,)),
            dma((NSEM,)),
            dma((Y - 1, Z)),
            dma((2, Y - 1)),
            dma((2, Y - 1)),
            dma((2 * NSUB, Z - 1)),
            dma((NV, 2, Z // 2 + 1)),
            dma((NV,)),
            dma((NV, 4)),
        ]
        vspec = pl.BlockSpec(memory_space=pltpu.VMEM)
        aspec = pl.BlockSpec(memory_space=pltpu.HBM)
        dw_one, dw_two, loss = pl.pallas_call(
            functools.partial(_step, (Z, Y, X, C, S, CB, H, F, NC)),
            out_shape=(jax.ShapeDtypeStruct((F, H), F32), jax.ShapeDtypeStruct((H, NC), F32), jax.ShapeDtypeStruct((8, LANES), F32)),
            in_specs=[aspec] * 6,
            out_specs=(vspec, vspec, vspec),
            scratch_shapes=scratch,
            compiler_params=pltpu.CompilerParams(collective_id=0, has_side_effects=True, vmem_limit_bytes=52 * 1024 * 1024),
            name="gcn_step",
        )(adj_blk.reshape(Z, Y, S, CB), feat_blk.T, label_blk[None, :], mask_blk[None, :], w_one, w_two)
        return loss[0, 0], dw_one, dw_two

    return jax.shard_map(device_step, mesh=mesh, in_specs=(P(None, "nodes", "rep"), row_spec, P(), P(), row_spec, row_spec), out_specs=(P(), P(), P()), check_vma=False)
```

```python
import functools

import jax
import jax.numpy as jnp
from jax import lax
from jax.experimental import pallas as pl
from jax.experimental.pallas import tpu as pltpu
from jax.sharding import PartitionSpec as P

Y_DIM = 4
X_DIM = 4
CORES = 2
LANES = 128
NSUB = 4
NV = 4
NSEM = 46
BF = jnp.bfloat16
F32 = jnp.float32


def _step(dims, a_hbm, feat_hbm, lab_hbm, msk_hbm, w_one, w_two, dw1_out, dw2_out, loss_out,
          af, feat, lab, msk, mt, mtt, w1f, w2f, w1, w2, w2t, xs, xp, y1, cs, cr, sb, rb, z1, h1, y2, yp, zp, zr, g2, gr, dp, rc, rx, ry, ry2, rx2d,
          d2, dg, ms, mk, gz, gt, dy, rcy, rx1, rx2, wb, wc, wx, wy, wz, wf, oz, oy, ox, oc, pb, px, pz, pf, qz, qy, qx, qxy, qyx,
          ssem, rsem, rsem_a, rsem_b, rsem_f, rsem_ring, rsem_ag, rsem_c, rsem_x):
    Z, Y, X, C, S, CB, H, F, NC = dims
    I = X * C
    NQ = Y * X
    HR = H // (2 * NSUB)
    HB = H // Y
    HU = HB // NV
    NCH = Y * S
    half = Z // 2
    rid = lax.axis_index("rep")
    nid = lax.axis_index("nodes")
    z, y, x, c = rid // Y, rid % Y, nid // C, nid % C
    chip = y * X + x
    partner = (rid, x * C + 1 - c)

    far = sorted(range(1, Z), key=lambda d: -min(d, Z - d))

    def at_z(zz):
        return (zz * Y + y, nid)

    def at_y(yy):
        return (z * Y + yy, nid)

    def at_x(xx):
        return (rid, xx * C + c)

    def at_chip(q):
        return (z * Y + q // X, (q % X) * C + c)

    def send(src, dst, ss, rs, dev):
        pltpu.make_async_remote_copy(src_ref=src, dst_ref=dst, send_sem=ss, recv_sem=rs, device_id=dev,
                                     device_id_type=pl.DeviceIdType.MESH).start()

    def arrived(ref, rs):
        pltpu.make_async_remote_copy(src_ref=ref, dst_ref=ref, send_sem=ssem.at[0], recv_sem=rs, device_id=partner,
                                     device_id_type=pl.DeviceIdType.MESH).wait_recv()

    def sent(ref, ss):
        pltpu.make_async_remote_copy(src_ref=ref, dst_ref=ref, send_sem=ss, recv_sem=rsem.at[0], device_id=partner,
                                     device_id_type=pl.DeviceIdType.MESH).wait_send()

    def dot(a, b):
        return jnp.dot(a, b, preferred_element_type=F32)

    def most(ref):
        return ref.at[0, pl.ds(0, NQ - 1)]

    def plane_rows(ref, yb):
        return jnp.stack([ref[k, yb * X:(yb + 1) * X] for k in range(C)], axis=1).reshape(CB, LANES)

    def added(ref, n):
        acc = ref[0]
        for k in range(1, n):
            acc = acc + ref[k]
        return acc

    (E_X, E_XC, E_A, E_B, E_F, E_RING, E_CNT, E_Y2, E_Y2C, E_Z2, E_G2, E_DC, E_DC1, E_DC2, E_DC3, E_DX, E_DY, E_AG, E_RC, E_RX, E_RX2,
     E_WC, E_WX, E_WY, E_WZ, E_OZ, E_OY, E_OX, E_OC, E_PX, E_PZ, E_QZ, E_QY, E_QX, E_LA, E_L1, E_L2,
     E_M, E_DY2, E_DX2, E_DG, E_QXY, E_QYX, E_IN, E_IN1, E_IN2) = range(NSEM)

    load_a = pltpu.make_async_copy(a_hbm, af.at[y], ssem.at[E_LA])
    load_1 = pltpu.make_async_copy(w_one, w1f, ssem.at[E_L1])
    load_2 = pltpu.make_async_copy(w_two, w2f, ssem.at[E_L2])
    loads = [pltpu.make_async_copy(src, dst, ssem.at[E_IN + k]) for k, (src, dst) in
             enumerate(((feat_hbm, feat), (lab_hbm, lab), (msk_hbm, msk)))]
    for load in loads:
        load.start()
    load_a.start()
    load_1.start()
    load_2.start()

    bar = pltpu.get_barrier_semaphore()
    for d in far:
        pl.semaphore_signal(bar, inc=1, device_id=at_z((z + d) % Z), device_id_type=pl.DeviceIdType.MESH)

    def greet_plane(d, u):
        pl.semaphore_signal(bar, inc=1, device_id=at_chip(lax.rem(chip + d, NQ)), device_id_type=pl.DeviceIdType.MESH)
        return u

    lax.fori_loop(1, NQ, greet_plane, 0)
    pl.semaphore_signal(bar, inc=1, device_id=partner, device_id_type=pl.DeviceIdType.MESH)

    for load in loads:
        load.wait()
    mt[...] = jnp.zeros_like(mt)
    mt[0:F] = feat[...].astype(F32)
    mt[F:F + 1] = msk[...].astype(F32)
    mt[F + 1:F + 2] = lab[...].astype(F32)
    mtt[...] = mt[...].T
    xs[...] = mtt[...].astype(BF)
    pl.semaphore_wait(bar, NQ + Z - 1)

    def send_x(d, u):
        q = lax.rem(chip + d, NQ)
        send(xs, xp.at[c, chip], ssem.at[E_X], rsem.at[E_X], at_chip(q))
        return u

    lax.fori_loop(1, NQ, send_x, 0)
    xp[c, chip] = xs[...]
    load_a.wait()

    order = []
    for k in range(1, half + 1):
        order.append(-k)
        if k < half:
            order.append(k)
    order.append(0)
    for k in order:
        zc = (z + k + Z) % Z
        for d in (2, 1, 3):
            yq = (y + d) % Y
            send(af.at[y, zc, yq], af.at[y, zc, yq], ssem.at[E_A], rsem_a.at[d - 1, zc], at_y(yq))
    def spread_a(k):
        for d in (1, 3):
            yq = (y + d) % Y
            ya = (yq + k) % Y
            send(af.at[y, :, ya], af.at[y, :, ya], ssem.at[E_B], rsem_b.at[d // 2, k - 1], at_y(yq))

    def forward_a():
        for k in range(1, Y):
            for d in (1, 3):
                arrived(af.at[0, :, 0], rsem_b.at[d // 2, k - 1])
        for k in range(1, Y):
            for d in (1, 3):
                ys, yq = (y - d + Y) % Y, (y + d) % Y
                lo = 0 if d == 1 else half
                ya = (yq + k) % Y
                send(af.at[ys, pl.ds(lo, half), ya], af.at[ys, pl.ds(lo, half), ya], ssem.at[E_F], rsem_f.at[d // 2, k - 1], at_y(yq))

    spread_a(1)
    spread_a(2)

    load_1.wait()
    w1[...] = jnp.zeros_like(w1)
    w1[0:F] = w1f[...].astype(BF)
    load_2.wait()
    w2[...] = jnp.zeros_like(w2)
    for k in range(Y):
        rows = slice(k * HB, (k + 1) * HB)
        w2[rows, 0:NC] = w2f[rows].astype(BF)
        w2t[:, rows] = w2[rows].T

    arrived(most(xp), rsem.at[E_X])
    send(xp.at[c], xp.at[c], ssem.at[E_XC], rsem.at[E_XC], partner)

    def columns(j):
        return pl.ds(pl.multiple_of(j * HR, HR), HR)

    def y1_half(k, j):
        y1[:, k, :, columns(j)] = dot(xp[k].reshape(NQ * S, LANES), w1[:, columns(j)]).astype(BF).reshape(NQ, S, HR)

    def y1_own(j, u):
        y1_half(c, j)
        return u

    def y1_block(yb, j):
        return y1[yb * X:(yb + 1) * X, :, :, columns(j)].reshape(CB, HR)

    lax.fori_loop(0, 2 * NSUB, y1_own, 0)
    arrived(xp.at[0], rsem.at[E_XC])

    def wait_a(zc):
        for d in range(1, Y):
            arrived(af.at[0, 0, 0], rsem_a.at[d - 1, zc])

    def products(s, j):
        up = j % 2 == 0
        dest = lax.rem(jnp.where(up, z - 1 - s, z + 1 + s) + 2 * Z, Z)
        fresh = ((j == 0) & ((s < half) | (s == Z - 1))) | ((j == 1) & (s < half - 1))

        @pl.when(fresh)
        def _():
            wait_a(dest)

        acc = dot(af[0, dest, y], y1_block(0, j))
        for yb in range(1, Y):
            acc = acc + dot(af[yb, dest, y], y1_block(yb, j))
        return acc

    def pass_on(s, j):
        nb = lax.rem(jnp.where(j % 2 == 0, z + 1, z - 1) + Z, Z)
        send(sb.at[j, s], rb.at[j, s], ssem.at[E_RING], rsem_ring.at[j, s], at_z(nb))

    def ring_first(j, u):
        y1_half(1 - c, j)
        sb[j, 0] = products(0, j)
        pass_on(0, j)
        return u

    def ring_next(t, u):
        s, j = t // (2 * NSUB) + 1, t % (2 * NSUB)
        acc = products(s, j)
        arrived(rb.at[0, 0], rsem_ring.at[j, s - 1])
        sb[j, s] = acc + rb[j, s - 1]
        pass_on(s, j)
        return u

    def ring_last(j, u):
        acc = products(Z - 1, j)
        arrived(rb.at[0, 0], rsem_ring.at[j, Z - 2])
        z1[:, columns(j)] = acc + rb[j, Z - 2]
        return u

    lax.fori_loop(0, 2 * NSUB, ring_first, 0)
    lax.fori_loop(0, (Z - 2) * 2 * NSUB, ring_next, 0)
    lax.fori_loop(0, 2 * NSUB, ring_last, 0)

    h1[...] = jnp.maximum(z1[...], 0.0).astype(BF)
    y2[...] = dot(h1[...], w2[...]).astype(BF)

    def send_y2(d, u):
        q = lax.rem(chip + d, NQ)
        send(y2, yp.at[c, chip], ssem.at[E_Y2], rsem.at[E_Y2], at_chip(q))
        return u

    lax.fori_loop(1, NQ, send_y2, 0)
    yp[c, chip] = y2[...]
    lane = lax.broadcasted_iota(jnp.int32, (S, LANES), 1)
    counted = jnp.sum(xp[...].astype(F32).reshape(Y * CB, LANES), axis=0, keepdims=True)
    counted = jnp.sum(jnp.where(lane[0:1] == F, counted, 0.0), axis=1, keepdims=True)
    cs[...] = jnp.broadcast_to(counted, (8, LANES))
    cr[z] = cs[...]
    for d in far:
        send(cs, cr.at[z], ssem.at[E_CNT], rsem.at[E_CNT], at_z((z + d) % Z))
    arrived(most(yp), rsem.at[E_Y2])
    send(yp.at[c], yp.at[c], ssem.at[E_Y2C], rsem.at[E_Y2C], partner)
    arrived(yp.at[0], rsem.at[E_Y2C])
    def z2_part(zq):
        part = dot(af[0, zq, y], plane_rows(yp, 0))
        for yb in range(1, Y):
            part = part + dot(af[yb, zq, y], plane_rows(yp, yb))
        return part

    for d in far:
        zq = (z + d) % Z
        zp[zq] = z2_part(zq)
        send(zp.at[zq], zr.at[z], ssem.at[E_Z2], rsem.at[E_Z2], at_z(zq))
    zr[z] = z2_part(z)
    for yb in range(Y):
        ms[yb] = jnp.where(z1[:, yb * HB:(yb + 1) * HB] > 0.0, 1.0, 0.0).astype(BF)
    for d in (2, 1, 3):
        yq = (y + d) % Y
        send(ms.at[yq], mk.at[y], ssem.at[E_M], rsem.at[E_M], at_y(yq))
    mk[y] = ms[y]
    spread_a(3)
    arrived(zr.at[pl.ds(0, Z - 1)], rsem.at[E_Z2])
    z2 = added(zr, Z)

    arrived(cr.at[pl.ds(0, Z - 1)], rsem.at[E_CNT])
    count = added(cr, Z)[0:1, 0:1]
    own = mtt[...]
    weights = jnp.sum(jnp.where(lane == F, own, 0.0), axis=1, keepdims=True)
    labels = jnp.sum(jnp.where(lane == F + 1, own, 0.0), axis=1, keepdims=True)
    real = lane < NC
    top = jnp.max(jnp.where(real, z2, -jnp.inf), axis=1, keepdims=True)
    shifted = jnp.where(real, z2 - top, 0.0)
    log_probs = shifted - jnp.log(jnp.sum(jnp.where(real, jnp.exp(shifted), 0.0), axis=1, keepdims=True))
    hot = labels == lane.astype(F32)
    picked = jnp.sum(jnp.where(hot, log_probs, 0.0), axis=1, keepdims=True)
    loss_part = -jnp.sum(weights * picked, axis=0, keepdims=True)
    diff = jnp.where(real, jnp.exp(log_probs), 0.0) - hot.astype(F32)
    g2[...] = (diff * (weights / count)).astype(BF)
    for d in far:
        send(g2, gr.at[z], ssem.at[E_G2], rsem.at[E_G2], at_z((z + d) % Z))
    gr[z] = g2[...]
    arrived(gr.at[pl.ds(0, Z - 1)], rsem.at[E_G2])

    g2t = gr[...].reshape(Z * S, LANES).T
    for yb in range(Y):
        part = dot(g2t, af[yb, :, y].reshape(Z * S, CB))
        dp[yb] = part.T.reshape(X, C, S, LANES)
        send(dp.at[yb, :, 1 - c], rc.at[yb], ssem.at[E_DC + yb], rsem.at[E_DC + yb], partner)
    for yb in range(Y):
        arrived(rc.at[yb], rsem.at[E_DC + yb])
        rc[yb] = rc[yb] + dp[yb, :, c]
    sh = S // 2
    for d in (2, 1, 3):
        xq, yq = (x + d) % X, (y + d) % Y
        send(rc.at[:, xq, pl.ds(0, sh)], rx.at[x], ssem.at[E_DX], rsem.at[E_DX], at_x(xq))
        send(rc.at[yq, :, pl.ds(sh, sh)], ry.at[y], ssem.at[E_DY], rsem.at[E_DY], at_y(yq))
    rx[x] = rc[:, x, 0:sh]
    ry[y] = rc[y, :, sh:S]
    arrived(rx.at[pl.ds(0, X - 1)], rsem.at[E_DX])
    rx[x] = added(rx, X)
    for d in (2, 1, 3):
        yq = (y + d) % Y
        send(rx.at[x, yq], ry2.at[y], ssem.at[E_DY2], rsem.at[E_DY2], at_y(yq))
    ry2[y] = rx[x, y]
    arrived(ry.at[pl.ds(0, Y - 1)], rsem.at[E_DY])
    ry[y] = added(ry, Y)
    for d in (2, 1, 3):
        xq = (x + d) % X
        send(ry.at[y, xq], rx2d.at[x], ssem.at[E_DX2], rsem.at[E_DX2], at_x(xq))
    rx2d[x] = ry[y, x]
    arrived(ry2.at[pl.ds(0, Y - 1)], rsem.at[E_DY2])
    arrived(rx2d.at[pl.ds(0, X - 1)], rsem.at[E_DX2])
    d2[0:sh] = added(ry2, Y).astype(BF)
    d2[sh:S] = added(rx2d, X).astype(BF)
    for d in (2, 1, 3):
        send(d2, dg.at[y], ssem.at[E_DG], rsem.at[E_DG], at_y((y + d) % Y))
    dg[y] = d2[...]
    forward_a()
    dy2 = d2[...]

    def g_one(v):
        col = pl.multiple_of(y * HB + v * HU, HU)
        dh = dot(dg[...].reshape(Y * S, LANES), w2t[:, pl.ds(col, HU)])
        keep = mk[:, :, v * HU:(v + 1) * HU].reshape(Y * S, HU).astype(F32)
        gz[v, z] = jnp.where(keep > 0.0, dh, 0.0).astype(BF).reshape(Y, S, HU)

    def gather_step(v, t):
        for d in range(2):
            sgn = 1 if d == 0 else -1
            blk = (z - sgn * (t - 1) + Z) % Z
            if t > 1:
                arrived(gz.at[v, 0], rsem_ag.at[v, d, t - 1])
            ref = gz.at[v, blk] if t < half else gz.at[v, blk, pl.ds(d * (Y // 2), Y // 2)]
            send(ref, ref, ssem.at[E_AG], rsem_ag.at[v, d, t], at_z((z + sgn + Z) % Z))

    def piece(v):
        return pl.ds(v % 2 * HU, HU)

    def prepare(p):
        for v in (2 * p, 2 * p + 1):
            for d in range(2):
                arrived(gz.at[v, 0, pl.ds(0, Y // 2)], rsem_ag.at[v, d, half])
            for k in range(Z):
                gt[p, piece(v), k * Y * S:(k + 1) * Y * S] = gz[v, k].reshape(Y * S, HU).T

    def chunks(p, lo, hi):
        def chunk(n, u):
            k = n % Y
            core = jnp.where(n < Y, 1 - c, c)
            yb = lax.rem(y + k + jnp.where(k == 2, 1, 0) - jnp.where(k == 3, 1, 0), Y)
            off = pl.multiple_of(core * NCH, NCH)
            dy[p, yb, core] = dot(gt[p], af[yb, :, :, :, pl.ds(off, NCH)].reshape(Z * Y * S, NCH))
            return u

        if p == 0 and lo < Y <= hi:
            lax.fori_loop(lo, Y - 1, chunk, 0)
            for d in (1, 3):
                for k in range(1, Y):
                    arrived(af.at[0, pl.ds(0, half), 0], rsem_f.at[d // 2, k - 1])
            lo = Y - 1
        lax.fori_loop(lo, hi, chunk, 0)

    def send_core(p):
        for v in (2 * p, 2 * p + 1):
            send(dy.at[p, :, 1 - c, piece(v)], rcy.at[p, :, piece(v)], ssem.at[E_RC], rsem_c.at[v], partner)

    nxt, prv, opp = (x + 1) % X, (x + X - 1) % X, (x + 2) % X
    hh = HU // 2

    def low(v):
        return pl.ds(v % 2 * HU, hh)

    def high(v):
        return pl.ds(v % 2 * HU + hh, hh)

    def reduce_core(v):
        p = v // 2
        arrived(rcy.at[p, :, piece(v)], rsem_c.at[v])
        for k in range(X):
            rcy[p, k, piece(v)] = rcy[p, k, piece(v)] + dy[p, k, c, piece(v)]
        send(rcy.at[p, opp, low(v)], rx1.at[v, 0], ssem.at[E_RX], rsem_x.at[v, 0], at_x(nxt))
        send(rcy.at[p, opp, high(v)], rx1.at[v, 1], ssem.at[E_RX], rsem_x.at[v, 1], at_x(prv))

    def reduce_x(v):
        p = v // 2
        arrived(rx1.at[v, 0], rsem_x.at[v, 0])
        rcy[p, nxt, low(v)] = rcy[p, nxt, low(v)] + rx1[v, 0]
        send(rcy.at[p, nxt, piece(v)], rx2.at[v, 0], ssem.at[E_RX2], rsem_x.at[v, 2], at_x(nxt))
        arrived(rx1.at[v, 1], rsem_x.at[v, 1])
        rcy[p, prv, high(v)] = rcy[p, prv, high(v)] + rx1[v, 1]
        send(rcy.at[p, prv, piece(v)], rx2.at[v, 1], ssem.at[E_RX2], rsem_x.at[v, 3], at_x(prv))

    def own_x():
        return jnp.concatenate([xp[m % C, nid * (Y // C) + m // C] for m in range(Y)], axis=0)

    def grad_one(v):
        arrived(rx2.at[v, 0], rsem_x.at[v, 2])
        arrived(rx2.at[v, 1], rsem_x.at[v, 3])
        acc = (rcy[v // 2, x, piece(v)] + rx2[v, 0] + rx2[v, 1]).astype(BF)
        part = dot(acc, own_x())
        if v >= NV // 2:
            part = jnp.concatenate([part[:, LANES // 2:], part[:, 0:LANES // 2]], axis=1)
        per = HU // (Z * 8)
        rows = part.reshape(per, Z, 8, LANES)
        for m in range(per):
            k = (v % (NV // 2)) * per + m
            pb[k] = rows[m] if v < NV // 2 else pb[k] + rows[m]

    def w_begin():
        mark = (lax.broadcasted_iota(jnp.int32, (HB, LANES), 0) == 0) & (lax.broadcasted_iota(jnp.int32, (HB, LANES), 1) == NC)
        for k in range(Y):
            part = lax.dot_general(h1[:, k * HB:(k + 1) * HB], dy2, (((0,), (0,)), ((), ())), preferred_element_type=F32)
            if k == 0:
                part = jnp.where(mark, loss_part, part)
            per = HB // (Y * Z * 8)
            rows = part.reshape(per, Y, Z, 8, LANES)
            for m in range(per):
                q = k * per + m
                wb[q // X, q % X] = rows[m]
        send(wb.at[1 - c], wc, ssem.at[E_WC], rsem.at[E_WC], partner)

    def w_core():
        arrived(wc, rsem.at[E_WC])
        wc[...] = wc[...] + wb[c]
        for d in (2, 1, 3):
            xq = (x + d) % X
            send(wc.at[xq], wx.at[x], ssem.at[E_WX], rsem.at[E_WX], at_x(xq))
        wx[x] = wc[x]

    def w_x():
        arrived(wx.at[pl.ds(0, X - 1)], rsem.at[E_WX])
        wx[x] = added(wx, X)
        for d in (2, 1, 3):
            yq = (y + d) % Y
            send(wx.at[x, yq], wy.at[y], ssem.at[E_WY], rsem.at[E_WY], at_y(yq))
        wy[y] = wx[x, y]

    def w_y():
        arrived(wy.at[pl.ds(0, Y - 1)], rsem.at[E_WY])
        wy[y] = added(wy, Y)
        for d in far:
            zq = (z + d) % Z
            send(wy.at[y, zq], wz.at[z], ssem.at[E_WZ], rsem.at[E_WZ], at_z(zq))
        wz[z] = wy[y, z]

    def w_z():
        arrived(wz.at[pl.ds(0, Z - 1)], rsem.at[E_WZ])
        wf[...] = added(wz, Z)
        for d in far:
            send(wf, oz.at[z], ssem.at[E_OZ], rsem.at[E_OZ], at_z((z + d) % Z))
        oz[z] = wf[...]

    def o_z():
        arrived(oz.at[pl.ds(0, Z - 1)], rsem.at[E_OZ])
        for d in (2, 1, 3):
            send(oz, oy.at[y], ssem.at[E_OY], rsem.at[E_OY], at_y((y + d) % Y))
        oy[y] = oz[...]

    def o_y():
        arrived(oy.at[pl.ds(0, Y - 1)], rsem.at[E_OY])
        for d in (2, 1, 3):
            send(oy, ox.at[x], ssem.at[E_OX], rsem.at[E_OX], at_x((x + d) % X))
        ox[x] = oy[...]

    def o_x():
        arrived(ox.at[pl.ds(0, X - 1)], rsem.at[E_OX])
        send(ox, oc.at[c], ssem.at[E_OC], rsem.at[E_OC], partner)
        oc[c] = ox[...]

    arrived(mk.at[pl.ds(0, Y - 1)], rsem.at[E_M])
    arrived(dg.at[pl.ds(0, Y - 1)], rsem.at[E_DG])
    steps = [
        (g_one, 0), (gather_step, 0, 1), (g_one, 1), (gather_step, 1, 1), (g_one, 2), (g_one, 3), (w_begin,),
        (gather_step, 0, 2), (gather_step, 1, 2), (w_core,)]
    for t in range(3, half + 1):
        steps += [(gather_step, 0, t), (gather_step, 1, t)]
    steps += [(gather_step, 2, 1), (gather_step, 3, 1), (prepare, 0), (chunks, 0, 0, 2), (gather_step, 2, 2), (gather_step, 3, 2),
              (chunks, 0, 2, 4), (send_core, 0), (chunks, 0, 4, 6)]
    for t in range(3, half + 1):
        steps += [(gather_step, 2, t), (gather_step, 3, t)]
        if t == 3:
            steps += [(chunks, 0, 6, 8), (w_x,)]
    steps += [(reduce_core, 0), (reduce_core, 1), (reduce_x, 0), (reduce_x, 1), (w_y,), (prepare, 1), (chunks, 1, 0, 4), (send_core, 1), (chunks, 1, 4, 8), (reduce_core, 2),
              (reduce_core, 3), (grad_one, 0), (grad_one, 1), (w_z,), (reduce_x, 2), (reduce_x, 3), (o_z,), (grad_one, 2), (grad_one, 3)]
    for step in steps:
        step[0](*step[1:])

    for d in (2, 1, 3):
        xq = (x + d) % X
        send(pb.at[xq], px.at[x], ssem.at[E_PX], rsem.at[E_PX], at_x(xq))
    px[x] = pb[x]
    o_y()
    arrived(px.at[pl.ds(0, X - 1)], rsem.at[E_PX])
    px[x] = added(px, X)
    for d in far:
        zq = (z + d) % Z
        for k in range(C):
            send(px.at[x, zq], pz.at[c * Z + z], ssem.at[E_PZ], rsem.at[E_PZ], (zq * Y + y, x * C + k))
    send(px.at[x, z], pz.at[c * Z + z], ssem.at[E_PZ], rsem.at[E_PZ], partner)
    pz[c * Z + z] = px[x, z]
    arrived(pz.at[pl.ds(0, C * Z - 1)], rsem.at[E_PZ])
    pf[...] = added(pz, C * Z)
    for d in far:
        send(pf, qz.at[z], ssem.at[E_QZ], rsem.at[E_QZ], at_z((z + d) % Z))
    qz[z] = pf[...]
    o_x()
    arrived(qz.at[pl.ds(0, Z - 1)], rsem.at[E_QZ])
    zl, zh = pl.ds(0, half), pl.ds(half, half)
    for d in (2, 1, 3):
        send(qz.at[zl], qy.at[y], ssem.at[E_QY], rsem.at[E_QY], at_y((y + d) % Y))
        send(qz.at[zh], qx.at[x], ssem.at[E_QX], rsem.at[E_QX], at_x((x + d) % X))
    qy[y] = qz[zl]
    qx[x] = qz[zh]
    arrived(oc.at[0], rsem.at[E_OC])
    for k in range(C):
        full = oc[k].reshape(H // C, LANES)
        dw2_out[k * (H // C):(k + 1) * (H // C), :] = full[:, 0:NC]
        if k == 0:
            loss_out[...] = jnp.broadcast_to(full[0:1, NC:NC + 1] / count, (8, LANES))
    arrived(qy.at[pl.ds(0, Y - 1)], rsem.at[E_QY])
    for d in (2, 1, 3):
        send(qy, qxy.at[x], ssem.at[E_QXY], rsem.at[E_QXY], at_x((x + d) % X))
    qxy[x] = qy[...]
    arrived(qx.at[pl.ds(0, X - 1)], rsem.at[E_QX])
    for d in (2, 1, 3):
        send(qx, qyx.at[y], ssem.at[E_QYX], rsem.at[E_QYX], at_y((y + d) % Y))
    qyx[y] = qx[...]
    arrived(qxy.at[pl.ds(0, X - 1)], rsem.at[E_QXY])
    arrived(qyx.at[pl.ds(0, Y - 1)], rsem.at[E_QYX])
    for yb in range(Y):
        part = jnp.concatenate([qxy[:, yb], qyx[yb]], axis=1).reshape(HB // 2, LANES).T
        dw1_out[:, yb * HB:yb * HB + HB // 2] = part[0:F]
        dw1_out[:, yb * HB + HB // 2:(yb + 1) * HB] = part[LANES // 2:LANES // 2 + F]

    sent(most(xp), ssem.at[E_X])
    sent(xp.at[0], ssem.at[E_XC])
    sent(af.at[pl.ds(0, Y - 1), :, 0], ssem.at[E_A])
    sent(af.at[pl.ds(0, Y - 1), :, pl.ds(0, 2)], ssem.at[E_B])
    sent(af.at[pl.ds(0, Y - 1), :, 0], ssem.at[E_F])
    sent(sb, ssem.at[E_RING])
    sent(cr.at[pl.ds(0, Z - 1)], ssem.at[E_CNT])
    sent(most(yp), ssem.at[E_Y2])
    sent(yp.at[0], ssem.at[E_Y2C])
    sent(zr.at[pl.ds(0, Z - 1)], ssem.at[E_Z2])
    sent(gr.at[pl.ds(0, Z - 1)], ssem.at[E_G2])
    for yb in range(Y):
        sent(rc.at[yb], ssem.at[E_DC + yb])
    sent(rx.at[pl.ds(0, X - 1)], ssem.at[E_DX])
    sent(ry.at[pl.ds(0, Y - 1)], ssem.at[E_DY])
    sent(ry2.at[pl.ds(0, Y - 1)], ssem.at[E_DY2])
    sent(rx2d.at[pl.ds(0, X - 1)], ssem.at[E_DX2])
    sent(dg.at[pl.ds(0, Y - 1)], ssem.at[E_DG])
    sent(mk.at[pl.ds(0, Y - 1)], ssem.at[E_M])
    sent(gz.at[:, pl.ds(0, Z - 1)], ssem.at[E_AG])
    sent(rcy, ssem.at[E_RC])
    sent(rx1, ssem.at[E_RX])
    sent(rx2, ssem.at[E_RX2])
    sent(wc, ssem.at[E_WC])
    sent(wx.at[pl.ds(0, X - 1)], ssem.at[E_WX])
    sent(wy.at[pl.ds(0, Y - 1)], ssem.at[E_WY])
    sent(wz.at[pl.ds(0, Z - 1)], ssem.at[E_WZ])
    sent(oz.at[pl.ds(0, Z - 1)], ssem.at[E_OZ])
    sent(oy.at[pl.ds(0, Y - 1)], ssem.at[E_OY])
    sent(ox.at[pl.ds(0, X - 1)], ssem.at[E_OX])
    sent(oc.at[0], ssem.at[E_OC])
    sent(px.at[pl.ds(0, X - 1)], ssem.at[E_PX])
    sent(pz.at[pl.ds(0, C * Z - 1)], ssem.at[E_PZ])
    sent(qz.at[pl.ds(0, Z - 1)], ssem.at[E_QZ])
    sent(qy.at[pl.ds(0, Y - 1)], ssem.at[E_QY])
    sent(qx.at[pl.ds(0, X - 1)], ssem.at[E_QX])
    sent(qxy.at[pl.ds(0, X - 1)], ssem.at[E_QXY])
    sent(qyx.at[pl.ds(0, Y - 1)], ssem.at[E_QYX])


def solution(mesh):
    Y, X, C = Y_DIM, X_DIM, CORES
    Z = mesh.shape["rep"] // Y
    row_spec = P(("rep", "nodes"))

    def device_step(adj_blk, feat_blk, w_one, w_two, label_blk, mask_blk):
        R, S, CB = adj_blk.shape
        F, H = w_one.shape
        NC = w_two.shape[1]
        I = X * C
        NQ = Y * X
        HR = H // (2 * NSUB)
        HB = H // Y
        HU = HB // NV
        NCH = Y * S
        assert R == Z * Y and CB == S * I and X == Y and F + 2 <= LANES // 2 and NC < LANES
        vm = pltpu.VMEM
        dma = pltpu.SemaphoreType.DMA
        scratch = [
            vm((Y, Z, Y, S, CB), BF),
            vm((F, S), BF),
            vm((1, S), jnp.int32),
            vm((1, S), jnp.int32),
            vm((LANES, S), F32),
            vm((S, LANES), F32),
            vm((F, H), F32),
            vm((H, NC), F32),
            vm((LANES, H), BF),
            vm((H, LANES), BF),
            vm((LANES, H), BF),
            vm((S, LANES), BF),
            vm((C, NQ, S, LANES), BF),
            vm((NQ, C, S, H), BF),
            vm((8, LANES), F32),
            vm((Z, 8, LANES), F32),
            vm((2 * NSUB, Z - 1, S, HR), F32),
            vm((2 * NSUB, Z - 1, S, HR), F32),
            vm((S, H), F32),
            vm((S, H), BF),
            vm((S, LANES), BF),
            vm((C, NQ, S, LANES), BF),
            vm((Z, S, LANES), F32),
            vm((Z, S, LANES), F32),
            vm((S, LANES), BF),
            vm((Z, S, LANES), BF),
            vm((Y, X, C, S, LANES), F32),
            vm((Y, X, S, LANES), F32),
            vm((X, Y, S // 2, LANES), F32),
            vm((Y, X, S // 2, LANES), F32),
            vm((Y, S // 2, LANES), F32),
            vm((X, S // 2, LANES), F32),
            vm((S, LANES), BF),
            vm((Y, S, LANES), BF),
            vm((Y, S, HB), BF),
            vm((Y, S, HB), BF),
            vm((NV, Z, Y, S, HU), BF),
            vm((NV // 2, 2 * HU, Z * Y * S), BF),
            vm((NV // 2, X, C, 2 * HU, NCH), F32),
            vm((NV // 2, X, 2 * HU, NCH), F32),
            vm((NV, 2, HU // 2, NCH), F32),
            vm((NV, 2, HU, NCH), F32),
            vm((C, X, Y, Z, 8, LANES), F32),
            vm((X, Y, Z, 8, LANES), F32),
            vm((X, Y, Z, 8, LANES), F32),
            vm((Y, Z, 8, LANES), F32),
            vm((Z, 8, LANES), F32),
            vm((8, LANES), F32),
            vm((Z, 8, LANES), F32),
            vm((Y, Z, 8, LANES), F32),
            vm((X, Y, Z, 8, LANES), F32),
            vm((C, X, Y, Z, 8, LANES), F32),
            vm((X, Z, 8, LANES), F32),
            vm((X, Z, 8, LANES), F32),
            vm((C * Z, 8, LANES), F32),
            vm((8, LANES), F32),
            vm((Z, 8, LANES), F32),
            vm((Y, Z // 2, 8, LANES), F32),
            vm((X, Z // 2, 8, LANES), F32),
            vm((X, Y, Z // 2, 8, LANES), F32),
            vm((Y, X, Z // 2, 8, LANES), F32),
            dma((NSEM,)),
            dma((NSEM,)),
            dma((Y - 1, Z)),
            dma((2, Y - 1)),
            dma((2, Y - 1)),
            dma((2 * NSUB, Z - 1)),
            dma((NV, 2, Z // 2 + 1)),
            dma((NV,)),
            dma((NV, 4)),
        ]
        vspec = pl.BlockSpec(memory_space=pltpu.VMEM)
        aspec = pl.BlockSpec(memory_space=pltpu.HBM)
        operands = (adj_blk.reshape(Z, Y, S, CB), feat_blk.T, label_blk[None, :], mask_blk[None, :], w_one, w_two)
        dw_one, dw_two, loss = pl.pallas_call(
            functools.partial(_step, (Z, Y, X, C, S, CB, H, F, NC)),
            out_shape=(jax.ShapeDtypeStruct((F, H), F32), jax.ShapeDtypeStruct((H, NC), F32), jax.ShapeDtypeStruct((8, LANES), F32)),
            in_specs=[aspec] * 6,
            out_specs=(vspec, vspec, vspec),
            scratch_shapes=scratch,
            compiler_params=pltpu.CompilerParams(collective_id=0, has_side_effects=True, vmem_limit_bytes=52 * 1024 * 1024),
            name="gcn_step",
        )(*[pltpu.with_memory_space_constraint(v, pltpu.HBM) for v in operands])
        return loss[0, 0], dw_one, dw_two

    return jax.shard_map(device_step, mesh=mesh, in_specs=(P(None, "nodes", "rep"), row_spec, P(), P(), row_spec, row_spec), out_specs=(P(), P(), P()), check_vma=False)
```

```python
import functools

import jax
import jax.numpy as jnp
from jax import lax
from jax.experimental import pallas as pl
from jax.experimental.pallas import tpu as pltpu
from jax.sharding import PartitionSpec as P

Y_DIM = 4
X_DIM = 4
CORES = 2
LANES = 128
NSUB = 4
NV = 4
NSEM = 46
BF = jnp.bfloat16
F32 = jnp.float32


def _step(dims, a_hbm, feat_hbm, lab_hbm, msk_hbm, w_one, w_two, dw1_out, dw2_out, loss_out,
          af, feat, lab, msk, mt, mtt, w1f, w2f, w1, w2, w2t, xs, xp, xn, y1, cs, cr, sb, rb, z1, h1, y2, yp, zp, zr, g2, gr, dp, rc, rx, ry, ry2, rx2d,
          d2, dg, ms, mk, gz, gt, dy, rcy, rx1, rx2, wb, wc, wx, wy, wz, wf, oz, oy, ox, oc, pb, px, pz, pf, qz, qy, qx, qxy, qyx,
          ssem, rsem, rsem_a, rsem_b, rsem_f, rsem_ring, rsem_ag, rsem_c, rsem_x):
    Z, Y, X, C, S, CB, H, F, NC = dims
    I = X * C
    NQ = Y * X
    HR = H // (2 * NSUB)
    HB = H // Y
    HU = HB // NV
    NCH = Y * S
    half = Z // 2
    rid = lax.axis_index("rep")
    nid = lax.axis_index("nodes")
    z, y, x, c = rid // Y, rid % Y, nid // C, nid % C
    chip = y * X + x
    partner = (rid, x * C + 1 - c)

    far = sorted(range(1, Z), key=lambda d: -min(d, Z - d))

    def at_z(zz):
        return (zz * Y + y, nid)

    def at_y(yy):
        return (z * Y + yy, nid)

    def at_x(xx):
        return (rid, xx * C + c)

    def at_chip(q):
        return (z * Y + q // X, (q % X) * C + c)

    def send(src, dst, ss, rs, dev):
        pltpu.make_async_remote_copy(src_ref=src, dst_ref=dst, send_sem=ss, recv_sem=rs, device_id=dev,
                                     device_id_type=pl.DeviceIdType.MESH).start()

    def arrived(ref, rs):
        pltpu.make_async_remote_copy(src_ref=ref, dst_ref=ref, send_sem=ssem.at[0], recv_sem=rs, device_id=partner,
                                     device_id_type=pl.DeviceIdType.MESH).wait_recv()

    def sent(ref, ss):
        pltpu.make_async_remote_copy(src_ref=ref, dst_ref=ref, send_sem=ss, recv_sem=rsem.at[0], device_id=partner,
                                     device_id_type=pl.DeviceIdType.MESH).wait_send()

    def dot(a, b):
        return jnp.dot(a, b, preferred_element_type=F32)

    def most(ref):
        return ref.at[0, pl.ds(0, NQ - 1)]

    def plane_rows(ref, yb):
        return jnp.stack([ref[k, yb * X:(yb + 1) * X] for k in range(C)], axis=1).reshape(CB, LANES)

    def turned(v):
        return jnp.concatenate([v[:, LANES // 2:], v[:, 0:LANES // 2]], axis=1)

    def added(ref, n):
        acc = ref[0]
        for k in range(1, n):
            acc = acc + ref[k]
        return acc

    (E_X, E_XC, E_A, E_B, E_F, E_RING, E_CNT, E_Y2, E_Y2C, E_Z2, E_G2, E_DC, E_DC1, E_DC2, E_DC3, E_DX, E_DY, E_AG, E_RC, E_RX, E_RX2,
     E_WC, E_WX, E_WY, E_WZ, E_OZ, E_OY, E_OX, E_OC, E_PX, E_PZ, E_QZ, E_QY, E_QX, E_LA, E_L1, E_L2,
     E_M, E_DY2, E_DX2, E_DG, E_QXY, E_QYX, E_IN, E_IN1, E_IN2) = range(NSEM)

    load_a = pltpu.make_async_copy(a_hbm, af.at[y], ssem.at[E_LA])
    load_1 = pltpu.make_async_copy(w_one, w1f, ssem.at[E_L1])
    load_2 = pltpu.make_async_copy(w_two, w2f, ssem.at[E_L2])
    loads = [pltpu.make_async_copy(src, dst, ssem.at[E_IN + k]) for k, (src, dst) in
             enumerate(((feat_hbm, feat), (lab_hbm, lab), (msk_hbm, msk)))]
    for load in loads:
        load.start()
    load_a.start()
    load_1.start()
    load_2.start()

    bar = pltpu.get_barrier_semaphore()
    for d in far:
        pl.semaphore_signal(bar, inc=1, device_id=at_z((z + d) % Z), device_id_type=pl.DeviceIdType.MESH)

    def greet_plane(d, u):
        pl.semaphore_signal(bar, inc=1, device_id=at_chip(lax.rem(chip + d, NQ)), device_id_type=pl.DeviceIdType.MESH)
        return u

    lax.fori_loop(1, NQ, greet_plane, 0)
    pl.semaphore_signal(bar, inc=1, device_id=partner, device_id_type=pl.DeviceIdType.MESH)

    for load in loads:
        load.wait()
    mt[...] = jnp.zeros_like(mt)
    mt[0:F] = feat[...].astype(F32)
    mt[F:F + 1] = msk[...].astype(F32)
    mt[F + 1:F + 2] = lab[...].astype(F32)
    mtt[...] = mt[...].T
    xs[...] = (mtt[0:S // 2] + turned(mtt[S // 2:S])).astype(BF)
    pl.semaphore_wait(bar, NQ + Z - 1)

    def send_x(d, u):
        q = lax.rem(chip + d, NQ)
        send(xs, xp.at[c, chip], ssem.at[E_X], rsem.at[E_X], at_chip(q))
        return u

    lax.fori_loop(1, NQ, send_x, 0)
    xp[c, chip] = xs[...]
    load_a.wait()

    order = []
    for k in range(1, half + 1):
        order.append(-k)
        if k < half:
            order.append(k)
    order.append(0)
    for k in order:
        zc = (z + k + Z) % Z
        for d in (2, 1, 3):
            yq = (y + d) % Y
            send(af.at[y, zc, yq], af.at[y, zc, yq], ssem.at[E_A], rsem_a.at[d - 1, zc], at_y(yq))
    def spread_a(k):
        for d in (1, 3):
            yq = (y + d) % Y
            ya = (yq + k) % Y
            send(af.at[y, :, ya], af.at[y, :, ya], ssem.at[E_B], rsem_b.at[d // 2, k - 1], at_y(yq))

    def forward_a():
        for k in range(1, Y):
            for d in (1, 3):
                arrived(af.at[0, :, 0], rsem_b.at[d // 2, k - 1])
        for k in range(1, Y):
            for d in (1, 3):
                ys, yq = (y - d + Y) % Y, (y + d) % Y
                lo = 0 if d == 1 else half
                ya = (yq + k) % Y
                send(af.at[ys, pl.ds(lo, half), ya], af.at[ys, pl.ds(lo, half), ya], ssem.at[E_F], rsem_f.at[d // 2, k - 1], at_y(yq))

    spread_a(1)
    spread_a(2)

    load_1.wait()
    w1[...] = jnp.zeros_like(w1)
    w1[0, 0:F] = w1f[...].astype(BF)
    w1[1, LANES // 2:LANES // 2 + F] = w1f[...].astype(BF)
    load_2.wait()
    w2[...] = jnp.zeros_like(w2)
    for k in range(Y):
        rows = slice(k * HB, (k + 1) * HB)
        w2[rows, 0:NC] = w2f[rows].astype(BF)
        w2t[:, rows] = w2[rows].T

    arrived(most(xp), rsem.at[E_X])
    send(xp.at[c], xp.at[c], ssem.at[E_XC], rsem.at[E_XC], partner)

    def columns(j):
        return pl.ds(pl.multiple_of(j * HR, HR), HR)

    def y1_half(k, j):
        rows = xp[k].reshape(NQ * S // 2, LANES)
        for m in range(2):
            y1[:, k, m * (S // 2):(m + 1) * (S // 2), columns(j)] = dot(rows, w1[m, :, columns(j)]).astype(BF).reshape(NQ, S // 2, HR)

    def y1_own(j, u):
        y1_half(c, j)
        return u

    def y1_block(yb, j):
        return y1[yb * X:(yb + 1) * X, :, :, columns(j)].reshape(CB, HR)

    lax.fori_loop(0, 2 * NSUB, y1_own, 0)
    arrived(xp.at[0], rsem.at[E_XC])

    def wait_a(zc):
        for d in range(1, Y):
            arrived(af.at[0, 0, 0], rsem_a.at[d - 1, zc])

    def products(s, j):
        up = j % 2 == 0
        dest = lax.rem(jnp.where(up, z - 1 - s, z + 1 + s) + 2 * Z, Z)
        fresh = ((j == 0) & ((s < half) | (s == Z - 1))) | ((j == 1) & (s < half - 1))

        @pl.when(fresh)
        def _():
            wait_a(dest)

        acc = dot(af[0, dest, y], y1_block(0, j))
        for yb in range(1, Y):
            acc = acc + dot(af[yb, dest, y], y1_block(yb, j))
        return acc

    def pass_on(s, j):
        nb = lax.rem(jnp.where(j % 2 == 0, z + 1, z - 1) + Z, Z)
        send(sb.at[j, s], rb.at[j, s], ssem.at[E_RING], rsem_ring.at[j, s], at_z(nb))

    def ring_first(j, u):
        y1_half(1 - c, j)
        sb[j, 0] = products(0, j)
        pass_on(0, j)
        return u

    def ring_next(t, u):
        s, j = t // (2 * NSUB) + 1, t % (2 * NSUB)
        acc = products(s, j)
        arrived(rb.at[0, 0], rsem_ring.at[j, s - 1])
        sb[j, s] = acc + rb[j, s - 1]
        pass_on(s, j)
        return u

    def ring_last(j, u):
        acc = products(Z - 1, j)
        arrived(rb.at[0, 0], rsem_ring.at[j, Z - 2])
        z1[:, columns(j)] = acc + rb[j, Z - 2]
        return u

    lax.fori_loop(0, 2 * NSUB, ring_first, 0)
    lax.fori_loop(0, (Z - 2) * 2 * NSUB, ring_next, 0)
    lax.fori_loop(0, 2 * NSUB, ring_last, 0)

    h1[...] = jnp.maximum(z1[...], 0.0).astype(BF)
    y2[...] = dot(h1[...], w2[...]).astype(BF)

    def send_y2(d, u):
        q = lax.rem(chip + d, NQ)
        send(y2, yp.at[c, chip], ssem.at[E_Y2], rsem.at[E_Y2], at_chip(q))
        return u

    lax.fori_loop(1, NQ, send_y2, 0)
    yp[c, chip] = y2[...]
    lane = lax.broadcasted_iota(jnp.int32, (S, LANES), 1)
    counted = jnp.sum(xp[...].astype(F32).reshape(Y * CB // 2, LANES), axis=0, keepdims=True)
    counted = jnp.sum(jnp.where(lane[0:1] % (LANES // 2) == F, counted, 0.0), axis=1, keepdims=True)
    cs[...] = jnp.broadcast_to(counted, (8, LANES))
    cr[z] = cs[...]
    for d in far:
        send(cs, cr.at[z], ssem.at[E_CNT], rsem.at[E_CNT], at_z((z + d) % Z))
    arrived(most(yp), rsem.at[E_Y2])
    send(yp.at[c], yp.at[c], ssem.at[E_Y2C], rsem.at[E_Y2C], partner)
    arrived(yp.at[0], rsem.at[E_Y2C])
    def z2_part(zq):
        part = dot(af[0, zq, y], plane_rows(yp, 0))
        for yb in range(1, Y):
            part = part + dot(af[yb, zq, y], plane_rows(yp, yb))
        return part

    for d in far:
        zq = (z + d) % Z
        zp[zq] = z2_part(zq)
        send(zp.at[zq], zr.at[z], ssem.at[E_Z2], rsem.at[E_Z2], at_z(zq))
    zr[z] = z2_part(z)
    for yb in range(Y):
        ms[yb] = jnp.where(z1[:, yb * HB:(yb + 1) * HB] > 0.0, 1.0, 0.0).astype(BF)
    for d in (2, 1, 3):
        yq = (y + d) % Y
        send(ms.at[yq], mk.at[y], ssem.at[E_M], rsem.at[E_M], at_y(yq))
    mk[y] = ms[y]
    spread_a(3)
    arrived(zr.at[pl.ds(0, Z - 1)], rsem.at[E_Z2])
    z2 = added(zr, Z)

    arrived(cr.at[pl.ds(0, Z - 1)], rsem.at[E_CNT])
    count = added(cr, Z)[0:1, 0:1]
    own = mtt[...]
    weights = jnp.sum(jnp.where(lane == F, own, 0.0), axis=1, keepdims=True)
    labels = jnp.sum(jnp.where(lane == F + 1, own, 0.0), axis=1, keepdims=True)
    real = lane < NC
    top = jnp.max(jnp.where(real, z2, -jnp.inf), axis=1, keepdims=True)
    shifted = jnp.where(real, z2 - top, 0.0)
    log_probs = shifted - jnp.log(jnp.sum(jnp.where(real, jnp.exp(shifted), 0.0), axis=1, keepdims=True))
    hot = labels == lane.astype(F32)
    picked = jnp.sum(jnp.where(hot, log_probs, 0.0), axis=1, keepdims=True)
    loss_part = -jnp.sum(weights * picked, axis=0, keepdims=True)
    diff = jnp.where(real, jnp.exp(log_probs), 0.0) - hot.astype(F32)
    g2[...] = (diff * (weights / count)).astype(BF)
    for d in far:
        send(g2, gr.at[z], ssem.at[E_G2], rsem.at[E_G2], at_z((z + d) % Z))
    gr[z] = g2[...]
    arrived(gr.at[pl.ds(0, Z - 1)], rsem.at[E_G2])

    g2t = gr[...].reshape(Z * S, LANES).T
    for yb in range(Y):
        part = dot(g2t, af[yb, :, y].reshape(Z * S, CB))
        dp[yb] = part.T.reshape(X, C, S, LANES)
        send(dp.at[yb, :, 1 - c], rc.at[yb], ssem.at[E_DC + yb], rsem.at[E_DC + yb], partner)
    for yb in range(Y):
        arrived(rc.at[yb], rsem.at[E_DC + yb])
        rc[yb] = rc[yb] + dp[yb, :, c]
    sh = S // 2
    for d in (2, 1, 3):
        xq, yq = (x + d) % X, (y + d) % Y
        send(rc.at[:, xq, pl.ds(0, sh)], rx.at[x], ssem.at[E_DX], rsem.at[E_DX], at_x(xq))
        send(rc.at[yq, :, pl.ds(sh, sh)], ry.at[y], ssem.at[E_DY], rsem.at[E_DY], at_y(yq))
    rx[x] = rc[:, x, 0:sh]
    ry[y] = rc[y, :, sh:S]
    arrived(rx.at[pl.ds(0, X - 1)], rsem.at[E_DX])
    rx[x] = added(rx, X)
    for d in (2, 1, 3):
        yq = (y + d) % Y
        send(rx.at[x, yq], ry2.at[y], ssem.at[E_DY2], rsem.at[E_DY2], at_y(yq))
    ry2[y] = rx[x, y]
    arrived(ry.at[pl.ds(0, Y - 1)], rsem.at[E_DY])
    ry[y] = added(ry, Y)
    for d in (2, 1, 3):
        xq = (x + d) % X
        send(ry.at[y, xq], rx2d.at[x], ssem.at[E_DX2], rsem.at[E_DX2], at_x(xq))
    rx2d[x] = ry[y, x]
    arrived(ry2.at[pl.ds(0, Y - 1)], rsem.at[E_DY2])
    arrived(rx2d.at[pl.ds(0, X - 1)], rsem.at[E_DX2])
    d2[0:sh] = added(ry2, Y).astype(BF)
    d2[sh:S] = added(rx2d, X).astype(BF)
    for d in (2, 1, 3):
        send(d2, dg.at[y], ssem.at[E_DG], rsem.at[E_DG], at_y((y + d) % Y))
    dg[y] = d2[...]
    forward_a()
    dy2 = d2[...]

    def g_one(v):
        col = pl.multiple_of(y * HB + v * HU, HU)
        dh = dot(dg[...].reshape(Y * S, LANES), w2t[:, pl.ds(col, HU)])
        keep = mk[:, :, v * HU:(v + 1) * HU].reshape(Y * S, HU).astype(F32)
        gz[v, z] = jnp.where(keep > 0.0, dh, 0.0).astype(BF).reshape(Y, S, HU)

    def gather_step(v, t):
        for d in range(2):
            sgn = 1 if d == 0 else -1
            blk = (z - sgn * (t - 1) + Z) % Z
            if t > 1:
                arrived(gz.at[v, 0], rsem_ag.at[v, d, t - 1])
            ref = gz.at[v, blk] if t < half else gz.at[v, blk, pl.ds(d * (Y // 2), Y // 2)]
            send(ref, ref, ssem.at[E_AG], rsem_ag.at[v, d, t], at_z((z + sgn + Z) % Z))

    def piece(v):
        return pl.ds(v % 2 * HU, HU)

    def prepare(p):
        for v in (2 * p, 2 * p + 1):
            for d in range(2):
                arrived(gz.at[v, 0, pl.ds(0, Y // 2)], rsem_ag.at[v, d, half])
            for k in range(Z):
                gt[p, piece(v), k * Y * S:(k + 1) * Y * S] = gz[v, k].reshape(Y * S, HU).T

    def chunks(p, lo, hi):
        def chunk(n, u):
            k = n % Y
            core = jnp.where(n < Y, 1 - c, c)
            yb = lax.rem(y + k + jnp.where(k == 2, 1, 0) - jnp.where(k == 3, 1, 0), Y)
            off = pl.multiple_of(core * NCH, NCH)
            dy[p, yb, core] = dot(gt[p], af[yb, :, :, :, pl.ds(off, NCH)].reshape(Z * Y * S, NCH))
            return u

        if p == 0 and lo < Y <= hi:
            lax.fori_loop(lo, Y - 1, chunk, 0)
            for d in (1, 3):
                for k in range(1, Y):
                    arrived(af.at[0, pl.ds(0, half), 0], rsem_f.at[d // 2, k - 1])
            lo = Y - 1
        lax.fori_loop(lo, hi, chunk, 0)

    def send_core(p):
        for v in (2 * p, 2 * p + 1):
            send(dy.at[p, :, 1 - c, piece(v)], rcy.at[p, :, piece(v)], ssem.at[E_RC], rsem_c.at[v], partner)

    nxt, prv, opp = (x + 1) % X, (x + X - 1) % X, (x + 2) % X
    hh = HU // 2

    def low(v):
        return pl.ds(v % 2 * HU, hh)

    def high(v):
        return pl.ds(v % 2 * HU + hh, hh)

    def reduce_core(v):
        p = v // 2
        arrived(rcy.at[p, :, piece(v)], rsem_c.at[v])
        for k in range(X):
            rcy[p, k, piece(v)] = rcy[p, k, piece(v)] + dy[p, k, c, piece(v)]
        send(rcy.at[p, opp, low(v)], rx1.at[v, 0], ssem.at[E_RX], rsem_x.at[v, 0], at_x(nxt))
        send(rcy.at[p, opp, high(v)], rx1.at[v, 1], ssem.at[E_RX], rsem_x.at[v, 1], at_x(prv))

    def reduce_x(v):
        p = v // 2
        arrived(rx1.at[v, 0], rsem_x.at[v, 0])
        rcy[p, nxt, low(v)] = rcy[p, nxt, low(v)] + rx1[v, 0]
        send(rcy.at[p, nxt, piece(v)], rx2.at[v, 0], ssem.at[E_RX2], rsem_x.at[v, 2], at_x(nxt))
        arrived(rx1.at[v, 1], rsem_x.at[v, 1])
        rcy[p, prv, high(v)] = rcy[p, prv, high(v)] + rx1[v, 1]
        send(rcy.at[p, prv, piece(v)], rx2.at[v, 1], ssem.at[E_RX2], rsem_x.at[v, 3], at_x(prv))

    def own_x():
        low_half = lax.broadcasted_iota(jnp.int32, (S // 2, LANES), 1) < LANES // 2
        for m in range(Y):
            rows = xp[m % C, nid * (Y // C) + m // C].astype(F32)
            xn[m * S:m * S + S // 2] = jnp.where(low_half, rows, 0.0).astype(BF)
            xn[m * S + S // 2:(m + 1) * S] = jnp.where(low_half, turned(rows), 0.0).astype(BF)

    def grad_one(v):
        arrived(rx2.at[v, 0], rsem_x.at[v, 2])
        arrived(rx2.at[v, 1], rsem_x.at[v, 3])
        acc = (rcy[v // 2, x, piece(v)] + rx2[v, 0] + rx2[v, 1]).astype(BF)
        part = dot(acc, xn[...])
        if v >= NV // 2:
            part = turned(part)
        per = HU // (Z * 8)
        rows = part.reshape(per, Z, 8, LANES)
        for m in range(per):
            k = (v % (NV // 2)) * per + m
            pb[k] = rows[m] if v < NV // 2 else pb[k] + rows[m]

    def w_begin():
        mark = (lax.broadcasted_iota(jnp.int32, (HB, LANES), 0) == 0) & (lax.broadcasted_iota(jnp.int32, (HB, LANES), 1) == NC)
        for k in range(Y):
            part = lax.dot_general(h1[:, k * HB:(k + 1) * HB], dy2, (((0,), (0,)), ((), ())), preferred_element_type=F32)
            if k == 0:
                part = jnp.where(mark, loss_part, part)
            per = HB // (Y * Z * 8)
            rows = part.reshape(per, Y, Z, 8, LANES)
            for m in range(per):
                q = k * per + m
                wb[q // X, q % X] = rows[m]
        send(wb.at[1 - c], wc, ssem.at[E_WC], rsem.at[E_WC], partner)

    def w_core():
        arrived(wc, rsem.at[E_WC])
        wc[...] = wc[...] + wb[c]
        for d in (2, 1, 3):
            xq = (x + d) % X
            send(wc.at[xq], wx.at[x], ssem.at[E_WX], rsem.at[E_WX], at_x(xq))
        wx[x] = wc[x]

    def w_x():
        arrived(wx.at[pl.ds(0, X - 1)], rsem.at[E_WX])
        wx[x] = added(wx, X)
        for d in (2, 1, 3):
            yq = (y + d) % Y
            send(wx.at[x, yq], wy.at[y], ssem.at[E_WY], rsem.at[E_WY], at_y(yq))
        wy[y] = wx[x, y]

    def w_y():
        arrived(wy.at[pl.ds(0, Y - 1)], rsem.at[E_WY])
        wy[y] = added(wy, Y)
        for d in far:
            zq = (z + d) % Z
            send(wy.at[y, zq], wz.at[z], ssem.at[E_WZ], rsem.at[E_WZ], at_z(zq))
        wz[z] = wy[y, z]

    def w_z():
        arrived(wz.at[pl.ds(0, Z - 1)], rsem.at[E_WZ])
        wf[...] = added(wz, Z)
        for d in far:
            send(wf, oz.at[z], ssem.at[E_OZ], rsem.at[E_OZ], at_z((z + d) % Z))
        oz[z] = wf[...]

    def o_z():
        arrived(oz.at[pl.ds(0, Z - 1)], rsem.at[E_OZ])
        for d in (2, 1, 3):
            send(oz, oy.at[y], ssem.at[E_OY], rsem.at[E_OY], at_y((y + d) % Y))
        oy[y] = oz[...]

    def o_y():
        arrived(oy.at[pl.ds(0, Y - 1)], rsem.at[E_OY])
        for d in (2, 1, 3):
            send(oy, ox.at[x], ssem.at[E_OX], rsem.at[E_OX], at_x((x + d) % X))
        ox[x] = oy[...]

    def o_x():
        arrived(ox.at[pl.ds(0, X - 1)], rsem.at[E_OX])
        send(ox, oc.at[c], ssem.at[E_OC], rsem.at[E_OC], partner)
        oc[c] = ox[...]

    arrived(mk.at[pl.ds(0, Y - 1)], rsem.at[E_M])
    arrived(dg.at[pl.ds(0, Y - 1)], rsem.at[E_DG])
    steps = [
        (g_one, 0), (gather_step, 0, 1), (g_one, 1), (gather_step, 1, 1), (g_one, 2), (g_one, 3), (w_begin,), (own_x,),
        (gather_step, 0, 2), (gather_step, 1, 2), (w_core,)]
    for t in range(3, half + 1):
        steps += [(gather_step, 0, t), (gather_step, 1, t)]
    steps += [(gather_step, 2, 1), (gather_step, 3, 1), (prepare, 0), (chunks, 0, 0, 2), (gather_step, 2, 2), (gather_step, 3, 2),
              (chunks, 0, 2, 4), (send_core, 0), (chunks, 0, 4, 6)]
    for t in range(3, half + 1):
        steps += [(gather_step, 2, t), (gather_step, 3, t)]
        if t == 3:
            steps += [(chunks, 0, 6, 8), (reduce_core, 0), (reduce_core, 1), (w_x,)]
    steps += [(reduce_x, 0), (reduce_x, 1), (w_y,), (prepare, 1), (chunks, 1, 0, 4), (send_core, 1), (chunks, 1, 4, 8), (reduce_core, 2),
              (reduce_core, 3), (grad_one, 0), (grad_one, 1), (w_z,), (reduce_x, 2), (reduce_x, 3), (o_z,), (grad_one, 2), (grad_one, 3)]
    for step in steps:
        step[0](*step[1:])

    for d in (2, 1, 3):
        xq = (x + d) % X
        send(pb.at[xq], px.at[x], ssem.at[E_PX], rsem.at[E_PX], at_x(xq))
    px[x] = pb[x]
    o_y()
    arrived(px.at[pl.ds(0, X - 1)], rsem.at[E_PX])
    px[x] = added(px, X)
    for d in far:
        zq = (z + d) % Z
        for k in range(C):
            send(px.at[x, zq], pz.at[c * Z + z], ssem.at[E_PZ], rsem.at[E_PZ], (zq * Y + y, x * C + k))
    send(px.at[x, z], pz.at[c * Z + z], ssem.at[E_PZ], rsem.at[E_PZ], partner)
    pz[c * Z + z] = px[x, z]
    arrived(pz.at[pl.ds(0, C * Z - 1)], rsem.at[E_PZ])
    pf[...] = added(pz, C * Z)
    for d in far:
        send(pf, qz.at[z], ssem.at[E_QZ], rsem.at[E_QZ], at_z((z + d) % Z))
    qz[z] = pf[...]
    o_x()
    arrived(qz.at[pl.ds(0, Z - 1)], rsem.at[E_QZ])
    zl, zh = pl.ds(0, half), pl.ds(half, half)
    for d in (2, 1, 3):
        send(qz.at[zl], qy.at[y], ssem.at[E_QY], rsem.at[E_QY], at_y((y + d) % Y))
        send(qz.at[zh], qx.at[x], ssem.at[E_QX], rsem.at[E_QX], at_x((x + d) % X))
    qy[y] = qz[zl]
    qx[x] = qz[zh]
    arrived(oc.at[0], rsem.at[E_OC])
    for k in range(C):
        full = oc[k].reshape(H // C, LANES)
        dw2_out[k * (H // C):(k + 1) * (H // C), :] = full[:, 0:NC]
        if k == 0:
            loss_out[...] = jnp.broadcast_to(full[0:1, NC:NC + 1] / count, (8, LANES))
    arrived(qy.at[pl.ds(0, Y - 1)], rsem.at[E_QY])
    for d in (2, 1, 3):
        send(qy, qxy.at[x], ssem.at[E_QXY], rsem.at[E_QXY], at_x((x + d) % X))
    qxy[x] = qy[...]
    arrived(qx.at[pl.ds(0, X - 1)], rsem.at[E_QX])
    for d in (2, 1, 3):
        send(qx, qyx.at[y], ssem.at[E_QYX], rsem.at[E_QYX], at_y((y + d) % Y))
    qyx[y] = qx[...]
    arrived(qxy.at[pl.ds(0, X - 1)], rsem.at[E_QXY])
    arrived(qyx.at[pl.ds(0, Y - 1)], rsem.at[E_QYX])
    for yb in range(Y):
        part = jnp.concatenate([qxy[:, yb], qyx[yb]], axis=1).reshape(HB // 2, LANES).T
        dw1_out[:, yb * HB:yb * HB + HB // 2] = part[0:F]
        dw1_out[:, yb * HB + HB // 2:(yb + 1) * HB] = part[LANES // 2:LANES // 2 + F]

    sent(most(xp), ssem.at[E_X])
    sent(xp.at[0], ssem.at[E_XC])
    sent(af.at[pl.ds(0, Y - 1), :, 0], ssem.at[E_A])
    sent(af.at[pl.ds(0, Y - 1), :, pl.ds(0, 2)], ssem.at[E_B])
    sent(af.at[pl.ds(0, Y - 1), :, 0], ssem.at[E_F])
    sent(sb, ssem.at[E_RING])
    sent(cr.at[pl.ds(0, Z - 1)], ssem.at[E_CNT])
    sent(most(yp), ssem.at[E_Y2])
    sent(yp.at[0], ssem.at[E_Y2C])
    sent(zr.at[pl.ds(0, Z - 1)], ssem.at[E_Z2])
    sent(gr.at[pl.ds(0, Z - 1)], ssem.at[E_G2])
    for yb in range(Y):
        sent(rc.at[yb], ssem.at[E_DC + yb])
    sent(rx.at[pl.ds(0, X - 1)], ssem.at[E_DX])
    sent(ry.at[pl.ds(0, Y - 1)], ssem.at[E_DY])
    sent(ry2.at[pl.ds(0, Y - 1)], ssem.at[E_DY2])
    sent(rx2d.at[pl.ds(0, X - 1)], ssem.at[E_DX2])
    sent(dg.at[pl.ds(0, Y - 1)], ssem.at[E_DG])
    sent(mk.at[pl.ds(0, Y - 1)], ssem.at[E_M])
    sent(gz.at[:, pl.ds(0, Z - 1)], ssem.at[E_AG])
    sent(rcy, ssem.at[E_RC])
    sent(rx1, ssem.at[E_RX])
    sent(rx2, ssem.at[E_RX2])
    sent(wc, ssem.at[E_WC])
    sent(wx.at[pl.ds(0, X - 1)], ssem.at[E_WX])
    sent(wy.at[pl.ds(0, Y - 1)], ssem.at[E_WY])
    sent(wz.at[pl.ds(0, Z - 1)], ssem.at[E_WZ])
    sent(oz.at[pl.ds(0, Z - 1)], ssem.at[E_OZ])
    sent(oy.at[pl.ds(0, Y - 1)], ssem.at[E_OY])
    sent(ox.at[pl.ds(0, X - 1)], ssem.at[E_OX])
    sent(oc.at[0], ssem.at[E_OC])
    sent(px.at[pl.ds(0, X - 1)], ssem.at[E_PX])
    sent(pz.at[pl.ds(0, C * Z - 1)], ssem.at[E_PZ])
    sent(qz.at[pl.ds(0, Z - 1)], ssem.at[E_QZ])
    sent(qy.at[pl.ds(0, Y - 1)], ssem.at[E_QY])
    sent(qx.at[pl.ds(0, X - 1)], ssem.at[E_QX])
    sent(qxy.at[pl.ds(0, X - 1)], ssem.at[E_QXY])
    sent(qyx.at[pl.ds(0, Y - 1)], ssem.at[E_QYX])


def solution(mesh):
    Y, X, C = Y_DIM, X_DIM, CORES
    Z = mesh.shape["rep"] // Y
    row_spec = P(("rep", "nodes"))

    def device_step(adj_blk, feat_blk, w_one, w_two, label_blk, mask_blk):
        R, S, CB = adj_blk.shape
        F, H = w_one.shape
        NC = w_two.shape[1]
        I = X * C
        NQ = Y * X
        HR = H // (2 * NSUB)
        HB = H // Y
        HU = HB // NV
        NCH = Y * S
        assert R == Z * Y and CB == S * I and X == Y and F + 2 <= LANES // 2 and NC < LANES
        vm = pltpu.VMEM
        dma = pltpu.SemaphoreType.DMA
        scratch = [
            vm((Y, Z, Y, S, CB), BF),
            vm((F, S), BF),
            vm((1, S), jnp.int32),
            vm((1, S), jnp.int32),
            vm((LANES, S), F32),
            vm((S, LANES), F32),
            vm((F, H), F32),
            vm((H, NC), F32),
            vm((2, LANES, H), BF),
            vm((H, LANES), BF),
            vm((LANES, H), BF),
            vm((S // 2, LANES), BF),
            vm((C, NQ, S // 2, LANES), BF),
            vm((NCH, LANES), BF),
            vm((NQ, C, S, H), BF),
            vm((8, LANES), F32),
            vm((Z, 8, LANES), F32),
            vm((2 * NSUB, Z - 1, S, HR), F32),
            vm((2 * NSUB, Z - 1, S, HR), F32),
            vm((S, H), F32),
            vm((S, H), BF),
            vm((S, LANES), BF),
            vm((C, NQ, S, LANES), BF),
            vm((Z, S, LANES), F32),
            vm((Z, S, LANES), F32),
            vm((S, LANES), BF),
            vm((Z, S, LANES), BF),
            vm((Y, X, C, S, LANES), F32),
            vm((Y, X, S, LANES), F32),
            vm((X, Y, S // 2, LANES), F32),
            vm((Y, X, S // 2, LANES), F32),
            vm((Y, S // 2, LANES), F32),
            vm((X, S // 2, LANES), F32),
            vm((S, LANES), BF),
            vm((Y, S, LANES), BF),
            vm((Y, S, HB), BF),
            vm((Y, S, HB), BF),
            vm((NV, Z, Y, S, HU), BF),
            vm((NV // 2, 2 * HU, Z * Y * S), BF),
            vm((NV // 2, X, C, 2 * HU, NCH), F32),
            vm((NV // 2, X, 2 * HU, NCH), F32),
            vm((NV, 2, HU // 2, NCH), F32),
            vm((NV, 2, HU, NCH), F32),
            vm((C, X, Y, Z, 8, LANES), F32),
            vm((X, Y, Z, 8, LANES), F32),
            vm((X, Y, Z, 8, LANES), F32),
            vm((Y, Z, 8, LANES), F32),
            vm((Z, 8, LANES), F32),
            vm((8, LANES), F32),
            vm((Z, 8, LANES), F32),
            vm((Y, Z, 8, LANES), F32),
            vm((X, Y, Z, 8, LANES), F32),
            vm((C, X, Y, Z, 8, LANES), F32),
            vm((X, Z, 8, LANES), F32),
            vm((X, Z, 8, LANES), F32),
            vm((C * Z, 8, LANES), F32),
            vm((8, LANES), F32),
            vm((Z, 8, LANES), F32),
            vm((Y, Z // 2, 8, LANES), F32),
            vm((X, Z // 2, 8, LANES), F32),
            vm((X, Y, Z // 2, 8, LANES), F32),
            vm((Y, X, Z // 2, 8, LANES), F32),
            dma((NSEM,)),
            dma((NSEM,)),
            dma((Y - 1, Z)),
            dma((2, Y - 1)),
            dma((2, Y - 1)),
            dma((2 * NSUB, Z - 1)),
            dma((NV, 2, Z // 2 + 1)),
            dma((NV,)),
            dma((NV, 4)),
        ]
        vspec = pl.BlockSpec(memory_space=pltpu.VMEM)
        aspec = pl.BlockSpec(memory_space=pltpu.HBM)
        operands = (adj_blk.reshape(Z, Y, S, CB), feat_blk.T, label_blk[None, :], mask_blk[None, :], w_one, w_two)
        dw_one, dw_two, loss = pl.pallas_call(
            functools.partial(_step, (Z, Y, X, C, S, CB, H, F, NC)),
            out_shape=(jax.ShapeDtypeStruct((F, H), F32), jax.ShapeDtypeStruct((H, NC), F32), jax.ShapeDtypeStruct((8, LANES), F32)),
            in_specs=[aspec] * 6,
            out_specs=(vspec, vspec, vspec),
            scratch_shapes=scratch,
            compiler_params=pltpu.CompilerParams(collective_id=0, has_side_effects=True, vmem_limit_bytes=52 * 1024 * 1024),
            name="gcn_step",
        )(*[pltpu.with_memory_space_constraint(v, pltpu.HBM) for v in operands])
        return loss[0, 0], dw_one, dw_two

    return jax.shard_map(device_step, mesh=mesh, in_specs=(P(None, "nodes", "rep"), row_spec, P(), P(), row_spec, row_spec), out_specs=(P(), P(), P()), check_vma=False)
```

```python
import functools

import jax
import jax.numpy as jnp
from jax import lax
from jax.experimental import pallas as pl
from jax.experimental.pallas import tpu as pltpu
from jax.sharding import PartitionSpec as P

Y_DIM = 4
X_DIM = 4
CORES = 2
LANES = 128
NSUB = 4
NV = 4
NSEM = 46
BF = jnp.bfloat16
F32 = jnp.float32


def _step(dims, a_hbm, feat_hbm, lab_hbm, msk_hbm, w_one, w_two, dw1_out, dw2_out, loss_out,
          af, feat, lab, msk, mt, mtt, w1f, w2f, w1, w2, w2t, xs, xp, xn, y1, cs, cr, sb, rb, z1, h1, y2, yp, zp, zr, g2, gr, dp, rc, rx, ry, ry2, rx2d,
          d2, dg, ms, mk, gz, gt, dy, rcy, rx1, rx2, wb, wc, wx, wy, wz, wf, oz, oy, ox, oc, pb, px, pz, pf, qz, qy, qx, qxy, qyx,
          ssem, rsem, rsem_a, rsem_b, rsem_f, rsem_ring, rsem_ag, rsem_c, rsem_x):
    Z, Y, X, C, S, CB, H, F, NC = dims
    I = X * C
    NQ = Y * X
    HR = H // (2 * NSUB)
    HB = H // Y
    HU = HB // NV
    NCH = Y * S
    half = Z // 2
    rid = lax.axis_index("rep")
    nid = lax.axis_index("nodes")
    z, y, x, c = rid // Y, rid % Y, nid // C, nid % C
    chip = y * X + x
    partner = (rid, x * C + 1 - c)

    far = sorted(range(1, Z), key=lambda d: -min(d, Z - d))

    def at_z(zz):
        return (zz * Y + y, nid)

    def at_y(yy):
        return (z * Y + yy, nid)

    def at_x(xx):
        return (rid, xx * C + c)

    def at_chip(q):
        return (z * Y + q // X, (q % X) * C + c)

    def send(src, dst, ss, rs, dev):
        pltpu.make_async_remote_copy(src_ref=src, dst_ref=dst, send_sem=ss, recv_sem=rs, device_id=dev,
                                     device_id_type=pl.DeviceIdType.MESH).start()

    def arrived(ref, rs):
        pltpu.make_async_remote_copy(src_ref=ref, dst_ref=ref, send_sem=ssem.at[0], recv_sem=rs, device_id=partner,
                                     device_id_type=pl.DeviceIdType.MESH).wait_recv()

    def sent(ref, ss):
        pltpu.make_async_remote_copy(src_ref=ref, dst_ref=ref, send_sem=ss, recv_sem=rsem.at[0], device_id=partner,
                                     device_id_type=pl.DeviceIdType.MESH).wait_send()

    def dot(a, b):
        return jnp.dot(a, b, preferred_element_type=F32)

    def most(ref):
        return ref.at[0, pl.ds(0, NQ - 1)]

    def plane_rows(ref, yb):
        return jnp.stack([ref[k, yb * X:(yb + 1) * X] for k in range(C)], axis=1).reshape(CB, LANES)

    def turned(v):
        return jnp.concatenate([v[:, LANES // 2:], v[:, 0:LANES // 2]], axis=1)

    def added(ref, n):
        acc = ref[0]
        for k in range(1, n):
            acc = acc + ref[k]
        return acc

    (E_X, E_XC, E_A, E_B, E_F, E_RING, E_CNT, E_Y2, E_Y2C, E_Z2, E_G2, E_DC, E_DC1, E_DC2, E_DC3, E_DX, E_DY, E_AG, E_RC, E_RX, E_RX2,
     E_WC, E_WX, E_WY, E_WZ, E_OZ, E_OY, E_OX, E_OC, E_PX, E_PZ, E_QZ, E_QY, E_QX, E_LA, E_L1, E_L2,
     E_M, E_DY2, E_DX2, E_DG, E_QXY, E_QYX, E_IN, E_IN1, E_IN2) = range(NSEM)

    load_a = pltpu.make_async_copy(a_hbm, af.at[y], ssem.at[E_LA])
    load_1 = pltpu.make_async_copy(w_one, w1f, ssem.at[E_L1])
    load_2 = pltpu.make_async_copy(w_two, w2f, ssem.at[E_L2])
    loads = [pltpu.make_async_copy(src, dst, ssem.at[E_IN + k]) for k, (src, dst) in
             enumerate(((feat_hbm, feat), (lab_hbm, lab), (msk_hbm, msk)))]
    for load in loads:
        load.start()
    load_a.start()
    load_1.start()
    load_2.start()

    bar = pltpu.get_barrier_semaphore()
    for d in far:
        pl.semaphore_signal(bar, inc=1, device_id=at_z((z + d) % Z), device_id_type=pl.DeviceIdType.MESH)

    def greet_plane(d, u):
        pl.semaphore_signal(bar, inc=1, device_id=at_chip(lax.rem(chip + d, NQ)), device_id_type=pl.DeviceIdType.MESH)
        return u

    lax.fori_loop(1, NQ, greet_plane, 0)
    pl.semaphore_signal(bar, inc=1, device_id=partner, device_id_type=pl.DeviceIdType.MESH)

    for load in loads:
        load.wait()
    mt[...] = jnp.zeros_like(mt)
    mt[0:F] = feat[...].astype(F32)
    mt[F:F + 1] = msk[...].astype(F32)
    mt[F + 1:F + 2] = lab[...].astype(F32)
    mtt[...] = mt[...].T
    xs[...] = (mtt[0:S // 2] + turned(mtt[S // 2:S])).astype(BF)
    pl.semaphore_wait(bar, NQ + Z - 1)

    def send_x(d, u):
        q = lax.rem(chip + d, NQ)
        send(xs, xp.at[c, chip], ssem.at[E_X], rsem.at[E_X], at_chip(q))
        return u

    lax.fori_loop(1, NQ, send_x, 0)
    xp[c, chip] = xs[...]
    load_a.wait()

    order = []
    for k in range(1, half + 1):
        order.append(-k)
        if k < half:
            order.append(k)
    order.append(0)
    for k in order:
        zc = (z + k + Z) % Z
        for d in (2, 1, 3):
            yq = (y + d) % Y
            send(af.at[y, zc, yq], af.at[y, zc, yq], ssem.at[E_A], rsem_a.at[d - 1, zc], at_y(yq))
    def spread_a(k):
        for d in (1, 3):
            yq = (y + d) % Y
            ya = (yq + k) % Y
            send(af.at[y, :, ya], af.at[y, :, ya], ssem.at[E_B], rsem_b.at[d // 2, k - 1], at_y(yq))

    def forward_a():
        for k in range(1, Y):
            for d in (1, 3):
                arrived(af.at[0, :, 0], rsem_b.at[d // 2, k - 1])
        for k in range(1, Y):
            for d in (1, 3):
                ys, yq = (y - d + Y) % Y, (y + d) % Y
                lo = 0 if d == 1 else half
                ya = (yq + k) % Y
                send(af.at[ys, pl.ds(lo, half), ya], af.at[ys, pl.ds(lo, half), ya], ssem.at[E_F], rsem_f.at[d // 2, k - 1], at_y(yq))

    spread_a(1)
    spread_a(2)

    load_1.wait()
    w1[...] = jnp.zeros_like(w1)
    w1[0, 0:F] = w1f[...].astype(BF)
    w1[1, LANES // 2:LANES // 2 + F] = w1f[...].astype(BF)
    load_2.wait()
    w2[...] = jnp.zeros_like(w2)
    for k in range(Y):
        rows = slice(k * HB, (k + 1) * HB)
        w2[rows, 0:NC] = w2f[rows].astype(BF)
        w2t[:, rows] = w2[rows].T

    arrived(most(xp), rsem.at[E_X])
    send(xp.at[c], xp.at[c], ssem.at[E_XC], rsem.at[E_XC], partner)

    def columns(j):
        return pl.ds(pl.multiple_of(j * HR, HR), HR)

    def y1_half(k, j):
        rows = xp[k].reshape(NQ * S // 2, LANES)
        for m in range(2):
            y1[:, k, m * (S // 2):(m + 1) * (S // 2), columns(j)] = dot(rows, w1[m, :, columns(j)]).astype(BF).reshape(NQ, S // 2, HR)

    def y1_own(j, u):
        y1_half(c, j)
        return u

    def y1_block(yb, j):
        return y1[yb * X:(yb + 1) * X, :, :, columns(j)].reshape(CB, HR)

    lax.fori_loop(0, 2 * NSUB, y1_own, 0)
    arrived(xp.at[0], rsem.at[E_XC])

    def wait_a(zc):
        for d in range(1, Y):
            arrived(af.at[0, 0, 0], rsem_a.at[d - 1, zc])

    def products(s, j):
        up = j % 2 == 0
        dest = lax.rem(jnp.where(up, z - 1 - s, z + 1 + s) + 2 * Z, Z)
        fresh = ((j == 0) & ((s < half) | (s == Z - 1))) | ((j == 1) & (s < half - 1))

        @pl.when(fresh)
        def _():
            wait_a(dest)

        acc = dot(af[0, dest, y], y1_block(0, j))
        for yb in range(1, Y):
            acc = acc + dot(af[yb, dest, y], y1_block(yb, j))
        return acc

    def pass_on(s, j):
        nb = lax.rem(jnp.where(j % 2 == 0, z + 1, z - 1) + Z, Z)
        send(sb.at[j, s], rb.at[j, s], ssem.at[E_RING], rsem_ring.at[j, s], at_z(nb))

    def ring_first(j, u):
        y1_half(1 - c, j)
        sb[j, 0] = products(0, j)
        pass_on(0, j)
        return u

    def ring_next(t, u):
        s, j = t // (2 * NSUB) + 1, t % (2 * NSUB)
        acc = products(s, j)
        arrived(rb.at[0, 0], rsem_ring.at[j, s - 1])
        sb[j, s] = acc + rb[j, s - 1]
        pass_on(s, j)
        return u

    def ring_last(j, u):
        acc = products(Z - 1, j)
        arrived(rb.at[0, 0], rsem_ring.at[j, Z - 2])
        z1[:, columns(j)] = acc + rb[j, Z - 2]
        return u

    lax.fori_loop(0, 2 * NSUB, ring_first, 0)
    lax.fori_loop(0, (Z - 2) * 2 * NSUB, ring_next, 0)
    lax.fori_loop(0, 2 * NSUB, ring_last, 0)

    h1[...] = jnp.maximum(z1[...], 0.0).astype(BF)
    y2[...] = dot(h1[...], w2[...]).astype(BF)

    def send_y2(d, u):
        q = lax.rem(chip + d, NQ)
        send(y2, yp.at[c, chip], ssem.at[E_Y2], rsem.at[E_Y2], at_chip(q))
        return u

    lax.fori_loop(1, NQ, send_y2, 0)
    yp[c, chip] = y2[...]
    lane = lax.broadcasted_iota(jnp.int32, (S, LANES), 1)
    counted = jnp.sum(xp[...].astype(F32).reshape(Y * CB // 2, LANES), axis=0, keepdims=True)
    counted = jnp.sum(jnp.where(lane[0:1] % (LANES // 2) == F, counted, 0.0), axis=1, keepdims=True)
    cs[...] = jnp.broadcast_to(counted, (8, LANES))
    cr[z] = cs[...]
    for d in far:
        send(cs, cr.at[z], ssem.at[E_CNT], rsem.at[E_CNT], at_z((z + d) % Z))
    arrived(most(yp), rsem.at[E_Y2])
    send(yp.at[c], yp.at[c], ssem.at[E_Y2C], rsem.at[E_Y2C], partner)
    arrived(yp.at[0], rsem.at[E_Y2C])
    def z2_part(zq):
        part = dot(af[0, zq, y], plane_rows(yp, 0))
        for yb in range(1, Y):
            part = part + dot(af[yb, zq, y], plane_rows(yp, yb))
        return part

    for d in far:
        zq = (z + d) % Z
        zp[zq] = z2_part(zq)
        send(zp.at[zq], zr.at[z], ssem.at[E_Z2], rsem.at[E_Z2], at_z(zq))
    zr[z] = z2_part(z)
    for yb in range(Y):
        ms[yb] = jnp.where(z1[:, yb * HB:(yb + 1) * HB] > 0.0, 1.0, 0.0).astype(BF)
    for d in (2, 1, 3):
        yq = (y + d) % Y
        send(ms.at[yq], mk.at[y], ssem.at[E_M], rsem.at[E_M], at_y(yq))
    mk[y] = ms[y]
    spread_a(3)
    arrived(zr.at[pl.ds(0, Z - 1)], rsem.at[E_Z2])
    z2 = added(zr, Z)

    arrived(cr.at[pl.ds(0, Z - 1)], rsem.at[E_CNT])
    count = added(cr, Z)[0:1, 0:1]
    own = mtt[...]
    weights = jnp.sum(jnp.where(lane == F, own, 0.0), axis=1, keepdims=True)
    labels = jnp.sum(jnp.where(lane == F + 1, own, 0.0), axis=1, keepdims=True)
    real = lane < NC
    top = jnp.max(jnp.where(real, z2, -jnp.inf), axis=1, keepdims=True)
    shifted = jnp.where(real, z2 - top, 0.0)
    log_probs = shifted - jnp.log(jnp.sum(jnp.where(real, jnp.exp(shifted), 0.0), axis=1, keepdims=True))
    hot = labels == lane.astype(F32)
    picked = jnp.sum(jnp.where(hot, log_probs, 0.0), axis=1, keepdims=True)
    loss_part = -jnp.sum(weights * picked, axis=0, keepdims=True)
    diff = jnp.where(real, jnp.exp(log_probs), 0.0) - hot.astype(F32)
    g2[...] = (diff * (weights / count)).astype(BF)
    for d in far:
        send(g2, gr.at[z], ssem.at[E_G2], rsem.at[E_G2], at_z((z + d) % Z))
    gr[z] = g2[...]
    arrived(gr.at[pl.ds(0, Z - 1)], rsem.at[E_G2])

    g2t = gr[...].reshape(Z * S, LANES).T
    for yb in range(Y):
        part = dot(g2t, af[yb, :, y].reshape(Z * S, CB))
        dp[yb] = part.T.reshape(X, C, S, LANES)
        send(dp.at[yb, :, 1 - c], rc.at[yb], ssem.at[E_DC + yb], rsem.at[E_DC + yb], partner)
    for yb in range(Y):
        arrived(rc.at[yb], rsem.at[E_DC + yb])
        rc[yb] = rc[yb] + dp[yb, :, c]
    sh = S // 2
    for d in (2, 1, 3):
        xq, yq = (x + d) % X, (y + d) % Y
        send(rc.at[:, xq, pl.ds(0, sh)], rx.at[x], ssem.at[E_DX], rsem.at[E_DX], at_x(xq))
        send(rc.at[yq, :, pl.ds(sh, sh)], ry.at[y], ssem.at[E_DY], rsem.at[E_DY], at_y(yq))
    rx[x] = rc[:, x, 0:sh]
    ry[y] = rc[y, :, sh:S]
    arrived(rx.at[pl.ds(0, X - 1)], rsem.at[E_DX])
    rx[x] = added(rx, X)
    for d in (2, 1, 3):
        yq = (y + d) % Y
        send(rx.at[x, yq], ry2.at[y], ssem.at[E_DY2], rsem.at[E_DY2], at_y(yq))
    ry2[y] = rx[x, y]
    arrived(ry.at[pl.ds(0, Y - 1)], rsem.at[E_DY])
    ry[y] = added(ry, Y)
    for d in (2, 1, 3):
        xq = (x + d) % X
        send(ry.at[y, xq], rx2d.at[x], ssem.at[E_DX2], rsem.at[E_DX2], at_x(xq))
    rx2d[x] = ry[y, x]
    arrived(ry2.at[pl.ds(0, Y - 1)], rsem.at[E_DY2])
    arrived(rx2d.at[pl.ds(0, X - 1)], rsem.at[E_DX2])
    d2[0:sh] = added(ry2, Y).astype(BF)
    d2[sh:S] = added(rx2d, X).astype(BF)
    for d in (2, 1, 3):
        send(d2, dg.at[y], ssem.at[E_DG], rsem.at[E_DG], at_y((y + d) % Y))
    dg[y] = d2[...]
    forward_a()
    dy2 = d2[...]

    def g_one(v):
        col = pl.multiple_of(y * HB + v * HU, HU)
        dh = dot(dg[...].reshape(Y * S, LANES), w2t[:, pl.ds(col, HU)])
        keep = mk[:, :, v * HU:(v + 1) * HU].reshape(Y * S, HU).astype(F32)
        gz[v, z] = jnp.where(keep > 0.0, dh, 0.0).astype(BF).reshape(Y, S, HU)

    def gather_step(v, t):
        for d in range(2):
            sgn = 1 if d == 0 else -1
            blk = (z - sgn * (t - 1) + Z) % Z
            if t > 1:
                arrived(gz.at[v, 0], rsem_ag.at[v, d, t - 1])
            ref = gz.at[v, blk] if t < half else gz.at[v, blk, pl.ds(d * (Y // 2), Y // 2)]
            send(ref, ref, ssem.at[E_AG], rsem_ag.at[v, d, t], at_z((z + sgn + Z) % Z))

    def piece(v):
        return pl.ds(v % 2 * HU, HU)

    def prepare(p):
        for v in (2 * p, 2 * p + 1):
            for d in range(2):
                arrived(gz.at[v, 0, pl.ds(0, Y // 2)], rsem_ag.at[v, d, half])
            for k in range(Z):
                gt[p, piece(v), k * Y * S:(k + 1) * Y * S] = gz[v, k].reshape(Y * S, HU).T

    nxt, prv, opp = (x + 1) % X, (x + X - 1) % X, (x + 2) % X
    hh = HU // 2

    def low(v):
        return pl.ds(v % 2 * HU, hh)

    def high(v):
        return pl.ds(v % 2 * HU + hh, hh)

    def chunk(p, xb, core):
        off = pl.multiple_of(core * NCH, NCH)
        dy[p, xb, core] = dot(gt[p], af[xb, :, :, :, pl.ds(off, NCH)].reshape(Z * Y * S, NCH))

    def send_core(p, k):
        xb = (x + 2 + k) % X
        send(dy.at[p, xb, 1 - c], rcy.at[p, xb], ssem.at[E_RC], rsem_c.at[p, k], partner)

    def chunks_far(p):
        if p == 0:
            for d in (1, 3):
                for k in range(1, Y):
                    arrived(af.at[0, pl.ds(0, half), 0], rsem_f.at[d // 2, k - 1])
        chunk(p, opp, 1 - c)
        send_core(p, 0)
        chunk(p, opp, c)

    def chunks_rest(p, own):
        def body(k, u):
            chunk(p, lax.rem(x + 2 + k, X), c if own else 1 - c)
            return u

        lax.fori_loop(1, X, body, 0)
        if not own:
            for k in range(1, X):
                send_core(p, k)

    def sum_core(p, k):
        xb = (x + 2 + k) % X
        arrived(rcy.at[p, xb], rsem_c.at[p, k])
        rcy[p, xb] = rcy[p, xb] + dy[p, xb, c]

    def reduce_far(p):
        sum_core(p, 0)
        for v in (2 * p, 2 * p + 1):
            send(rcy.at[p, opp, low(v)], rx1.at[v, 0], ssem.at[E_RX], rsem_x.at[v, 0], at_x(nxt))
            send(rcy.at[p, opp, high(v)], rx1.at[v, 1], ssem.at[E_RX], rsem_x.at[v, 1], at_x(prv))

    def reduce_rest(p):
        for k in range(1, X):
            sum_core(p, k)

    def reduce_x(v):
        p = v // 2
        arrived(rx1.at[v, 0], rsem_x.at[v, 0])
        rcy[p, nxt, low(v)] = rcy[p, nxt, low(v)] + rx1[v, 0]
        send(rcy.at[p, nxt, piece(v)], rx2.at[v, 0], ssem.at[E_RX2], rsem_x.at[v, 2], at_x(nxt))
        arrived(rx1.at[v, 1], rsem_x.at[v, 1])
        rcy[p, prv, high(v)] = rcy[p, prv, high(v)] + rx1[v, 1]
        send(rcy.at[p, prv, piece(v)], rx2.at[v, 1], ssem.at[E_RX2], rsem_x.at[v, 3], at_x(prv))

    def own_x():
        low_half = lax.broadcasted_iota(jnp.int32, (S // 2, LANES), 1) < LANES // 2
        for m in range(Y):
            rows = xp[m % C, nid * (Y // C) + m // C].astype(F32)
            xn[m * S:m * S + S // 2] = jnp.where(low_half, rows, 0.0).astype(BF)
            xn[m * S + S // 2:(m + 1) * S] = jnp.where(low_half, turned(rows), 0.0).astype(BF)

    def grad_one(v):
        arrived(rx2.at[v, 0], rsem_x.at[v, 2])
        arrived(rx2.at[v, 1], rsem_x.at[v, 3])
        acc = (rcy[v // 2, x, piece(v)] + rx2[v, 0] + rx2[v, 1]).astype(BF)
        part = dot(acc, xn[...])
        if v >= NV // 2:
            part = turned(part)
        per = HU // (Z * 8)
        rows = part.reshape(per, Z, 8, LANES)
        for m in range(per):
            k = (v % (NV // 2)) * per + m
            pb[k] = rows[m] if v < NV // 2 else pb[k] + rows[m]

    def w_begin():
        mark = (lax.broadcasted_iota(jnp.int32, (HB, LANES), 0) == 0) & (lax.broadcasted_iota(jnp.int32, (HB, LANES), 1) == NC)
        for k in range(Y):
            part = lax.dot_general(h1[:, k * HB:(k + 1) * HB], dy2, (((0,), (0,)), ((), ())), preferred_element_type=F32)
            if k == 0:
                part = jnp.where(mark, loss_part, part)
            per = HB // (Y * Z * 8)
            rows = part.reshape(per, Y, Z, 8, LANES)
            for m in range(per):
                q = k * per + m
                wb[q // X, q % X] = rows[m]
        send(wb.at[1 - c], wc, ssem.at[E_WC], rsem.at[E_WC], partner)

    def w_core():
        arrived(wc, rsem.at[E_WC])
        wc[...] = wc[...] + wb[c]
        for d in (2, 1, 3):
            xq = (x + d) % X
            send(wc.at[xq], wx.at[x], ssem.at[E_WX], rsem.at[E_WX], at_x(xq))
        wx[x] = wc[x]

    def w_x():
        arrived(wx.at[pl.ds(0, X - 1)], rsem.at[E_WX])
        wx[x] = added(wx, X)
        for d in (2, 1, 3):
            yq = (y + d) % Y
            send(wx.at[x, yq], wy.at[y], ssem.at[E_WY], rsem.at[E_WY], at_y(yq))
        wy[y] = wx[x, y]

    def w_y():
        arrived(wy.at[pl.ds(0, Y - 1)], rsem.at[E_WY])
        wy[y] = added(wy, Y)
        for d in far:
            zq = (z + d) % Z
            send(wy.at[y, zq], wz.at[z], ssem.at[E_WZ], rsem.at[E_WZ], at_z(zq))
        wz[z] = wy[y, z]

    def w_z():
        arrived(wz.at[pl.ds(0, Z - 1)], rsem.at[E_WZ])
        wf[...] = added(wz, Z)
        for d in far:
            send(wf, oz.at[z], ssem.at[E_OZ], rsem.at[E_OZ], at_z((z + d) % Z))
        oz[z] = wf[...]

    def o_z():
        arrived(oz.at[pl.ds(0, Z - 1)], rsem.at[E_OZ])
        for d in (2, 1, 3):
            send(oz, oy.at[y], ssem.at[E_OY], rsem.at[E_OY], at_y((y + d) % Y))
        oy[y] = oz[...]

    def o_y():
        arrived(oy.at[pl.ds(0, Y - 1)], rsem.at[E_OY])
        for d in (2, 1, 3):
            send(oy, ox.at[x], ssem.at[E_OX], rsem.at[E_OX], at_x((x + d) % X))
        ox[x] = oy[...]

    def o_x():
        arrived(ox.at[pl.ds(0, X - 1)], rsem.at[E_OX])
        send(ox, oc.at[c], ssem.at[E_OC], rsem.at[E_OC], partner)
        oc[c] = ox[...]

    arrived(mk.at[pl.ds(0, Y - 1)], rsem.at[E_M])
    arrived(dg.at[pl.ds(0, Y - 1)], rsem.at[E_DG])
    steps = [
        (g_one, 0), (gather_step, 0, 1), (g_one, 1), (gather_step, 1, 1), (g_one, 2), (g_one, 3), (w_begin,), (own_x,),
        (gather_step, 0, 2), (gather_step, 1, 2), (w_core,)]
    for t in range(3, half + 1):
        steps += [(gather_step, 0, t), (gather_step, 1, t)]
    steps += [(gather_step, 2, 1), (gather_step, 3, 1), (prepare, 0), (chunks_far, 0), (gather_step, 2, 2), (gather_step, 3, 2),
              (reduce_far, 0), (chunks_rest, 0, False)]
    for t in range(3, half + 1):
        steps += [(gather_step, 2, t), (gather_step, 3, t)]
        if t == 3:
            steps += [(chunks_rest, 0, True), (reduce_rest, 0), (w_x,)]
    steps += [(reduce_x, 0), (reduce_x, 1), (w_y,), (prepare, 1), (chunks_far, 1), (reduce_far, 1), (chunks_rest, 1, False),
              (chunks_rest, 1, True), (reduce_rest, 1), (grad_one, 0), (grad_one, 1), (w_z,), (reduce_x, 2), (reduce_x, 3), (o_z,),
              (grad_one, 2), (grad_one, 3)]
    for step in steps:
        step[0](*step[1:])

    for d in (2, 1, 3):
        xq = (x + d) % X
        send(pb.at[xq], px.at[x], ssem.at[E_PX], rsem.at[E_PX], at_x(xq))
    px[x] = pb[x]
    arrived(px.at[pl.ds(0, X - 1)], rsem.at[E_PX])
    px[x] = added(px, X)
    for d in far:
        zq = (z + d) % Z
        for k in range(C):
            send(px.at[x, zq], pz.at[c * Z + z], ssem.at[E_PZ], rsem.at[E_PZ], (zq * Y + y, x * C + k))
    send(px.at[x, z], pz.at[c * Z + z], ssem.at[E_PZ], rsem.at[E_PZ], partner)
    pz[c * Z + z] = px[x, z]
    o_y()
    arrived(pz.at[pl.ds(0, C * Z - 1)], rsem.at[E_PZ])
    pf[...] = added(pz, C * Z)
    for d in far:
        send(pf, qz.at[z], ssem.at[E_QZ], rsem.at[E_QZ], at_z((z + d) % Z))
    qz[z] = pf[...]
    arrived(qz.at[pl.ds(0, Z - 1)], rsem.at[E_QZ])
    zl, zh = pl.ds(0, half), pl.ds(half, half)
    for d in (2, 1, 3):
        send(qz.at[zl], qy.at[y], ssem.at[E_QY], rsem.at[E_QY], at_y((y + d) % Y))
        send(qz.at[zh], qx.at[x], ssem.at[E_QX], rsem.at[E_QX], at_x((x + d) % X))
    qy[y] = qz[zl]
    qx[x] = qz[zh]
    o_x()
    arrived(qy.at[pl.ds(0, Y - 1)], rsem.at[E_QY])
    for d in (2, 1, 3):
        send(qy, qxy.at[x], ssem.at[E_QXY], rsem.at[E_QXY], at_x((x + d) % X))
    qxy[x] = qy[...]
    arrived(qx.at[pl.ds(0, X - 1)], rsem.at[E_QX])
    for d in (2, 1, 3):
        send(qx, qyx.at[y], ssem.at[E_QYX], rsem.at[E_QYX], at_y((y + d) % Y))
    qyx[y] = qx[...]
    arrived(oc.at[0], rsem.at[E_OC])
    for k in range(C):
        full = oc[k].reshape(H // C, LANES)
        dw2_out[k * (H // C):(k + 1) * (H // C), :] = full[:, 0:NC]
        if k == 0:
            loss_out[...] = jnp.broadcast_to(full[0:1, NC:NC + 1] / count, (8, LANES))
    arrived(qxy.at[pl.ds(0, X - 1)], rsem.at[E_QXY])
    arrived(qyx.at[pl.ds(0, Y - 1)], rsem.at[E_QYX])
    for yb in range(Y):
        part = jnp.concatenate([qxy[:, yb], qyx[yb]], axis=1).reshape(HB // 2, LANES).T
        dw1_out[:, yb * HB:yb * HB + HB // 2] = part[0:F]
        dw1_out[:, yb * HB + HB // 2:(yb + 1) * HB] = part[LANES // 2:LANES // 2 + F]

    sent(most(xp), ssem.at[E_X])
    sent(xp.at[0], ssem.at[E_XC])
    sent(af.at[pl.ds(0, Y - 1), :, 0], ssem.at[E_A])
    sent(af.at[pl.ds(0, Y - 1), :, pl.ds(0, 2)], ssem.at[E_B])
    sent(af.at[pl.ds(0, Y - 1), :, 0], ssem.at[E_F])
    sent(sb, ssem.at[E_RING])
    sent(cr.at[pl.ds(0, Z - 1)], ssem.at[E_CNT])
    sent(most(yp), ssem.at[E_Y2])
    sent(yp.at[0], ssem.at[E_Y2C])
    sent(zr.at[pl.ds(0, Z - 1)], ssem.at[E_Z2])
    sent(gr.at[pl.ds(0, Z - 1)], ssem.at[E_G2])
    for yb in range(Y):
        sent(rc.at[yb], ssem.at[E_DC + yb])
    sent(rx.at[pl.ds(0, X - 1)], ssem.at[E_DX])
    sent(ry.at[pl.ds(0, Y - 1)], ssem.at[E_DY])
    sent(ry2.at[pl.ds(0, Y - 1)], ssem.at[E_DY2])
    sent(rx2d.at[pl.ds(0, X - 1)], ssem.at[E_DX2])
    sent(dg.at[pl.ds(0, Y - 1)], ssem.at[E_DG])
    sent(mk.at[pl.ds(0, Y - 1)], ssem.at[E_M])
    sent(gz.at[:, pl.ds(0, Z - 1)], ssem.at[E_AG])
    sent(rcy, ssem.at[E_RC])
    sent(rx1, ssem.at[E_RX])
    sent(rx2, ssem.at[E_RX2])
    sent(wc, ssem.at[E_WC])
    sent(wx.at[pl.ds(0, X - 1)], ssem.at[E_WX])
    sent(wy.at[pl.ds(0, Y - 1)], ssem.at[E_WY])
    sent(wz.at[pl.ds(0, Z - 1)], ssem.at[E_WZ])
    sent(oz.at[pl.ds(0, Z - 1)], ssem.at[E_OZ])
    sent(oy.at[pl.ds(0, Y - 1)], ssem.at[E_OY])
    sent(ox.at[pl.ds(0, X - 1)], ssem.at[E_OX])
    sent(oc.at[0], ssem.at[E_OC])
    sent(px.at[pl.ds(0, X - 1)], ssem.at[E_PX])
    sent(pz.at[pl.ds(0, C * Z - 1)], ssem.at[E_PZ])
    sent(qz.at[pl.ds(0, Z - 1)], ssem.at[E_QZ])
    sent(qy.at[pl.ds(0, Y - 1)], ssem.at[E_QY])
    sent(qx.at[pl.ds(0, X - 1)], ssem.at[E_QX])
    sent(qxy.at[pl.ds(0, X - 1)], ssem.at[E_QXY])
    sent(qyx.at[pl.ds(0, Y - 1)], ssem.at[E_QYX])


def solution(mesh):
    Y, X, C = Y_DIM, X_DIM, CORES
    Z = mesh.shape["rep"] // Y
    row_spec = P(("rep", "nodes"))

    def device_step(adj_blk, feat_blk, w_one, w_two, label_blk, mask_blk):
        R, S, CB = adj_blk.shape
        F, H = w_one.shape
        NC = w_two.shape[1]
        I = X * C
        NQ = Y * X
        HR = H // (2 * NSUB)
        HB = H // Y
        HU = HB // NV
        NCH = Y * S
        assert R == Z * Y and CB == S * I and X == Y and F + 2 <= LANES // 2 and NC < LANES
        vm = pltpu.VMEM
        dma = pltpu.SemaphoreType.DMA
        scratch = [
            vm((Y, Z, Y, S, CB), BF),
            vm((F, S), BF),
            vm((1, S), jnp.int32),
            vm((1, S), jnp.int32),
            vm((LANES, S), F32),
            vm((S, LANES), F32),
            vm((F, H), F32),
            vm((H, NC), F32),
            vm((2, LANES, H), BF),
            vm((H, LANES), BF),
            vm((LANES, H), BF),
            vm((S // 2, LANES), BF),
            vm((C, NQ, S // 2, LANES), BF),
            vm((NCH, LANES), BF),
            vm((NQ, C, S, H), BF),
            vm((8, LANES), F32),
            vm((Z, 8, LANES), F32),
            vm((2 * NSUB, Z - 1, S, HR), F32),
            vm((2 * NSUB, Z - 1, S, HR), F32),
            vm((S, H), F32),
            vm((S, H), BF),
            vm((S, LANES), BF),
            vm((C, NQ, S, LANES), BF),
            vm((Z, S, LANES), F32),
            vm((Z, S, LANES), F32),
            vm((S, LANES), BF),
            vm((Z, S, LANES), BF),
            vm((Y, X, C, S, LANES), F32),
            vm((Y, X, S, LANES), F32),
            vm((X, Y, S // 2, LANES), F32),
            vm((Y, X, S // 2, LANES), F32),
            vm((Y, S // 2, LANES), F32),
            vm((X, S // 2, LANES), F32),
            vm((S, LANES), BF),
            vm((Y, S, LANES), BF),
            vm((Y, S, HB), BF),
            vm((Y, S, HB), BF),
            vm((NV, Z, Y, S, HU), BF),
            vm((NV // 2, 2 * HU, Z * Y * S), BF),
            vm((NV // 2, X, C, 2 * HU, NCH), F32),
            vm((NV // 2, X, 2 * HU, NCH), F32),
            vm((NV, 2, HU // 2, NCH), F32),
            vm((NV, 2, HU, NCH), F32),
            vm((C, X, Y, Z, 8, LANES), F32),
            vm((X, Y, Z, 8, LANES), F32),
            vm((X, Y, Z, 8, LANES), F32),
            vm((Y, Z, 8, LANES), F32),
            vm((Z, 8, LANES), F32),
            vm((8, LANES), F32),
            vm((Z, 8, LANES), F32),
            vm((Y, Z, 8, LANES), F32),
            vm((X, Y, Z, 8, LANES), F32),
            vm((C, X, Y, Z, 8, LANES), F32),
            vm((X, Z, 8, LANES), F32),
            vm((X, Z, 8, LANES), F32),
            vm((C * Z, 8, LANES), F32),
            vm((8, LANES), F32),
            vm((Z, 8, LANES), F32),
            vm((Y, Z // 2, 8, LANES), F32),
            vm((X, Z // 2, 8, LANES), F32),
            vm((X, Y, Z // 2, 8, LANES), F32),
            vm((Y, X, Z // 2, 8, LANES), F32),
            dma((NSEM,)),
            dma((NSEM,)),
            dma((Y - 1, Z)),
            dma((2, Y - 1)),
            dma((2, Y - 1)),
            dma((2 * NSUB, Z - 1)),
            dma((NV, 2, Z // 2 + 1)),
            dma((NV // 2, X)),
            dma((NV, 4)),
        ]
        vspec = pl.BlockSpec(memory_space=pltpu.VMEM)
        aspec = pl.BlockSpec(memory_space=pltpu.HBM)
        operands = (adj_blk.reshape(Z, Y, S, CB), feat_blk.T, label_blk[None, :], mask_blk[None, :], w_one, w_two)
        dw_one, dw_two, loss = pl.pallas_call(
            functools.partial(_step, (Z, Y, X, C, S, CB, H, F, NC)),
            out_shape=(jax.ShapeDtypeStruct((F, H), F32), jax.ShapeDtypeStruct((H, NC), F32), jax.ShapeDtypeStruct((8, LANES), F32)),
            in_specs=[aspec] * 6,
            out_specs=(vspec, vspec, vspec),
            scratch_shapes=scratch,
            compiler_params=pltpu.CompilerParams(collective_id=0, has_side_effects=True, vmem_limit_bytes=52 * 1024 * 1024),
            name="gcn_step",
        )(*[pltpu.with_memory_space_constraint(v, pltpu.HBM) for v in operands])
        return loss[0, 0], dw_one, dw_two

    return jax.shard_map(device_step, mesh=mesh, in_specs=(P(None, "nodes", "rep"), row_spec, P(), P(), row_spec, row_spec), out_specs=(P(), P(), P()), check_vma=False)
```

```python
import functools

import jax
import jax.numpy as jnp
from jax import lax
from jax.experimental import pallas as pl
from jax.experimental.pallas import tpu as pltpu
from jax.sharding import PartitionSpec as P

Y_DIM = 4
X_DIM = 4
CORES = 2
LANES = 128
NSUB = 4
NV = 4
NSEM = 46
BF = jnp.bfloat16
F32 = jnp.float32


def _step(dims, a_hbm, feat_hbm, lab_hbm, msk_hbm, w_one, w_two, dw1_out, dw2_out, loss_out,
          af, feat, lab, msk, mt, mtt, w1f, w2f, w1, w2, w2t, xs, xp, xn, y1, cs, cr, sb, rb, z1, h1, y2, yp, zp, zr, g2, gr, dp, rc, rx, ry, ry2, rx2d,
          d2, dg, ms, mk, gz, gt, dy, rcy, rx1, rx2, wb, wc, wx, wy, wz, wf, oz, oy, ox, oc, pb, px, pz, pf, qz, qy, qx, qxy, qyx,
          ssem, rsem, rsem_a, rsem_b, rsem_f, rsem_ring, rsem_ag, rsem_c, rsem_x):
    Z, Y, X, C, S, CB, H, F, NC = dims
    I = X * C
    NQ = Y * X
    HR = H // (2 * NSUB)
    HB = H // Y
    HU = HB // NV
    NCH = Y * S
    half = Z // 2
    rid = lax.axis_index("rep")
    nid = lax.axis_index("nodes")
    z, y, x, c = rid // Y, rid % Y, nid // C, nid % C
    chip = y * X + x
    partner = (rid, x * C + 1 - c)

    far = sorted(range(1, Z), key=lambda d: -min(d, Z - d))

    def at_z(zz):
        return (zz * Y + y, nid)

    def at_y(yy):
        return (z * Y + yy, nid)

    def at_x(xx):
        return (rid, xx * C + c)

    def at_chip(q):
        return (z * Y + q // X, (q % X) * C + c)

    def send(src, dst, ss, rs, dev):
        pltpu.make_async_remote_copy(src_ref=src, dst_ref=dst, send_sem=ss, recv_sem=rs, device_id=dev,
                                     device_id_type=pl.DeviceIdType.MESH).start()

    def arrived(ref, rs):
        pltpu.make_async_remote_copy(src_ref=ref, dst_ref=ref, send_sem=ssem.at[0], recv_sem=rs, device_id=partner,
                                     device_id_type=pl.DeviceIdType.MESH).wait_recv()

    def sent(ref, ss):
        pltpu.make_async_remote_copy(src_ref=ref, dst_ref=ref, send_sem=ss, recv_sem=rsem.at[0], device_id=partner,
                                     device_id_type=pl.DeviceIdType.MESH).wait_send()

    def dot(a, b):
        return jnp.dot(a, b, preferred_element_type=F32)

    def most(ref):
        return ref.at[0, pl.ds(0, NQ - 1)]

    def plane_rows(ref, yb):
        return jnp.stack([ref[k, yb * X:(yb + 1) * X] for k in range(C)], axis=1).reshape(CB, LANES)

    def turned(v):
        return jnp.concatenate([v[:, LANES // 2:], v[:, 0:LANES // 2]], axis=1)

    def added(ref, n):
        acc = ref[0]
        for k in range(1, n):
            acc = acc + ref[k]
        return acc

    (E_X, E_XC, E_A, E_B, E_F, E_RING, E_CNT, E_Y2, E_Y2C, E_Z2, E_G2, E_DC, E_DC1, E_DC2, E_DC3, E_DX, E_DY, E_AG, E_RC, E_RX, E_RX2,
     E_WC, E_WX, E_WY, E_WZ, E_OZ, E_OY, E_OX, E_OC, E_PX, E_PZ, E_QZ, E_QY, E_QX, E_LA, E_L1, E_L2,
     E_M, E_DY2, E_DX2, E_DG, E_QXY, E_QYX, E_IN, E_IN1, E_IN2) = range(NSEM)

    load_a = pltpu.make_async_copy(a_hbm, af.at[y], ssem.at[E_LA])
    load_1 = pltpu.make_async_copy(w_one, w1f, ssem.at[E_L1])
    load_2 = pltpu.make_async_copy(w_two, w2f, ssem.at[E_L2])
    loads = [pltpu.make_async_copy(src, dst, ssem.at[E_IN + k]) for k, (src, dst) in
             enumerate(((feat_hbm, feat), (lab_hbm, lab), (msk_hbm, msk)))]
    for load in loads:
        load.start()
    load_a.start()
    load_1.start()
    load_2.start()

    bar = pltpu.get_barrier_semaphore()
    for d in far:
        pl.semaphore_signal(bar, inc=1, device_id=at_z((z + d) % Z), device_id_type=pl.DeviceIdType.MESH)

    def greet_plane(d, u):
        pl.semaphore_signal(bar, inc=1, device_id=at_chip(lax.rem(chip + d, NQ)), device_id_type=pl.DeviceIdType.MESH)
        return u

    lax.fori_loop(1, NQ, greet_plane, 0)
    pl.semaphore_signal(bar, inc=1, device_id=partner, device_id_type=pl.DeviceIdType.MESH)

    for load in loads:
        load.wait()
    mt[...] = jnp.zeros_like(mt)
    mt[0:F] = feat[...].astype(F32)
    mt[F:F + 1] = msk[...].astype(F32)
    mt[F + 1:F + 2] = lab[...].astype(F32)
    mtt[...] = mt[...].T
    xs[...] = (mtt[0:S // 2] + turned(mtt[S // 2:S])).astype(BF)
    pl.semaphore_wait(bar, NQ + Z - 1)

    def send_x(d, u):
        q = lax.rem(chip + d, NQ)
        send(xs, xp.at[c, chip], ssem.at[E_X], rsem.at[E_X], at_chip(q))
        return u

    lax.fori_loop(1, NQ, send_x, 0)
    xp[c, chip] = xs[...]
    load_a.wait()

    order = []
    for k in range(1, half + 1):
        order.append(-k)
        if k < half:
            order.append(k)
    order.append(0)
    for k in order:
        zc = (z + k + Z) % Z
        for d in (2, 1, 3):
            yq = (y + d) % Y
            send(af.at[y, zc, yq], af.at[y, zc, yq], ssem.at[E_A], rsem_a.at[d - 1, zc], at_y(yq))
    def spread_a(k):
        for d in (1, 3):
            yq = (y + d) % Y
            ya = (yq + k) % Y
            send(af.at[y, :, ya], af.at[y, :, ya], ssem.at[E_B], rsem_b.at[d // 2, k - 1], at_y(yq))

    def forward_a():
        for k in range(1, Y):
            for d in (1, 3):
                arrived(af.at[0, :, 0], rsem_b.at[d // 2, k - 1])
        for k in range(1, Y):
            for d in (1, 3):
                ys, yq = (y - d + Y) % Y, (y + d) % Y
                lo = 0 if d == 1 else half
                ya = (yq + k) % Y
                send(af.at[ys, pl.ds(lo, half), ya], af.at[ys, pl.ds(lo, half), ya], ssem.at[E_F], rsem_f.at[d // 2, k - 1], at_y(yq))

    spread_a(1)
    spread_a(2)

    load_1.wait()
    w1[...] = jnp.zeros_like(w1)
    w1[0, 0:F] = w1f[...].astype(BF)
    w1[1, LANES // 2:LANES // 2 + F] = w1f[...].astype(BF)
    load_2.wait()
    w2[...] = jnp.zeros_like(w2)
    for k in range(Y):
        rows = slice(k * HB, (k + 1) * HB)
        w2[rows, 0:NC] = w2f[rows].astype(BF)
        w2t[:, rows] = w2[rows].T

    arrived(most(xp), rsem.at[E_X])
    send(xp.at[c], xp.at[c], ssem.at[E_XC], rsem.at[E_XC], partner)

    def columns(j):
        return pl.ds(pl.multiple_of(j * HR, HR), HR)

    def y1_half(k, j):
        rows = xp[k].reshape(NQ * S // 2, LANES)
        for m in range(2):
            y1[:, k, m * (S // 2):(m + 1) * (S // 2), columns(j)] = dot(rows, w1[m, :, columns(j)]).astype(BF).reshape(NQ, S // 2, HR)

    def y1_own(j, u):
        y1_half(c, j)
        return u

    def y1_block(yb, j):
        return y1[yb * X:(yb + 1) * X, :, :, columns(j)].reshape(CB, HR)

    lax.fori_loop(0, 2 * NSUB, y1_own, 0)
    arrived(xp.at[0], rsem.at[E_XC])

    def wait_a(zc):
        for d in range(1, Y):
            arrived(af.at[0, 0, 0], rsem_a.at[d - 1, zc])

    def products(s, j):
        up = j % 2 == 0
        dest = lax.rem(jnp.where(up, z - 1 - s, z + 1 + s) + 2 * Z, Z)
        fresh = ((j == 0) & ((s < half) | (s == Z - 1))) | ((j == 1) & (s < half - 1))

        @pl.when(fresh)
        def _():
            wait_a(dest)

        acc = dot(af[0, dest, y], y1_block(0, j))
        for yb in range(1, Y):
            acc = acc + dot(af[yb, dest, y], y1_block(yb, j))
        return acc

    def pass_on(s, j):
        nb = lax.rem(jnp.where(j % 2 == 0, z + 1, z - 1) + Z, Z)
        send(sb.at[j, s], rb.at[j, s], ssem.at[E_RING], rsem_ring.at[j, s], at_z(nb))

    def ring_first(j, u):
        y1_half(1 - c, j)
        sb[j, 0] = products(0, j)
        pass_on(0, j)
        return u

    def ring_next(t, u):
        s, j = t // (2 * NSUB) + 1, t % (2 * NSUB)
        acc = products(s, j)
        arrived(rb.at[0, 0], rsem_ring.at[j, s - 1])
        sb[j, s] = acc + rb[j, s - 1]
        pass_on(s, j)
        return u

    def ring_last(j, u):
        acc = products(Z - 1, j)
        arrived(rb.at[0, 0], rsem_ring.at[j, Z - 2])
        z1[:, columns(j)] = acc + rb[j, Z - 2]
        return u

    lax.fori_loop(0, 2 * NSUB, ring_first, 0)
    lax.fori_loop(0, (Z - 2) * 2 * NSUB, ring_next, 0)
    lax.fori_loop(0, 2 * NSUB, ring_last, 0)

    h1[...] = jnp.maximum(z1[...], 0.0).astype(BF)
    y2[...] = dot(h1[...], w2[...]).astype(BF)

    def send_y2(d, u):
        q = lax.rem(chip + d, NQ)
        send(y2, yp.at[c, chip], ssem.at[E_Y2], rsem.at[E_Y2], at_chip(q))
        return u

    lax.fori_loop(1, NQ, send_y2, 0)
    yp[c, chip] = y2[...]
    lane = lax.broadcasted_iota(jnp.int32, (S, LANES), 1)
    counted = jnp.sum(xp[...].astype(F32).reshape(Y * CB // 2, LANES), axis=0, keepdims=True)
    counted = jnp.sum(jnp.where(lane[0:1] % (LANES // 2) == F, counted, 0.0), axis=1, keepdims=True)
    cs[...] = jnp.broadcast_to(counted, (8, LANES))
    cr[z] = cs[...]
    for d in far:
        send(cs, cr.at[z], ssem.at[E_CNT], rsem.at[E_CNT], at_z((z + d) % Z))
    arrived(most(yp), rsem.at[E_Y2])
    send(yp.at[c], yp.at[c], ssem.at[E_Y2C], rsem.at[E_Y2C], partner)
    arrived(yp.at[0], rsem.at[E_Y2C])
    def z2_part(zq):
        part = dot(af[0, zq, y], plane_rows(yp, 0))
        for yb in range(1, Y):
            part = part + dot(af[yb, zq, y], plane_rows(yp, yb))
        return part

    for d in far:
        zq = (z + d) % Z
        zp[zq] = z2_part(zq)
        send(zp.at[zq], zr.at[z], ssem.at[E_Z2], rsem.at[E_Z2], at_z(zq))
    zr[z] = z2_part(z)
    for yb in range(Y):
        ms[yb] = jnp.where(z1[:, yb * HB:(yb + 1) * HB] > 0.0, 1.0, 0.0).astype(BF)
    for d in (2, 1, 3):
        yq = (y + d) % Y
        send(ms.at[yq], mk.at[y], ssem.at[E_M], rsem.at[E_M], at_y(yq))
    mk[y] = ms[y]
    spread_a(3)
    arrived(zr.at[pl.ds(0, Z - 1)], rsem.at[E_Z2])
    z2 = added(zr, Z)

    arrived(cr.at[pl.ds(0, Z - 1)], rsem.at[E_CNT])
    count = added(cr, Z)[0:1, 0:1]
    own = mtt[...]
    weights = jnp.sum(jnp.where(lane == F, own, 0.0), axis=1, keepdims=True)
    labels = jnp.sum(jnp.where(lane == F + 1, own, 0.0), axis=1, keepdims=True)
    real = lane < NC
    top = jnp.max(jnp.where(real, z2, -jnp.inf), axis=1, keepdims=True)
    shifted = jnp.where(real, z2 - top, 0.0)
    log_probs = shifted - jnp.log(jnp.sum(jnp.where(real, jnp.exp(shifted), 0.0), axis=1, keepdims=True))
    hot = labels == lane.astype(F32)
    picked = jnp.sum(jnp.where(hot, log_probs, 0.0), axis=1, keepdims=True)
    loss_part = -jnp.sum(weights * picked, axis=0, keepdims=True)
    diff = jnp.where(real, jnp.exp(log_probs), 0.0) - hot.astype(F32)
    g2[...] = (diff * (weights / count)).astype(BF)
    for d in far:
        send(g2, gr.at[z], ssem.at[E_G2], rsem.at[E_G2], at_z((z + d) % Z))
    gr[z] = g2[...]
    arrived(gr.at[pl.ds(0, Z - 1)], rsem.at[E_G2])

    g2t = gr[...].reshape(Z * S, LANES).T
    for yb in range(Y):
        part = dot(g2t, af[yb, :, y].reshape(Z * S, CB))
        dp[yb] = part.T.reshape(X, C, S, LANES)
        send(dp.at[yb, :, 1 - c], rc.at[yb], ssem.at[E_DC + yb], rsem.at[E_DC + yb], partner)
    for yb in range(Y):
        arrived(rc.at[yb], rsem.at[E_DC + yb])
        rc[yb] = rc[yb] + dp[yb, :, c]
    sh = S // 2
    for d in (2, 1, 3):
        xq, yq = (x + d) % X, (y + d) % Y
        send(rc.at[:, xq, pl.ds(0, sh)], rx.at[x], ssem.at[E_DX], rsem.at[E_DX], at_x(xq))
        send(rc.at[yq, :, pl.ds(sh, sh)], ry.at[y], ssem.at[E_DY], rsem.at[E_DY], at_y(yq))
    rx[x] = rc[:, x, 0:sh]
    ry[y] = rc[y, :, sh:S]
    arrived(rx.at[pl.ds(0, X - 1)], rsem.at[E_DX])
    rx[x] = added(rx, X)
    for d in (2, 1, 3):
        yq = (y + d) % Y
        send(rx.at[x, yq], ry2.at[y], ssem.at[E_DY2], rsem.at[E_DY2], at_y(yq))
    ry2[y] = rx[x, y]
    arrived(ry.at[pl.ds(0, Y - 1)], rsem.at[E_DY])
    ry[y] = added(ry, Y)
    for d in (2, 1, 3):
        xq = (x + d) % X
        send(ry.at[y, xq], rx2d.at[x], ssem.at[E_DX2], rsem.at[E_DX2], at_x(xq))
    rx2d[x] = ry[y, x]
    arrived(ry2.at[pl.ds(0, Y - 1)], rsem.at[E_DY2])
    arrived(rx2d.at[pl.ds(0, X - 1)], rsem.at[E_DX2])
    d2[0:sh] = added(ry2, Y).astype(BF)
    d2[sh:S] = added(rx2d, X).astype(BF)
    for d in (2, 1, 3):
        send(d2, dg.at[y], ssem.at[E_DG], rsem.at[E_DG], at_y((y + d) % Y))
    dg[y] = d2[...]
    forward_a()
    dy2 = d2[...]

    def g_one(v):
        col = pl.multiple_of(y * HB + v * HU, HU)
        dh = dot(dg[...].reshape(Y * S, LANES), w2t[:, pl.ds(col, HU)])
        keep = mk[:, :, v * HU:(v + 1) * HU].reshape(Y * S, HU).astype(F32)
        gz[v, z] = jnp.where(keep > 0.0, dh, 0.0).astype(BF).reshape(Y, S, HU)

    def gather_step(v, t):
        for d in range(2):
            sgn = 1 if d == 0 else -1
            blk = (z - sgn * (t - 1) + Z) % Z
            if t > 1:
                arrived(gz.at[v, 0], rsem_ag.at[v, d, t - 1])
            ref = gz.at[v, blk] if t < half else gz.at[v, blk, pl.ds(d * (Y // 2), Y // 2)]
            send(ref, ref, ssem.at[E_AG], rsem_ag.at[v, d, t], at_z((z + sgn + Z) % Z))

    def piece(v):
        return pl.ds(v % 2 * HU, HU)

    def prepare(p):
        for v in (2 * p, 2 * p + 1):
            for d in range(2):
                arrived(gz.at[v, 0, pl.ds(0, Y // 2)], rsem_ag.at[v, d, half])
            for k in range(Z):
                gt[p, piece(v), k * Y * S:(k + 1) * Y * S] = gz[v, k].reshape(Y * S, HU).T

    nxt, prv, opp = (x + 1) % X, (x + X - 1) % X, (x + 2) % X
    hh = HU // 2

    def low(v):
        return pl.ds(v % 2 * HU, hh)

    def high(v):
        return pl.ds(v % 2 * HU + hh, hh)

    def chunk(p, xb, core):
        off = pl.multiple_of(core * NCH, NCH)
        dy[p, xb, core] = dot(gt[p], af[xb, :, :, :, pl.ds(off, NCH)].reshape(Z * Y * S, NCH))

    def send_core(p, k):
        xb = (x + 2 + k) % X
        send(dy.at[p, xb, 1 - c], rcy.at[p, xb], ssem.at[E_RC], rsem_c.at[p, k], partner)

    def chunks_far(p):
        if p == 0:
            for d in (1, 3):
                for k in range(1, Y):
                    arrived(af.at[0, pl.ds(0, half), 0], rsem_f.at[d // 2, k - 1])
        chunk(p, opp, 1 - c)
        send_core(p, 0)
        chunk(p, opp, c)

    def chunks_rest(p, own):
        def body(k, u):
            chunk(p, lax.rem(x + 2 + k, X), c if own else 1 - c)
            return u

        lax.fori_loop(1, X, body, 0)
        if not own:
            for k in range(1, X):
                send_core(p, k)

    def sum_core(p, k):
        xb = (x + 2 + k) % X
        arrived(rcy.at[p, xb], rsem_c.at[p, k])
        rcy[p, xb] = rcy[p, xb] + dy[p, xb, c]

    def reduce_far(p):
        sum_core(p, 0)
        for v in (2 * p, 2 * p + 1):
            send(rcy.at[p, opp, low(v)], rx1.at[v, 0], ssem.at[E_RX], rsem_x.at[v, 0], at_x(nxt))
            send(rcy.at[p, opp, high(v)], rx1.at[v, 1], ssem.at[E_RX], rsem_x.at[v, 1], at_x(prv))

    def far_and_rest(p):
        @pl.when(c == 0)
        def _():
            reduce_far(p)
            chunks_rest(p, False)

        @pl.when(c == 1)
        def _():
            chunks_rest(p, False)
            reduce_far(p)

    def reduce_rest(p):
        for k in range(1, X):
            sum_core(p, k)

    def reduce_x(v):
        p = v // 2
        arrived(rx1.at[v, 0], rsem_x.at[v, 0])
        rcy[p, nxt, low(v)] = rcy[p, nxt, low(v)] + rx1[v, 0]
        send(rcy.at[p, nxt, piece(v)], rx2.at[v, 0], ssem.at[E_RX2], rsem_x.at[v, 2], at_x(nxt))
        arrived(rx1.at[v, 1], rsem_x.at[v, 1])
        rcy[p, prv, high(v)] = rcy[p, prv, high(v)] + rx1[v, 1]
        send(rcy.at[p, prv, piece(v)], rx2.at[v, 1], ssem.at[E_RX2], rsem_x.at[v, 3], at_x(prv))

    def own_x():
        low_half = lax.broadcasted_iota(jnp.int32, (S // 2, LANES), 1) < LANES // 2
        for m in range(Y):
            rows = xp[m % C, nid * (Y // C) + m // C].astype(F32)
            xn[m * S:m * S + S // 2] = jnp.where(low_half, rows, 0.0).astype(BF)
            xn[m * S + S // 2:(m + 1) * S] = jnp.where(low_half, turned(rows), 0.0).astype(BF)

    def grad_one(v):
        arrived(rx2.at[v, 0], rsem_x.at[v, 2])
        arrived(rx2.at[v, 1], rsem_x.at[v, 3])
        acc = (rcy[v // 2, x, piece(v)] + rx2[v, 0] + rx2[v, 1]).astype(BF)
        part = dot(acc, xn[...])
        if v >= NV // 2:
            part = turned(part)
        per = HU // (Z * 8)
        rows = part.reshape(per, Z, 8, LANES)
        for m in range(per):
            k = (v % (NV // 2)) * per + m
            pb[k] = rows[m] if v < NV // 2 else pb[k] + rows[m]

    def w_begin():
        mark = (lax.broadcasted_iota(jnp.int32, (HB, LANES), 0) == 0) & (lax.broadcasted_iota(jnp.int32, (HB, LANES), 1) == NC)
        for k in range(Y):
            part = lax.dot_general(h1[:, k * HB:(k + 1) * HB], dy2, (((0,), (0,)), ((), ())), preferred_element_type=F32)
            if k == 0:
                part = jnp.where(mark, loss_part, part)
            per = HB // (Y * Z * 8)
            rows = part.reshape(per, Y, Z, 8, LANES)
            for m in range(per):
                q = k * per + m
                wb[q // X, q % X] = rows[m]
        send(wb.at[1 - c], wc, ssem.at[E_WC], rsem.at[E_WC], partner)

    def w_core():
        arrived(wc, rsem.at[E_WC])
        wc[...] = wc[...] + wb[c]
        for d in (2, 1, 3):
            xq = (x + d) % X
            send(wc.at[xq], wx.at[x], ssem.at[E_WX], rsem.at[E_WX], at_x(xq))
        wx[x] = wc[x]

    def w_x():
        arrived(wx.at[pl.ds(0, X - 1)], rsem.at[E_WX])
        wx[x] = added(wx, X)
        for d in (2, 1, 3):
            yq = (y + d) % Y
            send(wx.at[x, yq], wy.at[y], ssem.at[E_WY], rsem.at[E_WY], at_y(yq))
        wy[y] = wx[x, y]

    def w_y():
        arrived(wy.at[pl.ds(0, Y - 1)], rsem.at[E_WY])
        wy[y] = added(wy, Y)
        for d in far:
            zq = (z + d) % Z
            send(wy.at[y, zq], wz.at[z], ssem.at[E_WZ], rsem.at[E_WZ], at_z(zq))
        wz[z] = wy[y, z]

    def w_z():
        arrived(wz.at[pl.ds(0, Z - 1)], rsem.at[E_WZ])
        wf[...] = added(wz, Z)
        for d in far:
            send(wf, oz.at[z], ssem.at[E_OZ], rsem.at[E_OZ], at_z((z + d) % Z))
        oz[z] = wf[...]

    def o_z():
        arrived(oz.at[pl.ds(0, Z - 1)], rsem.at[E_OZ])
        for d in (2, 1, 3):
            send(oz, oy.at[y], ssem.at[E_OY], rsem.at[E_OY], at_y((y + d) % Y))
        oy[y] = oz[...]

    def o_y():
        arrived(oy.at[pl.ds(0, Y - 1)], rsem.at[E_OY])
        for d in (2, 1, 3):
            send(oy, ox.at[x], ssem.at[E_OX], rsem.at[E_OX], at_x((x + d) % X))
        ox[x] = oy[...]

    def o_x():
        arrived(ox.at[pl.ds(0, X - 1)], rsem.at[E_OX])
        send(ox, oc.at[c], ssem.at[E_OC], rsem.at[E_OC], partner)
        oc[c] = ox[...]

    arrived(mk.at[pl.ds(0, Y - 1)], rsem.at[E_M])
    arrived(dg.at[pl.ds(0, Y - 1)], rsem.at[E_DG])
    steps = [
        (g_one, 0), (gather_step, 0, 1), (g_one, 1), (gather_step, 1, 1), (g_one, 2), (g_one, 3), (w_begin,), (own_x,),
        (gather_step, 0, 2), (gather_step, 1, 2), (w_core,), (gather_step, 2, 1),
        (gather_step, 0, 3), (gather_step, 1, 3), (gather_step, 3, 1),
        (gather_step, 0, 4), (gather_step, 1, 4), (gather_step, 2, 2), (gather_step, 3, 2),
        (prepare, 0), (chunks_far, 0), (far_and_rest, 0), (gather_step, 2, 3), (gather_step, 3, 3),
        (chunks_rest, 0, True), (reduce_rest, 0), (reduce_x, 0), (reduce_x, 1), (gather_step, 2, 4), (gather_step, 3, 4), (w_x,),
        (prepare, 1), (chunks_far, 1), (far_and_rest, 1), (w_y,), (chunks_rest, 1, True), (reduce_rest, 1), (grad_one, 0), (grad_one, 1),
        (reduce_x, 2), (reduce_x, 3), (w_z,), (grad_one, 2), (o_z,), (grad_one, 3)]
    for step in steps:
        step[0](*step[1:])

    for d in (2, 1, 3):
        xq = (x + d) % X
        send(pb.at[xq], px.at[x], ssem.at[E_PX], rsem.at[E_PX], at_x(xq))
    px[x] = pb[x]
    arrived(px.at[pl.ds(0, X - 1)], rsem.at[E_PX])
    px[x] = added(px, X)
    for d in far:
        zq = (z + d) % Z
        for k in range(C):
            send(px.at[x, zq], pz.at[c * Z + z], ssem.at[E_PZ], rsem.at[E_PZ], (zq * Y + y, x * C + k))
    send(px.at[x, z], pz.at[c * Z + z], ssem.at[E_PZ], rsem.at[E_PZ], partner)
    pz[c * Z + z] = px[x, z]
    o_y()
    arrived(pz.at[pl.ds(0, C * Z - 1)], rsem.at[E_PZ])
    pf[...] = added(pz, C * Z)
    for d in far:
        send(pf, qz.at[z], ssem.at[E_QZ], rsem.at[E_QZ], at_z((z + d) % Z))
    qz[z] = pf[...]
    arrived(qz.at[pl.ds(0, Z - 1)], rsem.at[E_QZ])
    zl, zh = pl.ds(0, half), pl.ds(half, half)
    for d in (2, 1, 3):
        send(qz.at[zl], qy.at[y], ssem.at[E_QY], rsem.at[E_QY], at_y((y + d) % Y))
        send(qz.at[zh], qx.at[x], ssem.at[E_QX], rsem.at[E_QX], at_x((x + d) % X))
    qy[y] = qz[zl]
    qx[x] = qz[zh]
    o_x()
    arrived(qy.at[pl.ds(0, Y - 1)], rsem.at[E_QY])
    for d in (2, 1, 3):
        send(qy, qxy.at[x], ssem.at[E_QXY], rsem.at[E_QXY], at_x((x + d) % X))
    qxy[x] = qy[...]
    arrived(qx.at[pl.ds(0, X - 1)], rsem.at[E_QX])
    for d in (2, 1, 3):
        send(qx, qyx.at[y], ssem.at[E_QYX], rsem.at[E_QYX], at_y((y + d) % Y))
    qyx[y] = qx[...]
    arrived(oc.at[0], rsem.at[E_OC])
    for k in range(C):
        full = oc[k].reshape(H // C, LANES)
        dw2_out[k * (H // C):(k + 1) * (H // C), :] = full[:, 0:NC]
        if k == 0:
            loss_out[...] = jnp.broadcast_to(full[0:1, NC:NC + 1] / count, (8, LANES))
    arrived(qxy.at[pl.ds(0, X - 1)], rsem.at[E_QXY])
    arrived(qyx.at[pl.ds(0, Y - 1)], rsem.at[E_QYX])
    for yb in range(Y):
        part = jnp.concatenate([qxy[:, yb], qyx[yb]], axis=1).reshape(HB // 2, LANES).T
        dw1_out[:, yb * HB:yb * HB + HB // 2] = part[0:F]
        dw1_out[:, yb * HB + HB // 2:(yb + 1) * HB] = part[LANES // 2:LANES // 2 + F]

    sent(most(xp), ssem.at[E_X])
    sent(xp.at[0], ssem.at[E_XC])
    sent(af.at[pl.ds(0, Y - 1), :, 0], ssem.at[E_A])
    sent(af.at[pl.ds(0, Y - 1), :, pl.ds(0, 2)], ssem.at[E_B])
    sent(af.at[pl.ds(0, Y - 1), :, 0], ssem.at[E_F])
    sent(sb, ssem.at[E_RING])
    sent(cr.at[pl.ds(0, Z - 1)], ssem.at[E_CNT])
    sent(most(yp), ssem.at[E_Y2])
    sent(yp.at[0], ssem.at[E_Y2C])
    sent(zr.at[pl.ds(0, Z - 1)], ssem.at[E_Z2])
    sent(gr.at[pl.ds(0, Z - 1)], ssem.at[E_G2])
    for yb in range(Y):
        sent(rc.at[yb], ssem.at[E_DC + yb])
    sent(rx.at[pl.ds(0, X - 1)], ssem.at[E_DX])
    sent(ry.at[pl.ds(0, Y - 1)], ssem.at[E_DY])
    sent(ry2.at[pl.ds(0, Y - 1)], ssem.at[E_DY2])
    sent(rx2d.at[pl.ds(0, X - 1)], ssem.at[E_DX2])
    sent(dg.at[pl.ds(0, Y - 1)], ssem.at[E_DG])
    sent(mk.at[pl.ds(0, Y - 1)], ssem.at[E_M])
    sent(gz.at[:, pl.ds(0, Z - 1)], ssem.at[E_AG])
    sent(rcy, ssem.at[E_RC])
    sent(rx1, ssem.at[E_RX])
    sent(rx2, ssem.at[E_RX2])
    sent(wc, ssem.at[E_WC])
    sent(wx.at[pl.ds(0, X - 1)], ssem.at[E_WX])
    sent(wy.at[pl.ds(0, Y - 1)], ssem.at[E_WY])
    sent(wz.at[pl.ds(0, Z - 1)], ssem.at[E_WZ])
    sent(oz.at[pl.ds(0, Z - 1)], ssem.at[E_OZ])
    sent(oy.at[pl.ds(0, Y - 1)], ssem.at[E_OY])
    sent(ox.at[pl.ds(0, X - 1)], ssem.at[E_OX])
    sent(oc.at[0], ssem.at[E_OC])
    sent(px.at[pl.ds(0, X - 1)], ssem.at[E_PX])
    sent(pz.at[pl.ds(0, C * Z - 1)], ssem.at[E_PZ])
    sent(qz.at[pl.ds(0, Z - 1)], ssem.at[E_QZ])
    sent(qy.at[pl.ds(0, Y - 1)], ssem.at[E_QY])
    sent(qx.at[pl.ds(0, X - 1)], ssem.at[E_QX])
    sent(qxy.at[pl.ds(0, X - 1)], ssem.at[E_QXY])
    sent(qyx.at[pl.ds(0, Y - 1)], ssem.at[E_QYX])


def solution(mesh):
    Y, X, C = Y_DIM, X_DIM, CORES
    Z = mesh.shape["rep"] // Y
    row_spec = P(("rep", "nodes"))

    def device_step(adj_blk, feat_blk, w_one, w_two, label_blk, mask_blk):
        R, S, CB = adj_blk.shape
        F, H = w_one.shape
        NC = w_two.shape[1]
        I = X * C
        NQ = Y * X
        HR = H // (2 * NSUB)
        HB = H // Y
        HU = HB // NV
        NCH = Y * S
        assert R == Z * Y and CB == S * I and X == Y and Z == 8 and F + 2 <= LANES // 2 and NC < LANES
        vm = pltpu.VMEM
        dma = pltpu.SemaphoreType.DMA
        scratch = [
            vm((Y, Z, Y, S, CB), BF),
            vm((F, S), BF),
            vm((1, S), jnp.int32),
            vm((1, S), jnp.int32),
            vm((LANES, S), F32),
            vm((S, LANES), F32),
            vm((F, H), F32),
            vm((H, NC), F32),
            vm((2, LANES, H), BF),
            vm((H, LANES), BF),
            vm((LANES, H), BF),
            vm((S // 2, LANES), BF),
            vm((C, NQ, S // 2, LANES), BF),
            vm((NCH, LANES), BF),
            vm((NQ, C, S, H), BF),
            vm((8, LANES), F32),
            vm((Z, 8, LANES), F32),
            vm((2 * NSUB, Z - 1, S, HR), F32),
            vm((2 * NSUB, Z - 1, S, HR), F32),
            vm((S, H), F32),
            vm((S, H), BF),
            vm((S, LANES), BF),
            vm((C, NQ, S, LANES), BF),
            vm((Z, S, LANES), F32),
            vm((Z, S, LANES), F32),
            vm((S, LANES), BF),
            vm((Z, S, LANES), BF),
            vm((Y, X, C, S, LANES), F32),
            vm((Y, X, S, LANES), F32),
            vm((X, Y, S // 2, LANES), F32),
            vm((Y, X, S // 2, LANES), F32),
            vm((Y, S // 2, LANES), F32),
            vm((X, S // 2, LANES), F32),
            vm((S, LANES), BF),
            vm((Y, S, LANES), BF),
            vm((Y, S, HB), BF),
            vm((Y, S, HB), BF),
            vm((NV, Z, Y, S, HU), BF),
            vm((NV // 2, 2 * HU, Z * Y * S), BF),
            vm((NV // 2, X, C, 2 * HU, NCH), F32),
            vm((NV // 2, X, 2 * HU, NCH), F32),
            vm((NV, 2, HU // 2, NCH), F32),
            vm((NV, 2, HU, NCH), F32),
            vm((C, X, Y, Z, 8, LANES), F32),
            vm((X, Y, Z, 8, LANES), F32),
            vm((X, Y, Z, 8, LANES), F32),
            vm((Y, Z, 8, LANES), F32),
            vm((Z, 8, LANES), F32),
            vm((8, LANES), F32),
            vm((Z, 8, LANES), F32),
            vm((Y, Z, 8, LANES), F32),
            vm((X, Y, Z, 8, LANES), F32),
            vm((C, X, Y, Z, 8, LANES), F32),
            vm((X, Z, 8, LANES), F32),
            vm((X, Z, 8, LANES), F32),
            vm((C * Z, 8, LANES), F32),
            vm((8, LANES), F32),
            vm((Z, 8, LANES), F32),
            vm((Y, Z // 2, 8, LANES), F32),
            vm((X, Z // 2, 8, LANES), F32),
            vm((X, Y, Z // 2, 8, LANES), F32),
            vm((Y, X, Z // 2, 8, LANES), F32),
            dma((NSEM,)),
            dma((NSEM,)),
            dma((Y - 1, Z)),
            dma((2, Y - 1)),
            dma((2, Y - 1)),
            dma((2 * NSUB, Z - 1)),
            dma((NV, 2, Z // 2 + 1)),
            dma((NV // 2, X)),
            dma((NV, 4)),
        ]
        vspec = pl.BlockSpec(memory_space=pltpu.VMEM)
        aspec = pl.BlockSpec(memory_space=pltpu.HBM)
        operands = (adj_blk.reshape(Z, Y, S, CB), feat_blk.T, label_blk[None, :], mask_blk[None, :], w_one, w_two)
        dw_one, dw_two, loss = pl.pallas_call(
            functools.partial(_step, (Z, Y, X, C, S, CB, H, F, NC)),
            out_shape=(jax.ShapeDtypeStruct((F, H), F32), jax.ShapeDtypeStruct((H, NC), F32), jax.ShapeDtypeStruct((8, LANES), F32)),
            in_specs=[aspec] * 6,
            out_specs=(vspec, vspec, vspec),
            scratch_shapes=scratch,
            compiler_params=pltpu.CompilerParams(collective_id=0, has_side_effects=True, vmem_limit_bytes=52 * 1024 * 1024),
            name="gcn_step",
        )(*[pltpu.with_memory_space_constraint(v, pltpu.HBM) for v in operands])
        return loss[0, 0], dw_one, dw_two

    return jax.shard_map(device_step, mesh=mesh, in_specs=(P(None, "nodes", "rep"), row_spec, P(), P(), row_spec, row_spec), out_specs=(P(), P(), P()), check_vma=False)
```

```python
import functools

import jax
import jax.numpy as jnp
from jax import lax
from jax.experimental import pallas as pl
from jax.experimental.pallas import tpu as pltpu
from jax.sharding import PartitionSpec as P

Y_DIM = 4
X_DIM = 4
CORES = 2
LANES = 128
NSUB = 4
NV = 4
NSEM = 46
BF = jnp.bfloat16
F32 = jnp.float32


def _step(dims, a_hbm, feat_hbm, lab_hbm, msk_hbm, w_one, w_two, dw1_out, dw2_out, loss_out,
          af, feat, lab, msk, mt, mtt, w1f, w2f, w1, w2, w2t, xs, xp, xn, y1, cs, cr, sb, rb, z1, h1, y2, yp, zp, zr, g2, gr, dp, rc, rx, ry, ry2, rx2d,
          d2, dg, ms, mk, gz, gt, dy, rcy, rx1, rx2, wb, wc, wx, wy, wz, wf, oz, oy, ox, oc, pb, px, pz, pf, qz, qy, qx, qxy, qyx,
          ssem, rsem, rsem_a, rsem_b, rsem_f, rsem_ring, rsem_ag, rsem_c, rsem_x):
    Z, Y, X, C, S, CB, H, F, NC = dims
    I = X * C
    NQ = Y * X
    HR = H // (2 * NSUB)
    HB = H // Y
    HU = HB // NV
    NCH = Y * S
    half = Z // 2
    rid = lax.axis_index("rep")
    nid = lax.axis_index("nodes")
    z, y, x, c = rid // Y, rid % Y, nid // C, nid % C
    chip = y * X + x
    partner = (rid, x * C + 1 - c)

    far = sorted(range(1, Z), key=lambda d: -min(d, Z - d))

    def at_z(zz):
        return (zz * Y + y, nid)

    def at_y(yy):
        return (z * Y + yy, nid)

    def at_x(xx):
        return (rid, xx * C + c)

    def at_chip(q):
        return (z * Y + q // X, (q % X) * C + c)

    def send(src, dst, ss, rs, dev):
        pltpu.make_async_remote_copy(src_ref=src, dst_ref=dst, send_sem=ss, recv_sem=rs, device_id=dev,
                                     device_id_type=pl.DeviceIdType.MESH).start()

    def arrived(ref, rs):
        pltpu.make_async_remote_copy(src_ref=ref, dst_ref=ref, send_sem=ssem.at[0], recv_sem=rs, device_id=partner,
                                     device_id_type=pl.DeviceIdType.MESH).wait_recv()

    def sent(ref, ss):
        pltpu.make_async_remote_copy(src_ref=ref, dst_ref=ref, send_sem=ss, recv_sem=rsem.at[0], device_id=partner,
                                     device_id_type=pl.DeviceIdType.MESH).wait_send()

    def dot(a, b):
        return jnp.dot(a, b, preferred_element_type=F32)

    def most(ref):
        return ref.at[0, pl.ds(0, NQ - 1)]

    def plane_rows(ref, yb):
        return jnp.stack([ref[k, yb * X:(yb + 1) * X] for k in range(C)], axis=1).reshape(CB, LANES)

    def turned(v):
        return jnp.concatenate([v[:, LANES // 2:], v[:, 0:LANES // 2]], axis=1)

    def added(ref, n):
        acc = ref[0]
        for k in range(1, n):
            acc = acc + ref[k]
        return acc

    (E_X, E_XC, E_A, E_B, E_F, E_RING, E_CNT, E_Y2, E_Y2C, E_Z2, E_G2, E_DC, E_DC1, E_DC2, E_DC3, E_DX, E_DY, E_AG, E_RC, E_RX, E_RX2,
     E_WC, E_WX, E_WY, E_WZ, E_OZ, E_OY, E_OX, E_OC, E_PX, E_PZ, E_QZ, E_QY, E_QX, E_LA, E_L1, E_L2,
     E_M, E_DY2, E_DX2, E_DG, E_QXY, E_QYX, E_IN, E_IN1, E_IN2) = range(NSEM)

    load_a = pltpu.make_async_copy(a_hbm, af.at[y], ssem.at[E_LA])
    load_1 = pltpu.make_async_copy(w_one, w1f, ssem.at[E_L1])
    load_2 = pltpu.make_async_copy(w_two, w2f, ssem.at[E_L2])
    loads = [pltpu.make_async_copy(src, dst, ssem.at[E_IN + k]) for k, (src, dst) in
             enumerate(((feat_hbm, feat), (lab_hbm, lab), (msk_hbm, msk)))]
    for load in loads:
        load.start()
    load_a.start()
    load_1.start()
    load_2.start()

    bar = pltpu.get_barrier_semaphore()
    for d in far:
        pl.semaphore_signal(bar, inc=1, device_id=at_z((z + d) % Z), device_id_type=pl.DeviceIdType.MESH)

    def greet_plane(d, u):
        pl.semaphore_signal(bar, inc=1, device_id=at_chip(lax.rem(chip + d, NQ)), device_id_type=pl.DeviceIdType.MESH)
        return u

    lax.fori_loop(1, NQ, greet_plane, 0)
    pl.semaphore_signal(bar, inc=1, device_id=partner, device_id_type=pl.DeviceIdType.MESH)

    for load in loads:
        load.wait()
    mt[...] = jnp.zeros_like(mt)
    mt[0:F] = feat[...].astype(F32)
    mt[F:F + 1] = msk[...].astype(F32)
    mt[F + 1:F + 2] = lab[...].astype(F32)
    mtt[...] = mt[...].T
    xs[...] = (mtt[0:S // 2] + turned(mtt[S // 2:S])).astype(BF)
    pl.semaphore_wait(bar, NQ + Z - 1)

    def send_x(d, u):
        q = lax.rem(chip + d, NQ)
        send(xs, xp.at[c, chip], ssem.at[E_X], rsem.at[E_X], at_chip(q))
        return u

    lax.fori_loop(1, NQ, send_x, 0)
    xp[c, chip] = xs[...]
    load_a.wait()

    order = []
    for k in range(1, half + 1):
        order.append(-k)
        if k < half:
            order.append(k)
    order.append(0)
    for k in order:
        zc = (z + k + Z) % Z
        for d in (2, 1, 3):
            yq = (y + d) % Y
            send(af.at[y, zc, yq], af.at[y, zc, yq], ssem.at[E_A], rsem_a.at[d - 1, zc], at_y(yq))
    def spread_a(k):
        for d in (1, 3):
            yq = (y + d) % Y
            ya = (yq + k) % Y
            send(af.at[y, :, ya], af.at[y, :, ya], ssem.at[E_B], rsem_b.at[d // 2, k - 1], at_y(yq))

    def forward_a():
        for k in range(1, Y):
            for d in (1, 3):
                arrived(af.at[0, :, 0], rsem_b.at[d // 2, k - 1])
        for k in range(1, Y):
            for d in (1, 3):
                ys, yq = (y - d + Y) % Y, (y + d) % Y
                lo = 0 if d == 1 else half
                ya = (yq + k) % Y
                send(af.at[ys, pl.ds(lo, half), ya], af.at[ys, pl.ds(lo, half), ya], ssem.at[E_F], rsem_f.at[d // 2, k - 1], at_y(yq))

    spread_a(1)
    spread_a(2)

    load_1.wait()
    w1[...] = jnp.zeros_like(w1)
    w1[0, 0:F] = w1f[...].astype(BF)
    w1[1, LANES // 2:LANES // 2 + F] = w1f[...].astype(BF)
    load_2.wait()
    w2[...] = jnp.zeros_like(w2)
    for k in range(Y):
        rows = slice(k * HB, (k + 1) * HB)
        w2[rows, 0:NC] = w2f[rows].astype(BF)
        w2t[:, rows] = w2[rows].T

    arrived(most(xp), rsem.at[E_X])
    send(xp.at[c], xp.at[c], ssem.at[E_XC], rsem.at[E_XC], partner)

    def columns(j):
        return pl.ds(pl.multiple_of(j * HR, HR), HR)

    def y1_half(k, j):
        rows = xp[k].reshape(NQ * S // 2, LANES)
        for m in range(2):
            y1[:, k, m * (S // 2):(m + 1) * (S // 2), columns(j)] = dot(rows, w1[m, :, columns(j)]).astype(BF).reshape(NQ, S // 2, HR)

    def y1_own(j, u):
        y1_half(c, j)
        return u

    def y1_block(yb, j):
        return y1[yb * X:(yb + 1) * X, :, :, columns(j)].reshape(CB, HR)

    lax.fori_loop(0, 2 * NSUB, y1_own, 0)
    arrived(xp.at[0], rsem.at[E_XC])

    def wait_a(zc):
        for d in range(1, Y):
            arrived(af.at[0, 0, 0], rsem_a.at[d - 1, zc])

    def products(s, j):
        up = j % 2 == 0
        dest = lax.rem(jnp.where(up, z - 1 - s, z + 1 + s) + 2 * Z, Z)
        fresh = ((j == 0) & ((s < half) | (s == Z - 1))) | ((j == 1) & (s < half - 1))

        @pl.when(fresh)
        def _():
            wait_a(dest)

        acc = dot(af[0, dest, y], y1_block(0, j))
        for yb in range(1, Y):
            acc = acc + dot(af[yb, dest, y], y1_block(yb, j))
        return acc

    def pass_on(s, j):
        nb = lax.rem(jnp.where(j % 2 == 0, z + 1, z - 1) + Z, Z)
        send(sb.at[j, s], rb.at[j, s], ssem.at[E_RING], rsem_ring.at[j, s], at_z(nb))

    def ring_first(j, u):
        y1_half(1 - c, j)
        sb[j, 0] = products(0, j)
        pass_on(0, j)
        return u

    def ring_next(t, u):
        s, j = t // (2 * NSUB) + 1, t % (2 * NSUB)
        acc = products(s, j)
        arrived(rb.at[0, 0], rsem_ring.at[j, s - 1])
        sb[j, s] = acc + rb[j, s - 1]
        pass_on(s, j)
        return u

    def ring_last(j, u):
        acc = products(Z - 1, j)
        arrived(rb.at[0, 0], rsem_ring.at[j, Z - 2])
        z1[:, columns(j)] = acc + rb[j, Z - 2]
        return u

    lax.fori_loop(0, 2 * NSUB, ring_first, 0)
    lax.fori_loop(0, (Z - 2) * 2 * NSUB, ring_next, 0)
    lax.fori_loop(0, 2 * NSUB, ring_last, 0)

    h1[...] = jnp.maximum(z1[...], 0.0).astype(BF)
    y2[...] = dot(h1[...], w2[...]).astype(BF)

    def send_y2(d, u):
        q = lax.rem(chip + d, NQ)
        send(y2, yp.at[c, chip], ssem.at[E_Y2], rsem.at[E_Y2], at_chip(q))
        return u

    lax.fori_loop(1, NQ, send_y2, 0)
    yp[c, chip] = y2[...]
    lane = lax.broadcasted_iota(jnp.int32, (S, LANES), 1)
    counted = jnp.sum(xp[...].astype(F32).reshape(Y * CB // 2, LANES), axis=0, keepdims=True)
    counted = jnp.sum(jnp.where(lane[0:1] % (LANES // 2) == F, counted, 0.0), axis=1, keepdims=True)
    cs[...] = jnp.broadcast_to(counted, (8, LANES))
    cr[z] = cs[...]
    for d in far:
        send(cs, cr.at[z], ssem.at[E_CNT], rsem.at[E_CNT], at_z((z + d) % Z))
    arrived(most(yp), rsem.at[E_Y2])
    send(yp.at[c], yp.at[c], ssem.at[E_Y2C], rsem.at[E_Y2C], partner)
    arrived(yp.at[0], rsem.at[E_Y2C])
    def z2_part(zq):
        part = dot(af[0, zq, y], plane_rows(yp, 0))
        for yb in range(1, Y):
            part = part + dot(af[yb, zq, y], plane_rows(yp, yb))
        return part

    for d in far:
        zq = (z + d) % Z
        zp[zq] = z2_part(zq)
        send(zp.at[zq], zr.at[z], ssem.at[E_Z2], rsem.at[E_Z2], at_z(zq))
    zr[z] = z2_part(z)
    for yb in range(Y):
        ms[yb] = jnp.where(z1[:, yb * HB:(yb + 1) * HB] > 0.0, 1.0, 0.0).astype(BF)
    for d in (2, 1, 3):
        yq = (y + d) % Y
        send(ms.at[yq], mk.at[y], ssem.at[E_M], rsem.at[E_M], at_y(yq))
    mk[y] = ms[y]
    spread_a(3)
    arrived(zr.at[pl.ds(0, Z - 1)], rsem.at[E_Z2])
    z2 = added(zr, Z)

    arrived(cr.at[pl.ds(0, Z - 1)], rsem.at[E_CNT])
    count = added(cr, Z)[0:1, 0:1]
    own = mtt[...]
    weights = jnp.sum(jnp.where(lane == F, own, 0.0), axis=1, keepdims=True)
    labels = jnp.sum(jnp.where(lane == F + 1, own, 0.0), axis=1, keepdims=True)
    real = lane < NC
    top = jnp.max(jnp.where(real, z2, -jnp.inf), axis=1, keepdims=True)
    shifted = jnp.where(real, z2 - top, 0.0)
    log_probs = shifted - jnp.log(jnp.sum(jnp.where(real, jnp.exp(shifted), 0.0), axis=1, keepdims=True))
    hot = labels == lane.astype(F32)
    picked = jnp.sum(jnp.where(hot, log_probs, 0.0), axis=1, keepdims=True)
    loss_part = -jnp.sum(weights * picked, axis=0, keepdims=True)
    diff = jnp.where(real, jnp.exp(log_probs), 0.0) - hot.astype(F32)
    g2[...] = (diff * (weights / count)).astype(BF)
    for d in far:
        send(g2, gr.at[z], ssem.at[E_G2], rsem.at[E_G2], at_z((z + d) % Z))
    gr[z] = g2[...]
    arrived(gr.at[pl.ds(0, Z - 1)], rsem.at[E_G2])

    g2t = gr[...].reshape(Z * S, LANES).T
    for yb in range(Y):
        part = dot(g2t, af[yb, :, y].reshape(Z * S, CB))
        dp[yb] = part.T.reshape(X, C, S, LANES)
        send(dp.at[yb, :, 1 - c], rc.at[yb], ssem.at[E_DC + yb], rsem.at[E_DC + yb], partner)
    for yb in range(Y):
        arrived(rc.at[yb], rsem.at[E_DC + yb])
        rc[yb] = rc[yb] + dp[yb, :, c]
    sh = S // 2
    for d in (2, 1, 3):
        xq, yq = (x + d) % X, (y + d) % Y
        send(rc.at[:, xq, pl.ds(0, sh)], rx.at[x], ssem.at[E_DX], rsem.at[E_DX], at_x(xq))
        send(rc.at[yq, :, pl.ds(sh, sh)], ry.at[y], ssem.at[E_DY], rsem.at[E_DY], at_y(yq))
    rx[x] = rc[:, x, 0:sh]
    ry[y] = rc[y, :, sh:S]
    arrived(rx.at[pl.ds(0, X - 1)], rsem.at[E_DX])
    rx[x] = added(rx, X)
    for d in (2, 1, 3):
        yq = (y + d) % Y
        send(rx.at[x, yq], ry2.at[y], ssem.at[E_DY2], rsem.at[E_DY2], at_y(yq))
    ry2[y] = rx[x, y]
    arrived(ry.at[pl.ds(0, Y - 1)], rsem.at[E_DY])
    ry[y] = added(ry, Y)
    for d in (2, 1, 3):
        xq = (x + d) % X
        send(ry.at[y, xq], rx2d.at[x], ssem.at[E_DX2], rsem.at[E_DX2], at_x(xq))
    rx2d[x] = ry[y, x]
    arrived(ry2.at[pl.ds(0, Y - 1)], rsem.at[E_DY2])
    arrived(rx2d.at[pl.ds(0, X - 1)], rsem.at[E_DX2])
    d2[0:sh] = added(ry2, Y).astype(BF)
    d2[sh:S] = added(rx2d, X).astype(BF)
    for d in (2, 1, 3):
        send(d2, dg.at[y], ssem.at[E_DG], rsem.at[E_DG], at_y((y + d) % Y))
    dg[y] = d2[...]
    forward_a()
    dy2 = d2[...]

    def g_one(v):
        col = pl.multiple_of(y * HB + v * HU, HU)
        dh = dot(dg[...].reshape(Y * S, LANES), w2t[:, pl.ds(col, HU)])
        keep = mk[:, :, v * HU:(v + 1) * HU].reshape(Y * S, HU).astype(F32)
        gz[v, z] = jnp.where(keep > 0.0, dh, 0.0).astype(BF).reshape(Y, S, HU)

    def gather_step(v, t):
        for d in range(2):
            sgn = 1 if d == 0 else -1
            blk = (z - sgn * (t - 1) + Z) % Z
            if t > 1:
                arrived(gz.at[v, 0], rsem_ag.at[v, d, t - 1])
            ref = gz.at[v, blk] if t < half else gz.at[v, blk, pl.ds(d * (Y // 2), Y // 2)]
            send(ref, ref, ssem.at[E_AG], rsem_ag.at[v, d, t], at_z((z + sgn + Z) % Z))

    def piece(v):
        return pl.ds(v % 2 * HU, HU)

    def prepare(p):
        for v in (2 * p, 2 * p + 1):
            for d in range(2):
                arrived(gz.at[v, 0, pl.ds(0, Y // 2)], rsem_ag.at[v, d, half])
            for k in range(Z):
                gt[p, piece(v), k * Y * S:(k + 1) * Y * S] = gz[v, k].reshape(Y * S, HU).T

    nxt, prv, opp = (x + 1) % X, (x + X - 1) % X, (x + 2) % X
    hh = HU // 2

    def low(v):
        return pl.ds(v % 2 * HU, hh)

    def high(v):
        return pl.ds(v % 2 * HU + hh, hh)

    def chunk(p, xb, core):
        off = pl.multiple_of(core * NCH, NCH)
        dy[p, xb, core] = dot(gt[p], af[xb, :, :, :, pl.ds(off, NCH)].reshape(Z * Y * S, NCH))

    def send_core(p, k):
        xb = (x + 2 + k) % X
        send(dy.at[p, xb, 1 - c], rcy.at[p, xb], ssem.at[E_RC], rsem_c.at[p, k], partner)

    def chunks_far(p):
        if p == 0:
            for d in (1, 3):
                for k in range(1, Y):
                    arrived(af.at[0, pl.ds(0, half), 0], rsem_f.at[d // 2, k - 1])
        chunk(p, opp, 1 - c)
        send_core(p, 0)
        chunk(p, opp, c)

    def chunks_rest(p, own):
        def body(k, u):
            chunk(p, lax.rem(x + 2 + k, X), c if own else 1 - c)
            return u

        lax.fori_loop(1, X, body, 0)
        if not own:
            for k in range(1, X):
                send_core(p, k)

    def sum_core(p, k):
        xb = (x + 2 + k) % X
        arrived(rcy.at[p, xb], rsem_c.at[p, k])
        rcy[p, xb] = rcy[p, xb] + dy[p, xb, c]

    def reduce_far(p):
        sum_core(p, 0)
        for v in (2 * p, 2 * p + 1):
            send(rcy.at[p, opp, low(v)], rx1.at[v, 0], ssem.at[E_RX], rsem_x.at[v, 0], at_x(nxt))
            send(rcy.at[p, opp, high(v)], rx1.at[v, 1], ssem.at[E_RX], rsem_x.at[v, 1], at_x(prv))

    def far_and_rest(p):
        @pl.when(c == 0)
        def _():
            reduce_far(p)
            if p == 0:
                gather_step(2, 3)
                gather_step(3, 3)
            chunks_rest(p, False)

        @pl.when(c == 1)
        def _():
            if p == 0:
                gather_step(2, 3)
                gather_step(3, 3)
            chunks_rest(p, False)
            reduce_far(p)

    def reduce_rest(p):
        for k in range(1, X):
            sum_core(p, k)

    def reduce_x(v):
        p = v // 2
        arrived(rx1.at[v, 0], rsem_x.at[v, 0])
        rcy[p, nxt, low(v)] = rcy[p, nxt, low(v)] + rx1[v, 0]
        send(rcy.at[p, nxt, piece(v)], rx2.at[v, 0], ssem.at[E_RX2], rsem_x.at[v, 2], at_x(nxt))
        arrived(rx1.at[v, 1], rsem_x.at[v, 1])
        rcy[p, prv, high(v)] = rcy[p, prv, high(v)] + rx1[v, 1]
        send(rcy.at[p, prv, piece(v)], rx2.at[v, 1], ssem.at[E_RX2], rsem_x.at[v, 3], at_x(prv))

    def own_x():
        low_half = lax.broadcasted_iota(jnp.int32, (S // 2, LANES), 1) < LANES // 2
        for m in range(Y):
            rows = xp[m % C, nid * (Y // C) + m // C].astype(F32)
            xn[m * S:m * S + S // 2] = jnp.where(low_half, rows, 0.0).astype(BF)
            xn[m * S + S // 2:(m + 1) * S] = jnp.where(low_half, turned(rows), 0.0).astype(BF)

    def grad_one(v):
        arrived(rx2.at[v, 0], rsem_x.at[v, 2])
        arrived(rx2.at[v, 1], rsem_x.at[v, 3])
        acc = (rcy[v // 2, x, piece(v)] + rx2[v, 0] + rx2[v, 1]).astype(BF)
        part = dot(acc, xn[...])
        if v >= NV // 2:
            part = turned(part)
        per = HU // (Z * 8)
        rows = part.reshape(per, Z, 8, LANES)
        for m in range(per):
            k = (v % (NV // 2)) * per + m
            pb[k] = rows[m] if v < NV // 2 else pb[k] + rows[m]

    def w_begin():
        mark = (lax.broadcasted_iota(jnp.int32, (HB, LANES), 0) == 0) & (lax.broadcasted_iota(jnp.int32, (HB, LANES), 1) == NC)
        for k in range(Y):
            part = lax.dot_general(h1[:, k * HB:(k + 1) * HB], dy2, (((0,), (0,)), ((), ())), preferred_element_type=F32)
            if k == 0:
                part = jnp.where(mark, loss_part, part)
            per = HB // (Y * Z * 8)
            rows = part.reshape(per, Y, Z, 8, LANES)
            for m in range(per):
                q = k * per + m
                wb[q // X, q % X] = rows[m]
        send(wb.at[1 - c], wc, ssem.at[E_WC], rsem.at[E_WC], partner)

    def w_core():
        arrived(wc, rsem.at[E_WC])
        wc[...] = wc[...] + wb[c]
        for d in (2, 1, 3):
            xq = (x + d) % X
            send(wc.at[xq], wx.at[x], ssem.at[E_WX], rsem.at[E_WX], at_x(xq))
        wx[x] = wc[x]

    def w_x():
        arrived(wx.at[pl.ds(0, X - 1)], rsem.at[E_WX])
        wx[x] = added(wx, X)
        for d in (2, 1, 3):
            yq = (y + d) % Y
            send(wx.at[x, yq], wy.at[y], ssem.at[E_WY], rsem.at[E_WY], at_y(yq))
        wy[y] = wx[x, y]

    def w_y():
        arrived(wy.at[pl.ds(0, Y - 1)], rsem.at[E_WY])
        wy[y] = added(wy, Y)
        for d in far:
            zq = (z + d) % Z
            send(wy.at[y, zq], wz.at[z], ssem.at[E_WZ], rsem.at[E_WZ], at_z(zq))
        wz[z] = wy[y, z]

    def w_z():
        arrived(wz.at[pl.ds(0, Z - 1)], rsem.at[E_WZ])
        wf[...] = added(wz, Z)
        for d in far:
            send(wf, oz.at[z], ssem.at[E_OZ], rsem.at[E_OZ], at_z((z + d) % Z))
        oz[z] = wf[...]

    def o_z():
        arrived(oz.at[pl.ds(0, Z - 1)], rsem.at[E_OZ])
        for d in (2, 1, 3):
            send(oz, oy.at[y], ssem.at[E_OY], rsem.at[E_OY], at_y((y + d) % Y))
        oy[y] = oz[...]

    def o_y():
        arrived(oy.at[pl.ds(0, Y - 1)], rsem.at[E_OY])
        for d in (2, 1, 3):
            send(oy, ox.at[x], ssem.at[E_OX], rsem.at[E_OX], at_x((x + d) % X))
        ox[x] = oy[...]

    def o_x():
        arrived(ox.at[pl.ds(0, X - 1)], rsem.at[E_OX])
        send(ox, oc.at[c], ssem.at[E_OC], rsem.at[E_OC], partner)
        oc[c] = ox[...]

    arrived(mk.at[pl.ds(0, Y - 1)], rsem.at[E_M])
    arrived(dg.at[pl.ds(0, Y - 1)], rsem.at[E_DG])
    steps = [
        (g_one, 0), (gather_step, 0, 1), (g_one, 1), (gather_step, 1, 1), (g_one, 2), (g_one, 3), (w_begin,), (own_x,),
        (gather_step, 0, 2), (gather_step, 1, 2), (w_core,), (gather_step, 2, 1),
        (gather_step, 0, 3), (gather_step, 1, 3), (gather_step, 3, 1),
        (gather_step, 0, 4), (gather_step, 1, 4), (gather_step, 2, 2), (gather_step, 3, 2),
        (prepare, 0), (chunks_far, 0), (far_and_rest, 0),
        (chunks_rest, 0, True), (gather_step, 2, 4), (reduce_rest, 0), (reduce_x, 0), (gather_step, 3, 4), (reduce_x, 1), (w_x,),
        (prepare, 1), (chunks_far, 1), (far_and_rest, 1), (w_y,), (chunks_rest, 1, True), (reduce_rest, 1), (grad_one, 0), (grad_one, 1),
        (reduce_x, 2), (reduce_x, 3), (w_z,), (grad_one, 2), (o_z,), (grad_one, 3)]
    for step in steps:
        step[0](*step[1:])

    for d in (2, 1, 3):
        xq = (x + d) % X
        send(pb.at[xq], px.at[x], ssem.at[E_PX], rsem.at[E_PX], at_x(xq))
    px[x] = pb[x]
    arrived(px.at[pl.ds(0, X - 1)], rsem.at[E_PX])
    px[x] = added(px, X)
    for d in far:
        zq = (z + d) % Z
        for k in range(C):
            send(px.at[x, zq], pz.at[c * Z + z], ssem.at[E_PZ], rsem.at[E_PZ], (zq * Y + y, x * C + k))
    send(px.at[x, z], pz.at[c * Z + z], ssem.at[E_PZ], rsem.at[E_PZ], partner)
    pz[c * Z + z] = px[x, z]
    o_y()
    arrived(pz.at[pl.ds(0, C * Z - 1)], rsem.at[E_PZ])
    pf[...] = added(pz, C * Z)
    for d in far:
        send(pf, qz.at[z], ssem.at[E_QZ], rsem.at[E_QZ], at_z((z + d) % Z))
    qz[z] = pf[...]
    arrived(qz.at[pl.ds(0, Z - 1)], rsem.at[E_QZ])
    zl, zh = pl.ds(0, half), pl.ds(half, half)
    for d in (2, 1, 3):
        send(qz.at[zl], qy.at[y], ssem.at[E_QY], rsem.at[E_QY], at_y((y + d) % Y))
        send(qz.at[zh], qx.at[x], ssem.at[E_QX], rsem.at[E_QX], at_x((x + d) % X))
    qy[y] = qz[zl]
    qx[x] = qz[zh]
    o_x()
    arrived(qy.at[pl.ds(0, Y - 1)], rsem.at[E_QY])
    for d in (2, 1, 3):
        send(qy, qxy.at[x], ssem.at[E_QXY], rsem.at[E_QXY], at_x((x + d) % X))
    qxy[x] = qy[...]
    arrived(qx.at[pl.ds(0, X - 1)], rsem.at[E_QX])
    for d in (2, 1, 3):
        send(qx, qyx.at[y], ssem.at[E_QYX], rsem.at[E_QYX], at_y((y + d) % Y))
    qyx[y] = qx[...]
    arrived(oc.at[0], rsem.at[E_OC])
    for k in range(C):
        full = oc[k].reshape(H // C, LANES)
        dw2_out[k * (H // C):(k + 1) * (H // C), :] = full[:, 0:NC]
        if k == 0:
            loss_out[...] = jnp.broadcast_to(full[0:1, NC:NC + 1] / count, (8, LANES))
    arrived(qxy.at[pl.ds(0, X - 1)], rsem.at[E_QXY])
    arrived(qyx.at[pl.ds(0, Y - 1)], rsem.at[E_QYX])
    for yb in range(Y):
        part = jnp.concatenate([qxy[:, yb], qyx[yb]], axis=1).reshape(HB // 2, LANES).T
        dw1_out[:, yb * HB:yb * HB + HB // 2] = part[0:F]
        dw1_out[:, yb * HB + HB // 2:(yb + 1) * HB] = part[LANES // 2:LANES // 2 + F]

    sent(most(xp), ssem.at[E_X])
    sent(xp.at[0], ssem.at[E_XC])
    sent(af.at[pl.ds(0, Y - 1), :, 0], ssem.at[E_A])
    sent(af.at[pl.ds(0, Y - 1), :, pl.ds(0, 2)], ssem.at[E_B])
    sent(af.at[pl.ds(0, Y - 1), :, 0], ssem.at[E_F])
    sent(sb, ssem.at[E_RING])
    sent(cr.at[pl.ds(0, Z - 1)], ssem.at[E_CNT])
    sent(most(yp), ssem.at[E_Y2])
    sent(yp.at[0], ssem.at[E_Y2C])
    sent(zr.at[pl.ds(0, Z - 1)], ssem.at[E_Z2])
    sent(gr.at[pl.ds(0, Z - 1)], ssem.at[E_G2])
    for yb in range(Y):
        sent(rc.at[yb], ssem.at[E_DC + yb])
    sent(rx.at[pl.ds(0, X - 1)], ssem.at[E_DX])
    sent(ry.at[pl.ds(0, Y - 1)], ssem.at[E_DY])
    sent(ry2.at[pl.ds(0, Y - 1)], ssem.at[E_DY2])
    sent(rx2d.at[pl.ds(0, X - 1)], ssem.at[E_DX2])
    sent(dg.at[pl.ds(0, Y - 1)], ssem.at[E_DG])
    sent(mk.at[pl.ds(0, Y - 1)], ssem.at[E_M])
    sent(gz.at[:, pl.ds(0, Z - 1)], ssem.at[E_AG])
    sent(rcy, ssem.at[E_RC])
    sent(rx1, ssem.at[E_RX])
    sent(rx2, ssem.at[E_RX2])
    sent(wc, ssem.at[E_WC])
    sent(wx.at[pl.ds(0, X - 1)], ssem.at[E_WX])
    sent(wy.at[pl.ds(0, Y - 1)], ssem.at[E_WY])
    sent(wz.at[pl.ds(0, Z - 1)], ssem.at[E_WZ])
    sent(oz.at[pl.ds(0, Z - 1)], ssem.at[E_OZ])
    sent(oy.at[pl.ds(0, Y - 1)], ssem.at[E_OY])
    sent(ox.at[pl.ds(0, X - 1)], ssem.at[E_OX])
    sent(oc.at[0], ssem.at[E_OC])
    sent(px.at[pl.ds(0, X - 1)], ssem.at[E_PX])
    sent(pz.at[pl.ds(0, C * Z - 1)], ssem.at[E_PZ])
    sent(qz.at[pl.ds(0, Z - 1)], ssem.at[E_QZ])
    sent(qy.at[pl.ds(0, Y - 1)], ssem.at[E_QY])
    sent(qx.at[pl.ds(0, X - 1)], ssem.at[E_QX])
    sent(qxy.at[pl.ds(0, X - 1)], ssem.at[E_QXY])
    sent(qyx.at[pl.ds(0, Y - 1)], ssem.at[E_QYX])


def solution(mesh):
    Y, X, C = Y_DIM, X_DIM, CORES
    Z = mesh.shape["rep"] // Y
    row_spec = P(("rep", "nodes"))

    def device_step(adj_blk, feat_blk, w_one, w_two, label_blk, mask_blk):
        R, S, CB = adj_blk.shape
        F, H = w_one.shape
        NC = w_two.shape[1]
        I = X * C
        NQ = Y * X
        HR = H // (2 * NSUB)
        HB = H // Y
        HU = HB // NV
        NCH = Y * S
        assert R == Z * Y and CB == S * I and X == Y and Z == 8 and F + 2 <= LANES // 2 and NC < LANES
        vm = pltpu.VMEM
        dma = pltpu.SemaphoreType.DMA
        scratch = [
            vm((Y, Z, Y, S, CB), BF),
            vm((F, S), BF),
            vm((1, S), jnp.int32),
            vm((1, S), jnp.int32),
            vm((LANES, S), F32),
            vm((S, LANES), F32),
            vm((F, H), F32),
            vm((H, NC), F32),
            vm((2, LANES, H), BF),
            vm((H, LANES), BF),
            vm((LANES, H), BF),
            vm((S // 2, LANES), BF),
            vm((C, NQ, S // 2, LANES), BF),
            vm((NCH, LANES), BF),
            vm((NQ, C, S, H), BF),
            vm((8, LANES), F32),
            vm((Z, 8, LANES), F32),
            vm((2 * NSUB, Z - 1, S, HR), F32),
            vm((2 * NSUB, Z - 1, S, HR), F32),
            vm((S, H), F32),
            vm((S, H), BF),
            vm((S, LANES), BF),
            vm((C, NQ, S, LANES), BF),
            vm((Z, S, LANES), F32),
            vm((Z, S, LANES), F32),
            vm((S, LANES), BF),
            vm((Z, S, LANES), BF),
            vm((Y, X, C, S, LANES), F32),
            vm((Y, X, S, LANES), F32),
            vm((X, Y, S // 2, LANES), F32),
            vm((Y, X, S // 2, LANES), F32),
            vm((Y, S // 2, LANES), F32),
            vm((X, S // 2, LANES), F32),
            vm((S, LANES), BF),
            vm((Y, S, LANES), BF),
            vm((Y, S, HB), BF),
            vm((Y, S, HB), BF),
            vm((NV, Z, Y, S, HU), BF),
            vm((NV // 2, 2 * HU, Z * Y * S), BF),
            vm((NV // 2, X, C, 2 * HU, NCH), F32),
            vm((NV // 2, X, 2 * HU, NCH), F32),
            vm((NV, 2, HU // 2, NCH), F32),
            vm((NV, 2, HU, NCH), F32),
            vm((C, X, Y, Z, 8, LANES), F32),
            vm((X, Y, Z, 8, LANES), F32),
            vm((X, Y, Z, 8, LANES), F32),
            vm((Y, Z, 8, LANES), F32),
            vm((Z, 8, LANES), F32),
            vm((8, LANES), F32),
            vm((Z, 8, LANES), F32),
            vm((Y, Z, 8, LANES), F32),
            vm((X, Y, Z, 8, LANES), F32),
            vm((C, X, Y, Z, 8, LANES), F32),
            vm((X, Z, 8, LANES), F32),
            vm((X, Z, 8, LANES), F32),
            vm((C * Z, 8, LANES), F32),
            vm((8, LANES), F32),
            vm((Z, 8, LANES), F32),
            vm((Y, Z // 2, 8, LANES), F32),
            vm((X, Z // 2, 8, LANES), F32),
            vm((X, Y, Z // 2, 8, LANES), F32),
            vm((Y, X, Z // 2, 8, LANES), F32),
            dma((NSEM,)),
            dma((NSEM,)),
            dma((Y - 1, Z)),
            dma((2, Y - 1)),
            dma((2, Y - 1)),
            dma((2 * NSUB, Z - 1)),
            dma((NV, 2, Z // 2 + 1)),
            dma((NV // 2, X)),
            dma((NV, 4)),
        ]
        vspec = pl.BlockSpec(memory_space=pltpu.VMEM)
        aspec = pl.BlockSpec(memory_space=pltpu.HBM)
        operands = (adj_blk.reshape(Z, Y, S, CB), feat_blk.T, label_blk[None, :], mask_blk[None, :], w_one, w_two)
        dw_one, dw_two, loss = pl.pallas_call(
            functools.partial(_step, (Z, Y, X, C, S, CB, H, F, NC)),
            out_shape=(jax.ShapeDtypeStruct((F, H), F32), jax.ShapeDtypeStruct((H, NC), F32), jax.ShapeDtypeStruct((8, LANES), F32)),
            in_specs=[aspec] * 6,
            out_specs=(vspec, vspec, vspec),
            scratch_shapes=scratch,
            compiler_params=pltpu.CompilerParams(collective_id=0, has_side_effects=True, vmem_limit_bytes=52 * 1024 * 1024),
            name="gcn_step",
        )(*[pltpu.with_memory_space_constraint(v, pltpu.HBM) for v in operands])
        return loss[0, 0], dw_one, dw_two

    return jax.shard_map(device_step, mesh=mesh, in_specs=(P(None, "nodes", "rep"), row_spec, P(), P(), row_spec, row_spec), out_specs=(P(), P(), P()), check_vma=False)
```

```python
import functools

import jax
import jax.numpy as jnp
from jax import lax
from jax.experimental import pallas as pl
from jax.experimental.pallas import tpu as pltpu
from jax.sharding import PartitionSpec as P

Y_DIM = 4
X_DIM = 4
CORES = 2
LANES = 128
NSUB = 4
NV = 4
NSEM = 46
BF = jnp.bfloat16
F32 = jnp.float32


def _step(dims, a_hbm, feat_hbm, lab_hbm, msk_hbm, w_one, w_two, dw1_out, dw2_out, loss_out,
          af, feat, lab, msk, mt, mtt, w1f, w2f, w1, w2, w2t, xs, xp, xn, y1, cs, cr, sb, rb, z1, h1, y2, yp, zp, zr, g2, gr, dp, rc, rx, ry, ry2, rx2d,
          d2, dg, ms, mk, gz, gt, dy, rcy, rx1, rx2, wb, wc, wx, wy, wz, wf, oz, oy, ox, oc, pb, px, pz, pf, qz, qy, qx, qxy, qyx,
          ssem, rsem, rsem_a, rsem_b, rsem_f, rsem_ring, rsem_ag, rsem_c, rsem_x):
    Z, Y, X, C, S, CB, H, F, NC = dims
    I = X * C
    NQ = Y * X
    HR = H // (2 * NSUB)
    HB = H // Y
    HU = HB // NV
    NCH = Y * S
    half = Z // 2
    rid = lax.axis_index("rep")
    nid = lax.axis_index("nodes")
    z, y, x, c = rid // Y, rid % Y, nid // C, nid % C
    chip = y * X + x
    partner = (rid, x * C + 1 - c)

    far = sorted(range(1, Z), key=lambda d: -min(d, Z - d))

    def at_z(zz):
        return (zz * Y + y, nid)

    def at_y(yy):
        return (z * Y + yy, nid)

    def at_x(xx):
        return (rid, xx * C + c)

    def at_chip(q):
        return (z * Y + q // X, (q % X) * C + c)

    def send(src, dst, ss, rs, dev):
        pltpu.make_async_remote_copy(src_ref=src, dst_ref=dst, send_sem=ss, recv_sem=rs, device_id=dev,
                                     device_id_type=pl.DeviceIdType.MESH).start()

    def arrived(ref, rs):
        pltpu.make_async_remote_copy(src_ref=ref, dst_ref=ref, send_sem=ssem.at[0], recv_sem=rs, device_id=partner,
                                     device_id_type=pl.DeviceIdType.MESH).wait_recv()

    def sent(ref, ss):
        pltpu.make_async_remote_copy(src_ref=ref, dst_ref=ref, send_sem=ss, recv_sem=rsem.at[0], device_id=partner,
                                     device_id_type=pl.DeviceIdType.MESH).wait_send()

    def dot(a, b):
        return jnp.dot(a, b, preferred_element_type=F32)

    def most(ref):
        return ref.at[0, pl.ds(0, NQ - 1)]

    def plane_rows(ref, yb):
        return jnp.stack([ref[k, yb * X:(yb + 1) * X] for k in range(C)], axis=1).reshape(CB, LANES)

    def turned(v):
        return jnp.concatenate([v[:, LANES // 2:], v[:, 0:LANES // 2]], axis=1)

    def added(ref, n):
        acc = ref[0]
        for k in range(1, n):
            acc = acc + ref[k]
        return acc

    (E_X, E_XC, E_A, E_B, E_F, E_RING, E_CNT, E_Y2, E_Y2C, E_Z2, E_G2, E_DC, E_DC1, E_DC2, E_DC3, E_DX, E_DY, E_AG, E_RC, E_RX, E_RX2,
     E_WC, E_WX, E_WY, E_WZ, E_OZ, E_OY, E_OX, E_OC, E_PX, E_PZ, E_QZ, E_QY, E_QX, E_LA, E_L1, E_L2,
     E_M, E_DY2, E_DX2, E_DG, E_QXY, E_QYX, E_IN, E_IN1, E_IN2) = range(NSEM)

    load_a = pltpu.make_async_copy(a_hbm, af.at[y], ssem.at[E_LA])
    load_1 = pltpu.make_async_copy(w_one, w1f, ssem.at[E_L1])
    load_2 = pltpu.make_async_copy(w_two, w2f, ssem.at[E_L2])
    loads = [pltpu.make_async_copy(src, dst, ssem.at[E_IN + k]) for k, (src, dst) in
             enumerate(((feat_hbm, feat), (lab_hbm, lab), (msk_hbm, msk)))]
    for load in loads:
        load.start()
    load_a.start()
    load_1.start()
    load_2.start()

    bar = pltpu.get_barrier_semaphore()
    for d in far:
        pl.semaphore_signal(bar, inc=1, device_id=at_z((z + d) % Z), device_id_type=pl.DeviceIdType.MESH)

    def greet_plane(d, u):
        pl.semaphore_signal(bar, inc=1, device_id=at_chip(lax.rem(chip + d, NQ)), device_id_type=pl.DeviceIdType.MESH)
        return u

    lax.fori_loop(1, NQ, greet_plane, 0)
    pl.semaphore_signal(bar, inc=1, device_id=partner, device_id_type=pl.DeviceIdType.MESH)

    for load in loads:
        load.wait()
    mt[...] = jnp.zeros_like(mt)
    mt[0:F] = feat[...].astype(F32)
    mt[F:F + 1] = msk[...].astype(F32)
    mt[F + 1:F + 2] = lab[...].astype(F32)
    mtt[...] = mt[...].T
    xs[...] = (mtt[0:S // 2] + turned(mtt[S // 2:S])).astype(BF)
    pl.semaphore_wait(bar, NQ + Z - 1)

    def send_x(d, u):
        q = lax.rem(chip + d, NQ)
        send(xs, xp.at[c, chip], ssem.at[E_X], rsem.at[E_X], at_chip(q))
        return u

    lax.fori_loop(1, NQ, send_x, 0)
    xp[c, chip] = xs[...]
    load_a.wait()

    order = []
    for k in range(1, half + 1):
        order.append(-k)
        if k < half:
            order.append(k)
    order.append(0)
    for k in order:
        zc = (z + k + Z) % Z
        for d in (2, 1, 3):
            yq = (y + d) % Y
            send(af.at[y, zc, yq], af.at[y, zc, yq], ssem.at[E_A], rsem_a.at[d - 1, zc], at_y(yq))
    def spread_a(k, lo, n, slot):
        for d in (1, 3):
            yq = (y + d) % Y
            ref = af.at[y, pl.ds(lo, n), (yq + k) % Y]
            send(ref, ref, ssem.at[E_B], rsem_b.at[d // 2, slot], at_y(yq))

    def forward_a():
        for d in (1, 3):
            for slot, n in enumerate((Z, Z, half, half)):
                arrived(af.at[0, pl.ds(0, n), 0], rsem_b.at[d // 2, slot])
        for k in range(1, Y):
            for d in (1, 3):
                ys, yq = (y - d + Y) % Y, (y + d) % Y
                lo = 0 if d == 1 else half
                ya = (yq + k) % Y
                send(af.at[ys, pl.ds(lo, half), ya], af.at[ys, pl.ds(lo, half), ya], ssem.at[E_F], rsem_f.at[d // 2, k - 1], at_y(yq))

    spread_a(1, 0, Z, 0)
    spread_a(2, 0, Z, 1)
    spread_a(3, 0, half, 2)

    load_1.wait()
    w1[...] = jnp.zeros_like(w1)
    w1[0, 0:F] = w1f[...].astype(BF)
    w1[1, LANES // 2:LANES // 2 + F] = w1f[...].astype(BF)
    load_2.wait()
    w2[...] = jnp.zeros_like(w2)
    for k in range(Y):
        rows = slice(k * HB, (k + 1) * HB)
        w2[rows, 0:NC] = w2f[rows].astype(BF)
        w2t[:, rows] = w2[rows].T

    arrived(most(xp), rsem.at[E_X])
    send(xp.at[c], xp.at[c], ssem.at[E_XC], rsem.at[E_XC], partner)

    def columns(j):
        return pl.ds(pl.multiple_of(j * HR, HR), HR)

    def y1_half(k, j):
        rows = xp[k].reshape(NQ * S // 2, LANES)
        for m in range(2):
            y1[:, k, m * (S // 2):(m + 1) * (S // 2), columns(j)] = dot(rows, w1[m, :, columns(j)]).astype(BF).reshape(NQ, S // 2, HR)

    def y1_own(j, u):
        y1_half(c, j)
        return u

    def y1_block(yb, j):
        return y1[yb * X:(yb + 1) * X, :, :, columns(j)].reshape(CB, HR)

    lax.fori_loop(0, 2 * NSUB, y1_own, 0)
    arrived(xp.at[0], rsem.at[E_XC])

    def wait_a(zc):
        for d in range(1, Y):
            arrived(af.at[0, 0, 0], rsem_a.at[d - 1, zc])

    def products(s, j):
        up = j % 2 == 0
        dest = lax.rem(jnp.where(up, z - 1 - s, z + 1 + s) + 2 * Z, Z)
        fresh = ((j == 0) & ((s < half) | (s == Z - 1))) | ((j == 1) & (s < half - 1))

        @pl.when(fresh)
        def _():
            wait_a(dest)

        acc = dot(af[0, dest, y], y1_block(0, j))
        for yb in range(1, Y):
            acc = acc + dot(af[yb, dest, y], y1_block(yb, j))
        return acc

    def pass_on(s, j):
        nb = lax.rem(jnp.where(j % 2 == 0, z + 1, z - 1) + Z, Z)
        send(sb.at[j, s], rb.at[j, s], ssem.at[E_RING], rsem_ring.at[j, s], at_z(nb))

    def ring_first(j, u):
        y1_half(1 - c, j)
        sb[j, 0] = products(0, j)
        pass_on(0, j)
        return u

    def ring_next(t, u):
        s, j = t // (2 * NSUB) + 1, t % (2 * NSUB)
        acc = products(s, j)
        arrived(rb.at[0, 0], rsem_ring.at[j, s - 1])
        sb[j, s] = acc + rb[j, s - 1]
        pass_on(s, j)
        return u

    def ring_last(j, u):
        acc = products(Z - 1, j)
        arrived(rb.at[0, 0], rsem_ring.at[j, Z - 2])
        z1[:, columns(j)] = acc + rb[j, Z - 2]
        return u

    lax.fori_loop(0, 2 * NSUB, ring_first, 0)
    lax.fori_loop(0, (Z - 2) * 2 * NSUB, ring_next, 0)
    lax.fori_loop(0, 2 * NSUB, ring_last, 0)

    h1[...] = jnp.maximum(z1[...], 0.0).astype(BF)
    y2[...] = dot(h1[...], w2[...]).astype(BF)

    def send_y2(d, u):
        q = lax.rem(chip + d, NQ)
        send(y2, yp.at[c, chip], ssem.at[E_Y2], rsem.at[E_Y2], at_chip(q))
        return u

    lax.fori_loop(1, NQ, send_y2, 0)
    yp[c, chip] = y2[...]
    lane = lax.broadcasted_iota(jnp.int32, (S, LANES), 1)
    counted = jnp.sum(xp[...].astype(F32).reshape(Y * CB // 2, LANES), axis=0, keepdims=True)
    counted = jnp.sum(jnp.where(lane[0:1] % (LANES // 2) == F, counted, 0.0), axis=1, keepdims=True)
    cs[...] = jnp.broadcast_to(counted, (8, LANES))
    cr[z] = cs[...]
    for d in far:
        send(cs, cr.at[z], ssem.at[E_CNT], rsem.at[E_CNT], at_z((z + d) % Z))
    arrived(most(yp), rsem.at[E_Y2])
    send(yp.at[c], yp.at[c], ssem.at[E_Y2C], rsem.at[E_Y2C], partner)
    arrived(yp.at[0], rsem.at[E_Y2C])
    def z2_part(zq):
        part = dot(af[0, zq, y], plane_rows(yp, 0))
        for yb in range(1, Y):
            part = part + dot(af[yb, zq, y], plane_rows(yp, yb))
        return part

    for d in far:
        zq = (z + d) % Z
        zp[zq] = z2_part(zq)
        send(zp.at[zq], zr.at[z], ssem.at[E_Z2], rsem.at[E_Z2], at_z(zq))
    zr[z] = z2_part(z)
    for yb in range(Y):
        ms[yb] = jnp.where(z1[:, yb * HB:(yb + 1) * HB] > 0.0, 1.0, 0.0).astype(BF)
    for d in (2, 1, 3):
        yq = (y + d) % Y
        send(ms.at[yq], mk.at[y], ssem.at[E_M], rsem.at[E_M], at_y(yq))
    mk[y] = ms[y]
    spread_a(3, half, half, 3)
    arrived(zr.at[pl.ds(0, Z - 1)], rsem.at[E_Z2])
    z2 = added(zr, Z)

    arrived(cr.at[pl.ds(0, Z - 1)], rsem.at[E_CNT])
    count = added(cr, Z)[0:1, 0:1]
    own = mtt[...]
    weights = jnp.sum(jnp.where(lane == F, own, 0.0), axis=1, keepdims=True)
    labels = jnp.sum(jnp.where(lane == F + 1, own, 0.0), axis=1, keepdims=True)
    real = lane < NC
    top = jnp.max(jnp.where(real, z2, -jnp.inf), axis=1, keepdims=True)
    shifted = jnp.where(real, z2 - top, 0.0)
    log_probs = shifted - jnp.log(jnp.sum(jnp.where(real, jnp.exp(shifted), 0.0), axis=1, keepdims=True))
    hot = labels == lane.astype(F32)
    picked = jnp.sum(jnp.where(hot, log_probs, 0.0), axis=1, keepdims=True)
    loss_part = -jnp.sum(weights * picked, axis=0, keepdims=True)
    diff = jnp.where(real, jnp.exp(log_probs), 0.0) - hot.astype(F32)
    g2[...] = (diff * (weights / count)).astype(BF)
    for d in far:
        send(g2, gr.at[z], ssem.at[E_G2], rsem.at[E_G2], at_z((z + d) % Z))
    gr[z] = g2[...]
    arrived(gr.at[pl.ds(0, Z - 1)], rsem.at[E_G2])

    g2t = gr[...].reshape(Z * S, LANES).T
    for yb in range(Y):
        part = dot(g2t, af[yb, :, y].reshape(Z * S, CB))
        dp[yb] = part.T.reshape(X, C, S, LANES)
        send(dp.at[yb, :, 1 - c], rc.at[yb], ssem.at[E_DC + yb], rsem.at[E_DC + yb], partner)
    for yb in range(Y):
        arrived(rc.at[yb], rsem.at[E_DC + yb])
        rc[yb] = rc[yb] + dp[yb, :, c]
    sh = S // 2
    for d in (2, 1, 3):
        xq, yq = (x + d) % X, (y + d) % Y
        send(rc.at[:, xq, pl.ds(0, sh)], rx.at[x], ssem.at[E_DX], rsem.at[E_DX], at_x(xq))
        send(rc.at[yq, :, pl.ds(sh, sh)], ry.at[y], ssem.at[E_DY], rsem.at[E_DY], at_y(yq))
    rx[x] = rc[:, x, 0:sh]
    ry[y] = rc[y, :, sh:S]
    arrived(rx.at[pl.ds(0, X - 1)], rsem.at[E_DX])
    rx[x] = added(rx, X)
    for d in (2, 1, 3):
        yq = (y + d) % Y
        send(rx.at[x, yq], ry2.at[y], ssem.at[E_DY2], rsem.at[E_DY2], at_y(yq))
    ry2[y] = rx[x, y]
    arrived(ry.at[pl.ds(0, Y - 1)], rsem.at[E_DY])
    ry[y] = added(ry, Y)
    for d in (2, 1, 3):
        xq = (x + d) % X
        send(ry.at[y, xq], rx2d.at[x], ssem.at[E_DX2], rsem.at[E_DX2], at_x(xq))
    rx2d[x] = ry[y, x]
    arrived(ry2.at[pl.ds(0, Y - 1)], rsem.at[E_DY2])
    arrived(rx2d.at[pl.ds(0, X - 1)], rsem.at[E_DX2])
    d2[0:sh] = added(ry2, Y).astype(BF)
    d2[sh:S] = added(rx2d, X).astype(BF)
    for d in (2, 1, 3):
        send(d2, dg.at[y], ssem.at[E_DG], rsem.at[E_DG], at_y((y + d) % Y))
    dg[y] = d2[...]
    forward_a()
    dy2 = d2[...]

    def g_one(v):
        col = pl.multiple_of(y * HB + v * HU, HU)
        dh = dot(dg[...].reshape(Y * S, LANES), w2t[:, pl.ds(col, HU)])
        keep = mk[:, :, v * HU:(v + 1) * HU].reshape(Y * S, HU).astype(F32)
        gz[v, z] = jnp.where(keep > 0.0, dh, 0.0).astype(BF).reshape(Y, S, HU)

    def gather_step(v, t):
        for d in range(2):
            sgn = 1 if d == 0 else -1
            blk = (z - sgn * (t - 1) + Z) % Z
            if t > 1:
                arrived(gz.at[v, 0], rsem_ag.at[v, d, t - 1])
            ref = gz.at[v, blk] if t < half else gz.at[v, blk, pl.ds(d * (Y // 2), Y // 2)]
            send(ref, ref, ssem.at[E_AG], rsem_ag.at[v, d, t], at_z((z + sgn + Z) % Z))

    def piece(v):
        return pl.ds(v % 2 * HU, HU)

    def prepare(p):
        for v in (2 * p, 2 * p + 1):
            for d in range(2):
                arrived(gz.at[v, 0, pl.ds(0, Y // 2)], rsem_ag.at[v, d, half])
            for k in range(Z):
                gt[p, piece(v), k * Y * S:(k + 1) * Y * S] = gz[v, k].reshape(Y * S, HU).T

    nxt, prv, opp = (x + 1) % X, (x + X - 1) % X, (x + 2) % X
    hh = HU // 2

    def low(v):
        return pl.ds(v % 2 * HU, hh)

    def high(v):
        return pl.ds(v % 2 * HU + hh, hh)

    def chunk(p, xb, core):
        off = pl.multiple_of(core * NCH, NCH)
        dy[p, xb, core] = dot(gt[p], af[xb, :, :, :, pl.ds(off, NCH)].reshape(Z * Y * S, NCH))

    def send_core(p, k):
        xb = (x + 2 + k) % X
        send(dy.at[p, xb, 1 - c], rcy.at[p, xb], ssem.at[E_RC], rsem_c.at[p, k], partner)

    def chunks_far(p):
        if p == 0:
            for d in (1, 3):
                for k in range(1, Y):
                    arrived(af.at[0, pl.ds(0, half), 0], rsem_f.at[d // 2, k - 1])
        chunk(p, opp, 1 - c)
        send_core(p, 0)
        chunk(p, opp, c)

    def chunks_rest(p, own):
        def body(k, u):
            chunk(p, lax.rem(x + 2 + k, X), c if own else 1 - c)
            return u

        lax.fori_loop(1, X, body, 0)
        if not own:
            for k in range(1, X):
                send_core(p, k)

    def sum_core(p, k):
        xb = (x + 2 + k) % X
        arrived(rcy.at[p, xb], rsem_c.at[p, k])
        rcy[p, xb] = rcy[p, xb] + dy[p, xb, c]

    def reduce_far(p):
        sum_core(p, 0)
        for v in (2 * p, 2 * p + 1):
            send(rcy.at[p, opp, low(v)], rx1.at[v, 0], ssem.at[E_RX], rsem_x.at[v, 0], at_x(nxt))
            send(rcy.at[p, opp, high(v)], rx1.at[v, 1], ssem.at[E_RX], rsem_x.at[v, 1], at_x(prv))

    def far_and_rest(p):
        @pl.when(c == 0)
        def _():
            reduce_far(p)
            if p == 0:
                gather_step(2, 3)
                gather_step(3, 3)
            chunks_rest(p, False)

        @pl.when(c == 1)
        def _():
            if p == 0:
                gather_step(2, 3)
                gather_step(3, 3)
            chunks_rest(p, False)
            reduce_far(p)

    def reduce_rest(p):
        for k in range(1, X):
            sum_core(p, k)

    def reduce_x(v):
        p = v // 2
        arrived(rx1.at[v, 0], rsem_x.at[v, 0])
        rcy[p, nxt, low(v)] = rcy[p, nxt, low(v)] + rx1[v, 0]
        send(rcy.at[p, nxt, piece(v)], rx2.at[v, 0], ssem.at[E_RX2], rsem_x.at[v, 2], at_x(nxt))
        arrived(rx1.at[v, 1], rsem_x.at[v, 1])
        rcy[p, prv, high(v)] = rcy[p, prv, high(v)] + rx1[v, 1]
        send(rcy.at[p, prv, piece(v)], rx2.at[v, 1], ssem.at[E_RX2], rsem_x.at[v, 3], at_x(prv))

    def own_x():
        low_half = lax.broadcasted_iota(jnp.int32, (S // 2, LANES), 1) < LANES // 2
        for m in range(Y):
            rows = xp[m % C, nid * (Y // C) + m // C].astype(F32)
            xn[m * S:m * S + S // 2] = jnp.where(low_half, rows, 0.0).astype(BF)
            xn[m * S + S // 2:(m + 1) * S] = jnp.where(low_half, turned(rows), 0.0).astype(BF)

    def grad_one(v):
        arrived(rx2.at[v, 0], rsem_x.at[v, 2])
        arrived(rx2.at[v, 1], rsem_x.at[v, 3])
        acc = (rcy[v // 2, x, piece(v)] + rx2[v, 0] + rx2[v, 1]).astype(BF)
        part = dot(acc, xn[...])
        if v >= NV // 2:
            part = turned(part)
        per = HU // (Z * 8)
        rows = part.reshape(per, Z, 8, LANES)
        for m in range(per):
            k = (v % (NV // 2)) * per + m
            pb[k] = rows[m] if v < NV // 2 else pb[k] + rows[m]

    def w_begin():
        mark = (lax.broadcasted_iota(jnp.int32, (HB, LANES), 0) == 0) & (lax.broadcasted_iota(jnp.int32, (HB, LANES), 1) == NC)
        for k in range(Y):
            part = lax.dot_general(h1[:, k * HB:(k + 1) * HB], dy2, (((0,), (0,)), ((), ())), preferred_element_type=F32)
            if k == 0:
                part = jnp.where(mark, loss_part, part)
            per = HB // (Y * Z * 8)
            rows = part.reshape(per, Y, Z, 8, LANES)
            for m in range(per):
                q = k * per + m
                wb[q // X, q % X] = rows[m]
        send(wb.at[1 - c], wc, ssem.at[E_WC], rsem.at[E_WC], partner)

    def w_core():
        arrived(wc, rsem.at[E_WC])
        wc[...] = wc[...] + wb[c]
        for d in (2, 1, 3):
            xq = (x + d) % X
            send(wc.at[xq], wx.at[x], ssem.at[E_WX], rsem.at[E_WX], at_x(xq))
        wx[x] = wc[x]

    def w_x():
        arrived(wx.at[pl.ds(0, X - 1)], rsem.at[E_WX])
        wx[x] = added(wx, X)
        for d in (2, 1, 3):
            yq = (y + d) % Y
            send(wx.at[x, yq], wy.at[y], ssem.at[E_WY], rsem.at[E_WY], at_y(yq))
        wy[y] = wx[x, y]

    def w_y():
        arrived(wy.at[pl.ds(0, Y - 1)], rsem.at[E_WY])
        wy[y] = added(wy, Y)
        for d in far:
            zq = (z + d) % Z
            send(wy.at[y, zq], wz.at[z], ssem.at[E_WZ], rsem.at[E_WZ], at_z(zq))
        wz[z] = wy[y, z]

    def w_z():
        arrived(wz.at[pl.ds(0, Z - 1)], rsem.at[E_WZ])
        wf[...] = added(wz, Z)
        for d in far:
            send(wf, oz.at[z], ssem.at[E_OZ], rsem.at[E_OZ], at_z((z + d) % Z))
        oz[z] = wf[...]

    def o_z():
        arrived(oz.at[pl.ds(0, Z - 1)], rsem.at[E_OZ])
        for d in (2, 1, 3):
            send(oz, oy.at[y], ssem.at[E_OY], rsem.at[E_OY], at_y((y + d) % Y))
        oy[y] = oz[...]

    def o_y():
        arrived(oy.at[pl.ds(0, Y - 1)], rsem.at[E_OY])
        for d in (2, 1, 3):
            send(oy, ox.at[x], ssem.at[E_OX], rsem.at[E_OX], at_x((x + d) % X))
        ox[x] = oy[...]

    def o_x():
        arrived(ox.at[pl.ds(0, X - 1)], rsem.at[E_OX])
        send(ox, oc.at[c], ssem.at[E_OC], rsem.at[E_OC], partner)
        oc[c] = ox[...]

    arrived(mk.at[pl.ds(0, Y - 1)], rsem.at[E_M])
    arrived(dg.at[pl.ds(0, Y - 1)], rsem.at[E_DG])
    steps = [
        (g_one, 0), (gather_step, 0, 1), (g_one, 1), (gather_step, 1, 1), (g_one, 2), (g_one, 3), (w_begin,), (own_x,),
        (gather_step, 0, 2), (gather_step, 1, 2), (w_core,), (gather_step, 2, 1),
        (gather_step, 0, 3), (gather_step, 1, 3), (gather_step, 3, 1),
        (gather_step, 0, 4), (gather_step, 1, 4), (gather_step, 2, 2), (gather_step, 3, 2),
        (prepare, 0), (chunks_far, 0), (far_and_rest, 0),
        (chunks_rest, 0, True), (gather_step, 2, 4), (reduce_rest, 0), (reduce_x, 0), (gather_step, 3, 4), (reduce_x, 1), (w_x,),
        (prepare, 1), (chunks_far, 1), (far_and_rest, 1), (w_y,), (chunks_rest, 1, True), (reduce_rest, 1), (grad_one, 0), (grad_one, 1),
        (reduce_x, 2), (reduce_x, 3), (w_z,), (grad_one, 2), (o_z,), (grad_one, 3)]
    for step in steps:
        step[0](*step[1:])

    for d in (2, 1, 3):
        xq = (x + d) % X
        send(pb.at[xq], px.at[x], ssem.at[E_PX], rsem.at[E_PX], at_x(xq))
    px[x] = pb[x]
    arrived(px.at[pl.ds(0, X - 1)], rsem.at[E_PX])
    px[x] = added(px, X)
    for d in far:
        zq = (z + d) % Z
        for k in range(C):
            send(px.at[x, zq], pz.at[c * Z + z], ssem.at[E_PZ], rsem.at[E_PZ], (zq * Y + y, x * C + k))
    send(px.at[x, z], pz.at[c * Z + z], ssem.at[E_PZ], rsem.at[E_PZ], partner)
    pz[c * Z + z] = px[x, z]
    o_y()
    arrived(pz.at[pl.ds(0, C * Z - 1)], rsem.at[E_PZ])
    pf[...] = added(pz, C * Z)
    for d in far:
        send(pf, qz.at[z], ssem.at[E_QZ], rsem.at[E_QZ], at_z((z + d) % Z))
    qz[z] = pf[...]
    arrived(qz.at[pl.ds(0, Z - 1)], rsem.at[E_QZ])
    zl, zh = pl.ds(0, half), pl.ds(half, half)
    for d in (2, 1, 3):
        send(qz.at[zl], qy.at[y], ssem.at[E_QY], rsem.at[E_QY], at_y((y + d) % Y))
        send(qz.at[zh], qx.at[x], ssem.at[E_QX], rsem.at[E_QX], at_x((x + d) % X))
    qy[y] = qz[zl]
    qx[x] = qz[zh]
    o_x()
    arrived(qy.at[pl.ds(0, Y - 1)], rsem.at[E_QY])
    for d in (2, 1, 3):
        send(qy, qxy.at[x], ssem.at[E_QXY], rsem.at[E_QXY], at_x((x + d) % X))
    qxy[x] = qy[...]
    arrived(qx.at[pl.ds(0, X - 1)], rsem.at[E_QX])
    for d in (2, 1, 3):
        send(qx, qyx.at[y], ssem.at[E_QYX], rsem.at[E_QYX], at_y((y + d) % Y))
    qyx[y] = qx[...]
    arrived(oc.at[0], rsem.at[E_OC])
    for k in range(C):
        full = oc[k].reshape(H // C, LANES)
        dw2_out[k * (H // C):(k + 1) * (H // C), :] = full[:, 0:NC]
        if k == 0:
            loss_out[...] = jnp.broadcast_to(full[0:1, NC:NC + 1] / count, (8, LANES))
    arrived(qxy.at[pl.ds(0, X - 1)], rsem.at[E_QXY])
    arrived(qyx.at[pl.ds(0, Y - 1)], rsem.at[E_QYX])
    for yb in range(Y):
        part = jnp.concatenate([qxy[:, yb], qyx[yb]], axis=1).reshape(HB // 2, LANES).T
        dw1_out[:, yb * HB:yb * HB + HB // 2] = part[0:F]
        dw1_out[:, yb * HB + HB // 2:(yb + 1) * HB] = part[LANES // 2:LANES // 2 + F]

    sent(most(xp), ssem.at[E_X])
    sent(xp.at[0], ssem.at[E_XC])
    sent(af.at[pl.ds(0, Y - 1), :, 0], ssem.at[E_A])
    sent(af.at[pl.ds(0, Y - 1), :, pl.ds(0, 2)], ssem.at[E_B])
    sent(af.at[pl.ds(0, Y - 1), :, 0], ssem.at[E_F])
    sent(sb, ssem.at[E_RING])
    sent(cr.at[pl.ds(0, Z - 1)], ssem.at[E_CNT])
    sent(most(yp), ssem.at[E_Y2])
    sent(yp.at[0], ssem.at[E_Y2C])
    sent(zr.at[pl.ds(0, Z - 1)], ssem.at[E_Z2])
    sent(gr.at[pl.ds(0, Z - 1)], ssem.at[E_G2])
    for yb in range(Y):
        sent(rc.at[yb], ssem.at[E_DC + yb])
    sent(rx.at[pl.ds(0, X - 1)], ssem.at[E_DX])
    sent(ry.at[pl.ds(0, Y - 1)], ssem.at[E_DY])
    sent(ry2.at[pl.ds(0, Y - 1)], ssem.at[E_DY2])
    sent(rx2d.at[pl.ds(0, X - 1)], ssem.at[E_DX2])
    sent(dg.at[pl.ds(0, Y - 1)], ssem.at[E_DG])
    sent(mk.at[pl.ds(0, Y - 1)], ssem.at[E_M])
    sent(gz.at[:, pl.ds(0, Z - 1)], ssem.at[E_AG])
    sent(rcy, ssem.at[E_RC])
    sent(rx1, ssem.at[E_RX])
    sent(rx2, ssem.at[E_RX2])
    sent(wc, ssem.at[E_WC])
    sent(wx.at[pl.ds(0, X - 1)], ssem.at[E_WX])
    sent(wy.at[pl.ds(0, Y - 1)], ssem.at[E_WY])
    sent(wz.at[pl.ds(0, Z - 1)], ssem.at[E_WZ])
    sent(oz.at[pl.ds(0, Z - 1)], ssem.at[E_OZ])
    sent(oy.at[pl.ds(0, Y - 1)], ssem.at[E_OY])
    sent(ox.at[pl.ds(0, X - 1)], ssem.at[E_OX])
    sent(oc.at[0], ssem.at[E_OC])
    sent(px.at[pl.ds(0, X - 1)], ssem.at[E_PX])
    sent(pz.at[pl.ds(0, C * Z - 1)], ssem.at[E_PZ])
    sent(qz.at[pl.ds(0, Z - 1)], ssem.at[E_QZ])
    sent(qy.at[pl.ds(0, Y - 1)], ssem.at[E_QY])
    sent(qx.at[pl.ds(0, X - 1)], ssem.at[E_QX])
    sent(qxy.at[pl.ds(0, X - 1)], ssem.at[E_QXY])
    sent(qyx.at[pl.ds(0, Y - 1)], ssem.at[E_QYX])


def solution(mesh):
    Y, X, C = Y_DIM, X_DIM, CORES
    Z = mesh.shape["rep"] // Y
    row_spec = P(("rep", "nodes"))

    def device_step(adj_blk, feat_blk, w_one, w_two, label_blk, mask_blk):
        R, S, CB = adj_blk.shape
        F, H = w_one.shape
        NC = w_two.shape[1]
        I = X * C
        NQ = Y * X
        HR = H // (2 * NSUB)
        HB = H // Y
        HU = HB // NV
        NCH = Y * S
        assert R == Z * Y and CB == S * I and X == Y and Z == 8 and F + 2 <= LANES // 2 and NC < LANES
        vm = pltpu.VMEM
        dma = pltpu.SemaphoreType.DMA
        scratch = [
            vm((Y, Z, Y, S, CB), BF),
            vm((F, S), BF),
            vm((1, S), jnp.int32),
            vm((1, S), jnp.int32),
            vm((LANES, S), F32),
            vm((S, LANES), F32),
            vm((F, H), F32),
            vm((H, NC), F32),
            vm((2, LANES, H), BF),
            vm((H, LANES), BF),
            vm((LANES, H), BF),
            vm((S // 2, LANES), BF),
            vm((C, NQ, S // 2, LANES), BF),
            vm((NCH, LANES), BF),
            vm((NQ, C, S, H), BF),
            vm((8, LANES), F32),
            vm((Z, 8, LANES), F32),
            vm((2 * NSUB, Z - 1, S, HR), F32),
            vm((2 * NSUB, Z - 1, S, HR), F32),
            vm((S, H), F32),
            vm((S, H), BF),
            vm((S, LANES), BF),
            vm((C, NQ, S, LANES), BF),
            vm((Z, S, LANES), F32),
            vm((Z, S, LANES), F32),
            vm((S, LANES), BF),
            vm((Z, S, LANES), BF),
            vm((Y, X, C, S, LANES), F32),
            vm((Y, X, S, LANES), F32),
            vm((X, Y, S // 2, LANES), F32),
            vm((Y, X, S // 2, LANES), F32),
            vm((Y, S // 2, LANES), F32),
            vm((X, S // 2, LANES), F32),
            vm((S, LANES), BF),
            vm((Y, S, LANES), BF),
            vm((Y, S, HB), BF),
            vm((Y, S, HB), BF),
            vm((NV, Z, Y, S, HU), BF),
            vm((NV // 2, 2 * HU, Z * Y * S), BF),
            vm((NV // 2, X, C, 2 * HU, NCH), F32),
            vm((NV // 2, X, 2 * HU, NCH), F32),
            vm((NV, 2, HU // 2, NCH), F32),
            vm((NV, 2, HU, NCH), F32),
            vm((C, X, Y, Z, 8, LANES), F32),
            vm((X, Y, Z, 8, LANES), F32),
            vm((X, Y, Z, 8, LANES), F32),
            vm((Y, Z, 8, LANES), F32),
            vm((Z, 8, LANES), F32),
            vm((8, LANES), F32),
            vm((Z, 8, LANES), F32),
            vm((Y, Z, 8, LANES), F32),
            vm((X, Y, Z, 8, LANES), F32),
            vm((C, X, Y, Z, 8, LANES), F32),
            vm((X, Z, 8, LANES), F32),
            vm((X, Z, 8, LANES), F32),
            vm((C * Z, 8, LANES), F32),
            vm((8, LANES), F32),
            vm((Z, 8, LANES), F32),
            vm((Y, Z // 2, 8, LANES), F32),
            vm((X, Z // 2, 8, LANES), F32),
            vm((X, Y, Z // 2, 8, LANES), F32),
            vm((Y, X, Z // 2, 8, LANES), F32),
            dma((NSEM,)),
            dma((NSEM,)),
            dma((Y - 1, Z)),
            dma((2, 4)),
            dma((2, Y - 1)),
            dma((2 * NSUB, Z - 1)),
            dma((NV, 2, Z // 2 + 1)),
            dma((NV // 2, X)),
            dma((NV, 4)),
        ]
        vspec = pl.BlockSpec(memory_space=pltpu.VMEM)
        aspec = pl.BlockSpec(memory_space=pltpu.HBM)
        operands = (adj_blk.reshape(Z, Y, S, CB), feat_blk.T, label_blk[None, :], mask_blk[None, :], w_one, w_two)
        dw_one, dw_two, loss = pl.pallas_call(
            functools.partial(_step, (Z, Y, X, C, S, CB, H, F, NC)),
            out_shape=(jax.ShapeDtypeStruct((F, H), F32), jax.ShapeDtypeStruct((H, NC), F32), jax.ShapeDtypeStruct((8, LANES), F32)),
            in_specs=[aspec] * 6,
            out_specs=(vspec, vspec, vspec),
            scratch_shapes=scratch,
            compiler_params=pltpu.CompilerParams(collective_id=0, has_side_effects=True, vmem_limit_bytes=52 * 1024 * 1024),
            name="gcn_step",
        )(*[pltpu.with_memory_space_constraint(v, pltpu.HBM) for v in operands])
        return loss[0, 0], dw_one, dw_two

    return jax.shard_map(device_step, mesh=mesh, in_specs=(P(None, "nodes", "rep"), row_spec, P(), P(), row_spec, row_spec), out_specs=(P(), P(), P()), check_vma=False)
```
